8 devices in a mesh: data: 8 (over z, y, x, core).
Axes of the slice: x: 2, y: 2, z: 1, core: 2. Of those that a mesh axis runs over, the one named last changes fastest.
Arguments:
- x_now: bfloat16 [32, 784, 128], P('data')
- labels_now: int32 [32], P('data')
- x_next: bfloat16 [32, 784, 128], P('data')
- up_one: float32 [2, 128, 512], replicated
- down_one: float32 [2, 512, 128], replicated
- merge_proj: float32 [512, 512], replicated
- up_two: float32 [2, 512, 2048], replicated
- down_two: float32 [2, 2048, 512], replicated
- head_proj: float32 [512, 1000], replicated
- vel_up_one: float32 [2, 128, 512], replicated
- vel_down_one: float32 [2, 512, 128], replicated
- vel_merge_proj: float32 [512, 512], replicated
- vel_up_two: float32 [2, 512, 2048], replicated
- vel_down_two: float32 [2, 2048, 512], replicated
- vel_head_proj: float32 [512, 1000], replicated
Outputs:
- output 1: float32 [32, 1000], P('data')
- output 2: float32 [2, 128, 512], replicated
- output 3: float32 [2, 512, 128], replicated
- output 4: float32 [512, 512], replicated
- output 5: float32 [2, 512, 2048], replicated
- output 6: float32 [2, 2048, 512], replicated
- output 7: float32 [512, 1000], replicated
- output 8: float32 [2, 128, 512], replicated
- output 9: float32 [2, 512, 128], replicated
- output 10: float32 [512, 512], replicated
- output 11: float32 [2, 512, 2048], replicated
- output 12: float32 [2, 2048, 512], replicated
- output 13: float32 [512, 1000], replicated
All inputs are finite; a program needn't handle non-finite values.
Results may differ from the reference program's by a relative error of at most 0.0111885.
Values are sent between devices in bfloat16 or wider.
A program may use at most 1 GiB of HBM per device.

```python
import jax
import jax.numpy as jnp
from jax import lax

DATA_DEVS = 8
IMAGES_DEV = 4
TOKENS = 784
WIDTH = 128
DEPTH_ONE = 2
DEPTH_TWO = 2
CLASSES = 1000
BATCH = DATA_DEVS * IMAGES_DEV
MERGED = TOKENS // 4
WIDTH_TWO = 4 * WIDTH
HIDDEN_ONE = 4 * WIDTH
HIDDEN_TWO = 4 * WIDTH_TWO
MOMENTUM = 0.9
TRUST = 0.1
LN_EPS = 1e-6
SHIFT_SCALE = 1.5


def draw_weight(key_w, shape_w, fan_in, scale):
    return jax.random.normal(key_w, shape_w, jnp.float32) * (scale * fan_in ** -0.5)


def draw_images(key_img, key_shift):
    img_shift = jax.random.normal(key_shift, (BATCH, 1, WIDTH), jnp.float32) * SHIFT_SCALE
    raw_vals = jax.random.normal(key_img, (BATCH, TOKENS, WIDTH), jnp.float32)
    return (raw_vals + img_shift).astype(jnp.bfloat16)


def setup_inputs(seed: int = 0) -> dict:
    key_list = jax.random.split(jax.random.key(seed), 17)
    draw_specs = [
        ('up_one', (DEPTH_ONE, WIDTH, HIDDEN_ONE), WIDTH),
        ('down_one', (DEPTH_ONE, HIDDEN_ONE, WIDTH), HIDDEN_ONE),
        ('merge_proj', (4 * WIDTH, WIDTH_TWO), 4 * WIDTH),
        ('up_two', (DEPTH_TWO, WIDTH_TWO, HIDDEN_TWO), WIDTH_TWO),
        ('down_two', (DEPTH_TWO, HIDDEN_TWO, WIDTH_TWO), HIDDEN_TWO),
        ('head_proj', (WIDTH_TWO, CLASSES), WIDTH_TWO),
    ]
    drawn = {}
    drawn['x_now'] = draw_images(key_list[0], key_list[15])
    drawn['labels_now'] = jax.random.randint(key_list[1], (BATCH,), 0, CLASSES, jnp.int32)
    drawn['x_next'] = draw_images(key_list[2], key_list[16])
    for slot_num, spec_w in enumerate(draw_specs):
        drawn[spec_w[0]] = draw_weight(key_list[3 + slot_num], spec_w[1], spec_w[2], 1.0)
    for slot_num, spec_w in enumerate(draw_specs):
        drawn['vel_' + spec_w[0]] = draw_weight(key_list[9 + slot_num], spec_w[1], spec_w[2], TRUST)
    return drawn


def layer_norm(values):
    row_mean = jnp.mean(values, axis=-1, keepdims=True)
    centered = values - row_mean
    variance = jnp.mean(centered * centered, axis=-1, keepdims=True)
    return centered * lax.rsqrt(variance + LN_EPS)


def stage_block(residual, layer_weights):
    w_up, w_down = layer_weights
    normed = layer_norm(residual.astype(jnp.float32)).astype(jnp.bfloat16)
    pre_act = jnp.dot(normed, w_up.astype(jnp.bfloat16), preferred_element_type=jnp.float32)
    activated = jax.nn.gelu(pre_act, approximate=True).astype(jnp.bfloat16)
    block_out = jnp.dot(activated, w_down.astype(jnp.bfloat16), preferred_element_type=jnp.float32)
    return (residual.astype(jnp.float32) + block_out).astype(jnp.bfloat16), None


def model_logits(params, images):
    up_one, down_one, merge_proj, up_two, down_two, head_proj = params
    img_count = images.shape[0]
    residual = images.reshape(img_count * TOKENS, WIDTH)
    residual = lax.scan(stage_block, residual, (up_one, down_one))[0]
    merged = residual.reshape(img_count * MERGED, 4 * WIDTH)
    residual = jnp.dot(merged, merge_proj.astype(jnp.bfloat16), preferred_element_type=jnp.float32).astype(jnp.bfloat16)
    residual = lax.scan(stage_block, residual, (up_two, down_two))[0]
    pooled = jnp.mean(residual.reshape(img_count, MERGED, WIDTH_TWO).astype(jnp.float32), axis=1)
    normed = layer_norm(pooled).astype(jnp.bfloat16)
    return jnp.dot(normed, head_proj.astype(jnp.bfloat16), preferred_element_type=jnp.float32)


def shard_loss(params, images, labels):
    logits = model_logits(params, images)
    log_norm = jax.nn.logsumexp(logits, axis=-1)
    picked = jnp.sum(logits * jax.nn.one_hot(labels, CLASSES, dtype=jnp.float32), axis=-1)
    return jnp.sum(log_norm - picked) / BATCH


def lars_step(weight, velocity, grad_sum):
    red_axes = (weight.ndim - 2, weight.ndim - 1)
    w_norm = jnp.sqrt(jnp.sum(weight * weight, axis=red_axes, keepdims=True))
    g_norm = jnp.sqrt(jnp.sum(grad_sum * grad_sum, axis=red_axes, keepdims=True))
    new_vel = MOMENTUM * velocity + TRUST * (w_norm / g_norm) * grad_sum
    return weight - new_vel, new_vel


def reference(x_now, labels_now, x_next, up_one, down_one, merge_proj, up_two, down_two, head_proj, vel_up_one, vel_down_one, vel_merge_proj, vel_up_two, vel_down_two, vel_head_proj):
    params = (up_one, down_one, merge_proj, up_two, down_two, head_proj)
    grad_fn = jax.grad(shard_loss)

    def add_shard(running, shard_pair):
        grads = grad_fn(params, shard_pair[0], shard_pair[1])
        summed = jax.tree.map(lambda run_sum, shard_grad: run_sum + shard_grad.astype(jnp.bfloat16).astype(jnp.float32), running, grads)
        return summed, None

    zero_sums = jax.tree.map(jnp.zeros_like, params)
    img_shards = x_now.reshape(DATA_DEVS, IMAGES_DEV, TOKENS, WIDTH)
    label_shards = labels_now.reshape(DATA_DEVS, IMAGES_DEV)
    grad_sums = lax.scan(add_shard, zero_sums, (img_shards, label_shards))[0]
    new_up_one, new_vel_up_one = lars_step(up_one, vel_up_one, grad_sums[0])
    new_down_one, new_vel_down_one = lars_step(down_one, vel_down_one, grad_sums[1])
    new_merge_proj, new_vel_merge_proj = lars_step(merge_proj, vel_merge_proj, grad_sums[2])
    new_up_two, new_vel_up_two = lars_step(up_two, vel_up_two, grad_sums[3])
    new_down_two, new_vel_down_two = lars_step(down_two, vel_down_two, grad_sums[4])
    new_head_proj, new_vel_head_proj = lars_step(head_proj, vel_head_proj, grad_sums[5])
    new_params = (new_up_one, new_down_one, new_merge_proj, new_up_two, new_down_two, new_head_proj)
    next_shards = x_next.reshape(DATA_DEVS, IMAGES_DEV, TOKENS, WIDTH)
    logits_next = lax.map(lambda images: model_logits(new_params, images), next_shards).reshape(BATCH, CLASSES)
    return (logits_next, new_up_one, new_down_one, new_merge_proj, new_up_two, new_down_two, new_head_proj, new_vel_up_one, new_vel_down_one, new_vel_merge_proj, new_vel_up_two, new_vel_down_two, new_vel_head_proj)
```

```python
import jax
import jax.numpy as jnp
from jax import lax
from jax.experimental import pallas as pl
from jax.experimental.pallas import tpu as pltpu
from jax.sharding import PartitionSpec as P

MOMENTUM = 0.9
TRUST = 0.1
LN_EPS = 1e-6
GELU_A = 0.7978845608028654
GELU_B = 0.044715 * GELU_A
F32 = jnp.float32
BF16 = jnp.bfloat16
VMEM_BYTES = 62 * 1024 * 1024

IMGS, TOKENS, WIDTH = 4, 784, 128
MERGED = TOKENS // 4
ROWS = IMGS * MERGED
WIDE = 4 * WIDTH
HID_ONE, HID_TWO = 4 * WIDTH, 4 * WIDE
CLASSES = 1000
TILE = 256
N_TILES = HID_TWO // TILE
FWD_TILE = 512


def dot_nn(a, b):
    return lax.dot_general(a, b, (((1,), (0,)), ((), ())), preferred_element_type=F32)


def dot_nt(a, b):
    return lax.dot_general(a, b, (((1,), (1,)), ((), ())), preferred_element_type=F32)


def dot_tn(a, b):
    return lax.dot_general(a, b, (((0,), (0,)), ((), ())), preferred_element_type=F32)


def norm_parts(vals):
    centered = vals - jnp.mean(vals, axis=-1, keepdims=True)
    variance = jnp.mean(centered * centered, axis=-1, keepdims=True)
    rstd = lax.rsqrt(variance + LN_EPS)
    return centered * rstd, rstd


def norm_back(grad, normed, rstd):
    mean_g = jnp.mean(grad, axis=-1, keepdims=True)
    mean_gn = jnp.mean(grad * normed, axis=-1, keepdims=True)
    return rstd * (grad - mean_g - normed * mean_gn)


def gelu_parts(pre):
    square = pre * pre
    half = 0.5 * jnp.tanh(pre * (GELU_A + GELU_B * square)) + 0.5
    return square, half


def gelu_slope(pre, square, half):
    return half * (1.0 + pre * (1.0 - half) * (2.0 * GELU_A + 6.0 * GELU_B * square))


def cast_rows(dst, src, rows, step):
    def body(i, carry):
        sl = pl.ds(pl.multiple_of(i * step, step), step)
        dst[sl, :] = src[sl, :].astype(BF16)
        return carry
    lax.fori_loop(0, rows // step, body, 0)


def lanes(index, size):
    return pl.ds(pl.multiple_of(index * size, size), size)


def permute_tokens(x_ref, x_f32, r0):
    x_f32[...] = x_ref[...].astype(F32)
    for j in range(4):
        r0[:, j * WIDTH:(j + 1) * WIDTH] = x_f32[pl.ds(j, ROWS, stride=4), :].astype(BF16)


def stage_one_block(resid, w_up, w_down):
    res_f = resid.astype(F32)
    normed = norm_parts(res_f)[0].astype(BF16)
    pre = dot_nn(normed, w_up)
    act = (pre * gelu_parts(pre)[1]).astype(BF16)
    return (res_f + dot_nn(act, w_down)).astype(BF16)


def stage_one_forward(r0, r1, r2, up_one, down_one):
    def body(j, carry):
        sl = lanes(j, WIDTH)
        mid = stage_one_block(r0[:, sl], up_one[0], down_one[0])
        r1[:, sl] = mid
        r2[:, sl] = stage_one_block(mid, up_one[1], down_one[1])
        return carry
    lax.fori_loop(0, 4, body, 0)


def stage_two_block(src, dst, normed_ref, acc, up_ref, down_ref):
    res_f = src[...].astype(F32)
    normed_ref[...] = norm_parts(res_f)[0].astype(BF16)
    acc[...] = res_f

    def body(t, carry):
        sl = lanes(t, FWD_TILE)
        pre = dot_nn(normed_ref[...], up_ref[:, sl])
        act = (pre * gelu_parts(pre)[1]).astype(BF16)
        acc[...] += dot_nn(act, down_ref[sl, :])
        return carry
    lax.fori_loop(0, HID_TWO // FWD_TILE, body, 0)
    dst[...] = acc[...].astype(BF16)


def image_rows():
    image = lax.broadcasted_iota(jnp.int32, (8, ROWS), 0)
    row = lax.broadcasted_iota(jnp.int32, (8, ROWS), 1)
    inside = (row >= image * MERGED) & (row < (image + 1) * MERGED)
    return jnp.where(inside, 1.0, 0.0).astype(BF16)


def pooled_norm(resid):
    pooled = dot_nn(image_rows(), resid) * (1.0 / MERGED)
    return norm_parts(pooled)


def train_kernel(x_hbm, labels_ref, up1_hbm, dn1_hbm, mg_hbm, up2_hbm, dn2_hbm, hd_hbm,
                 g_up1, g_dn1, g_mg, g_up2, g_dn2, g_hd,
                 x_v, x_f32, st_up1, st_dn1, st_mg, st_up2, st_dn2, st_hd,
                 up1, dn1, mg, up2, dn2, hd,
                 r0, r1, r2, s0, s1, s2, normed_ref, acc, grad_a, grad_b, sems,
                 du1, dv1):
    copies = [pltpu.make_async_copy(src, dst, sems.at[i]) for i, (src, dst) in enumerate((
        (x_hbm, x_v), (up1_hbm, st_up1), (dn1_hbm, st_dn1), (mg_hbm, st_mg),
        (up2_hbm.at[0], st_up2.at[0]), (dn2_hbm.at[0], st_dn2.at[0]),
        (up2_hbm.at[1], st_up2.at[1]), (dn2_hbm.at[1], st_dn2.at[1]), (hd_hbm, st_hd)))]
    for copy in copies:
        copy.start()
    copies[0].wait()
    permute_tokens(x_v, x_f32, r0)
    copies[1].wait()
    copies[2].wait()
    for n in range(2):
        cast_rows(up1.at[n], st_up1.at[n], 128, 64)
        cast_rows(dn1.at[n], st_dn1.at[n], 512, 256)
    stage_one_forward(r0, r1, r2, up1, dn1)
    copies[3].wait()
    cast_rows(mg, st_mg, 512, 64)
    s0[...] = dot_nn(r2[...], mg[...]).astype(BF16)
    for n, (src, dst) in enumerate(((s0, s1), (s1, s2))):
        copies[4 + 2 * n].wait()
        copies[5 + 2 * n].wait()
        cast_rows(up2.at[n], st_up2.at[n], 512, 16)
        cast_rows(dn2.at[n], st_dn2.at[n], 2048, 64)
        stage_two_block(src, dst, normed_ref, acc, up2.at[n], dn2.at[n])
    copies[8].wait()
    cast_rows(hd, st_hd, 512, 64)
    head_normed, head_rstd = pooled_norm(s2[...])
    head_b = head_normed.astype(BF16)
    logits = dot_nn(head_b, hd[...])
    top = jnp.max(logits, axis=-1, keepdims=True)
    expd = jnp.exp(logits - top)
    probs = expd / jnp.sum(expd, axis=-1, keepdims=True)
    class_id = lax.broadcasted_iota(jnp.int32, (8, CLASSES), 1)
    real_row = lax.broadcasted_iota(jnp.int32, (8, CLASSES), 0) < IMGS
    onehot = jnp.where(class_id == labels_ref[...], 1.0, 0.0)
    grad_logits = jnp.where(real_row, (probs - onehot) * (1.0 / 32.0), 0.0).astype(BF16)
    g_hd[...] = dot_tn(head_b, grad_logits).astype(BF16)
    grad_pooled = norm_back(dot_nt(grad_logits, hd[...]), head_normed, head_rstd) * (1.0 / MERGED)
    grad_a[...] = dot_tn(image_rows(), grad_pooled.astype(BF16)).astype(BF16)

    grads = (grad_a, grad_b)
    for step, n in enumerate((1, 0)):
        g_in, g_out = grads[step], grads[1 - step]
        src = (s0, s1)[n]
        normed_f, rstd = norm_parts(src[...].astype(F32))
        normed_ref[...] = normed_f.astype(BF16)

        acc[...] = jnp.zeros_like(acc)

        def body(t, carry, n=n, g_in=g_in):
            sl = lanes(t, TILE)
            pre = dot_nn(normed_ref[...], up2[n, :, sl])
            square, half = gelu_parts(pre)
            act = (pre * half).astype(BF16)
            grad_pre = (gelu_slope(pre, square, half) * dot_nt(g_in[...], dn2[n, sl, :])).astype(BF16)
            g_dn2[n, sl, :] = dot_tn(act, g_in[...]).astype(BF16)
            g_up2[n, :, sl] = dot_tn(normed_ref[...], grad_pre).astype(BF16)
            acc[...] += dot_nt(grad_pre, up2[n, :, sl])
            return carry
        lax.fori_loop(0, N_TILES, body, 0)
        normed_f, rstd = norm_parts(src[...].astype(F32))
        g_out[...] = (norm_back(acc[...], normed_f, rstd) + g_in[...].astype(F32)).astype(BF16)
    g_mg[...] = dot_tn(r2[...], grad_a[...]).astype(BF16)
    grad_b[...] = dot_nt(grad_a[...], mg[...]).astype(BF16)

    for n, src, g_in, g_out in ((1, r1, grad_b, grad_a), (0, r0, grad_a, grad_b)):
        du1[...] = jnp.zeros_like(du1)
        dv1[...] = jnp.zeros_like(dv1)

        def body(j, carry, n=n, src=src, g_in=g_in, g_out=g_out):
            sl = lanes(j, WIDTH)
            normed_f, rstd = norm_parts(src[:, sl].astype(F32))
            normed = normed_f.astype(BF16)
            grad = g_in[:, sl]
            pre = dot_nn(normed, up1[n])
            square, half = gelu_parts(pre)
            act = (pre * half).astype(BF16)
            grad_pre = (gelu_slope(pre, square, half) * dot_nt(grad, dn1[n])).astype(BF16)
            dv1[...] += dot_tn(grad, act)
            du1[...] += dot_tn(normed, grad_pre)
            if n:
                back = norm_back(dot_nt(grad_pre, up1[n]), normed_f, rstd)
                g_out[:, sl] = (back + grad.astype(F32)).astype(BF16)
            return carry
        lax.fori_loop(0, 4, body, 0)
        g_up1[n] = du1[...].astype(BF16)
        g_dn1[n] = dv1[...].T.astype(BF16)


def sum_rows(tile):
    rows, cols = tile.shape
    return jnp.sum(tile.reshape(rows // 8, 8, cols), axis=0)


def lars_matrix(w_ref, v_ref, g_ref, b_ref, step):
    rows, cols = w_ref.shape
    zero = jnp.zeros((8, cols), F32)

    def norms(i, carry):
        sl = pl.ds(pl.multiple_of(i * step, step), step)
        w = w_ref[sl, :]
        g = g_ref[sl, :].astype(F32)
        return carry[0] + sum_rows(w * w), carry[1] + sum_rows(g * g)
    w_acc, g_acc = lax.fori_loop(0, rows // step, norms, (zero, zero))
    w_norm = jnp.sqrt(jnp.sum(jnp.sum(w_acc, axis=0, keepdims=True), axis=1, keepdims=True))
    g_norm = jnp.sqrt(jnp.sum(jnp.sum(g_acc, axis=0, keepdims=True), axis=1, keepdims=True))
    scale = TRUST * (w_norm / g_norm)

    def update(i, carry):
        sl = pl.ds(pl.multiple_of(i * step, step), step)
        new_v = MOMENTUM * v_ref[sl, :] + scale * g_ref[sl, :].astype(F32)
        new_w = w_ref[sl, :] - new_v
        v_ref[sl, :] = new_v
        w_ref[sl, :] = new_w
        b_ref[sl, :] = new_w.astype(BF16)
        return carry
    lax.fori_loop(0, rows // step, update, 0)


def next_kernel(x_hbm, up1_hbm, dn1_hbm, mg_hbm, up2_hbm, dn2_hbm, hd_hbm,
                vup1_hbm, vdn1_hbm, vmg_hbm, vup2_hbm, vdn2_hbm, vhd_hbm,
                gup1_hbm, gdn1_hbm, gmg_hbm, gup2_hbm, gdn2_hbm, ghd_hbm,
                logits_ref, o_up1, o_dn1, o_mg, o_up2, o_dn2, o_hd, ov_up1, ov_dn1, ov_mg, ov_up2, ov_dn2, ov_hd,
                x_v, x_f32, wb_up1, wb_dn1, wb_mg, wb_up2, wb_dn2, wb_hd, vb_up1, vb_dn1, vb_mg, vb_up2, vb_dn2, vb_hd,
                gb_up1, gb_dn1, gb_mg, gb_up2, gb_dn2, gb_hd,
                up1, dn1, mg, up2, dn2, hd, r0, s0, s1, normed_ref, acc, sem_in, sem_out, sem_x):
    jobs = []
    for n in range(2):
        jobs.append((up1_hbm.at[n], vup1_hbm.at[n], gup1_hbm.at[n], o_up1.at[n], ov_up1.at[n],
                     wb_up1.at[n], vb_up1.at[n], gb_up1.at[n], up1.at[n], 64, None))
        jobs.append((dn1_hbm.at[n], vdn1_hbm.at[n], gdn1_hbm.at[n], o_dn1.at[n], ov_dn1.at[n],
                     wb_dn1.at[n], vb_dn1.at[n], gb_dn1.at[n], dn1.at[n], 128, None))
    jobs.append((mg_hbm, vmg_hbm, gmg_hbm, o_mg, ov_mg, wb_mg, vb_mg, gb_mg, mg, 64, None))
    for n in range(2):
        jobs.append((up2_hbm.at[n], vup2_hbm.at[n], gup2_hbm.at[n], o_up2.at[n], ov_up2.at[n],
                     wb_up2, vb_up2, gb_up2, up2, 16, 5 if n else None))
        jobs.append((dn2_hbm.at[n], vdn2_hbm.at[n], gdn2_hbm.at[n], o_dn2.at[n], ov_dn2.at[n],
                     wb_dn2, vb_dn2, gb_dn2, dn2, 64, 6 if n else None))
    jobs.append((hd_hbm, vhd_hbm, ghd_hbm, o_hd, ov_hd, wb_hd, vb_hd, gb_hd, hd, 32, None))

    def loads(k):
        w, v, g, _, _, wb, vb, gb, _, _, _ = jobs[k]
        return [pltpu.make_async_copy(src, dst, sem_in.at[k, i])
                for i, (src, dst) in enumerate(((w, wb), (v, vb), (g, gb)))]

    def stores(k):
        _, _, _, ow, ov, wb, vb, _, _, _, _ = jobs[k]
        return [pltpu.make_async_copy(src, dst, sem_out.at[k, i]) for i, (src, dst) in enumerate(((wb, ow), (vb, ov)))]

    def run(k):
        for copy in loads(k):
            copy.wait()
        _, _, _, _, _, wb, vb, gb, b, step, _ = jobs[k]
        lars_matrix(wb, vb, gb, b, step)
        for copy in stores(k):
            copy.start()

    x_copy = pltpu.make_async_copy(x_hbm, x_v, sem_x)
    x_copy.start()
    for k in (0, 1, 2, 3, 4, 5, 6, 9):
        for copy in loads(k):
            copy.start()

    def reload(k, old):
        for copy in stores(old):
            copy.wait()
        for copy in loads(k):
            copy.start()

    x_copy.wait()
    permute_tokens(x_v, x_f32, r0)
    for k in range(4):
        run(k)
    stage_one_forward(r0, s0, s1, up1, dn1)
    run(4)
    s0[...] = dot_nn(s1[...], mg[...]).astype(BF16)
    run(5)
    run(6)
    stage_two_block(s0, s1, normed_ref, acc, up2, dn2)
    reload(7, 5)
    reload(8, 6)
    run(9)
    run(7)
    run(8)
    stage_two_block(s1, s0, normed_ref, acc, up2, dn2)
    head_b = pooled_norm(s0[...])[0].astype(BF16)
    logits_ref[...] = dot_nn(head_b, hd[...])[:IMGS]
    for k in (0, 1, 2, 3, 4, 9, 7, 8):
        for copy in stores(k):
            copy.wait()


W_SHAPES = ((2, 128, 512), (2, 512, 128), (512, 512), (2, 512, 2048), (2, 2048, 512), (512, 1000))
BIG_SHAPES = W_SHAPES[:3] + ((512, 2048), (2048, 512), (512, 1000))


def vmem(shape, dtype):
    return pltpu.VMEM(shape, dtype)


ANY_SPEC = pl.BlockSpec(memory_space=pl.ANY)
VMEM_SPEC = pl.BlockSpec(memory_space=pltpu.VMEM)


def run_train(x_now, labels, params):
    act = lambda dt=BF16: vmem((ROWS, WIDE), dt)
    return pl.pallas_call(
        train_kernel,
        out_shape=[jax.ShapeDtypeStruct(shape, BF16) for shape in W_SHAPES],
        in_specs=[ANY_SPEC, VMEM_SPEC] + [ANY_SPEC] * 6,
        out_specs=[VMEM_SPEC] * 6,
        scratch_shapes=[vmem((ROWS * 4, WIDTH), BF16), vmem((ROWS * 4, WIDTH), F32)]
        + [vmem(shape, F32) for shape in W_SHAPES] + [vmem(shape, BF16) for shape in W_SHAPES]
        + [act()] * 7 + [act(F32), act(), act(), pltpu.SemaphoreType.DMA((9,)), vmem((128, 512), F32), vmem((128, 512), F32)],
        compiler_params=pltpu.CompilerParams(vmem_limit_bytes=VMEM_BYTES),
        cost_estimate=pl.CostEstimate(flops=30_000_000_000, bytes_accessed=40_000_000, transcendentals=0),
        name='train_part',
    )(x_now, labels, *params)


def run_next(x_next, params, velocities, grads):
    act = lambda dt=BF16: vmem((ROWS, WIDE), dt)
    outs = [jax.ShapeDtypeStruct((IMGS, CLASSES), F32)] + [jax.ShapeDtypeStruct(shape, F32) for shape in W_SHAPES] * 2
    return pl.pallas_call(
        next_kernel,
        out_shape=outs,
        in_specs=[ANY_SPEC] * 19,
        out_specs=[VMEM_SPEC] + [ANY_SPEC] * 12,
        scratch_shapes=[vmem((ROWS * 4, WIDTH), BF16), vmem((ROWS * 4, WIDTH), F32)]
        + [vmem(shape, F32) for shape in BIG_SHAPES] * 2 + [vmem(shape, BF16) for shape in BIG_SHAPES] * 2
        + [act()] * 4 + [act(F32), pltpu.SemaphoreType.DMA((10, 3)), pltpu.SemaphoreType.DMA((10, 2)), pltpu.SemaphoreType.DMA],
        compiler_params=pltpu.CompilerParams(vmem_limit_bytes=VMEM_BYTES),
        cost_estimate=pl.CostEstimate(flops=10_000_000_000, bytes_accessed=100_000_000, transcendentals=0),
        name='next_part',
    )(x_next, *params, *velocities, *grads)


def solution(mesh):
    def local_step(x_now, labels_now, x_next, *weights):
        params, velocities = weights[:6], weights[6:]
        labels = jnp.pad(labels_now, (0, 8 - IMGS)).reshape(8, 1)
        grads = run_train(x_now.reshape(ROWS * 4, WIDTH), labels, params)
        sums = lax.psum(tuple(grads), 'data')
        return tuple(run_next(x_next.reshape(ROWS * 4, WIDTH), params, velocities, sums))

    split = P('data')
    in_specs = (split, split, split) + (P(),) * 12
    out_specs = (split,) + (P(),) * 12
    return jax.shard_map(local_step, mesh=mesh, in_specs=in_specs, out_specs=out_specs, check_vma=False)
```

```python
import jax
import jax.numpy as jnp
from jax import lax
from jax.experimental import pallas as pl
from jax.experimental.pallas import tpu as pltpu
from jax.sharding import PartitionSpec as P

MOMENTUM = 0.9
TRUST = 0.1
LN_EPS = 1e-6
GELU_A = 0.7978845608028654
GELU_B = 0.044715 * GELU_A
F32 = jnp.float32
BF16 = jnp.bfloat16
VMEM_BYTES = 62 * 1024 * 1024

IMGS, TOKENS, WIDTH = 4, 784, 128
MERGED = TOKENS // 4
ROWS = IMGS * MERGED
WIDE = 4 * WIDTH
HID_ONE, HID_TWO = 4 * WIDTH, 4 * WIDE
CLASSES = 1000
TILE = 256
SHARD = 64
N_TILES = HID_TWO // TILE
FWD_TILE = 512


def dot_nn(a, b):
    return lax.dot_general(a, b, (((1,), (0,)), ((), ())), preferred_element_type=F32)


def dot_nt(a, b):
    return lax.dot_general(a, b, (((1,), (1,)), ((), ())), preferred_element_type=F32)


def dot_tn(a, b):
    return lax.dot_general(a, b, (((0,), (0,)), ((), ())), preferred_element_type=F32)


def norm_parts(vals):
    centered = vals - jnp.mean(vals, axis=-1, keepdims=True)
    variance = jnp.mean(centered * centered, axis=-1, keepdims=True)
    rstd = lax.rsqrt(variance + LN_EPS)
    return centered * rstd, rstd


def norm_back(grad, normed, rstd):
    mean_g = jnp.mean(grad, axis=-1, keepdims=True)
    mean_gn = jnp.mean(grad * normed, axis=-1, keepdims=True)
    return rstd * (grad - mean_g - normed * mean_gn)


def gelu_parts(pre):
    square = pre * pre
    half = 0.5 * jnp.tanh(pre * (GELU_A + GELU_B * square)) + 0.5
    return square, half


def gelu_slope(pre, square, half):
    return half * (1.0 + pre * (1.0 - half) * (2.0 * GELU_A + 6.0 * GELU_B * square))


def cast_rows(dst, src, rows, step):
    def body(i, carry):
        sl = pl.ds(pl.multiple_of(i * step, step), step)
        dst[sl, :] = src[sl, :].astype(BF16)
        return carry
    lax.fori_loop(0, rows // step, body, 0)


def lanes(index, size):
    return pl.ds(pl.multiple_of(index * size, size), size)


def permute_tokens(x_ref, x_f32, r0):
    x_f32[...] = x_ref[...].astype(F32)
    for j in range(4):
        r0[:, j * WIDTH:(j + 1) * WIDTH] = x_f32[pl.ds(j, ROWS, stride=4), :].astype(BF16)


def stage_one_block(resid, w_up, w_down):
    res_f = resid.astype(F32)
    normed = norm_parts(res_f)[0].astype(BF16)
    pre = dot_nn(normed, w_up)
    act = (pre * gelu_parts(pre)[1]).astype(BF16)
    return (res_f + dot_nn(act, w_down)).astype(BF16)


def stage_one_forward(r0, r1, r2, up_one, down_one):
    def body(j, carry):
        sl = lanes(j, WIDTH)
        mid = stage_one_block(r0[:, sl], up_one[0], down_one[0])
        r1[:, sl] = mid
        r2[:, sl] = stage_one_block(mid, up_one[1], down_one[1])
        return carry
    lax.fori_loop(0, 4, body, 0)


def stage_two_block(src, dst, normed_ref, acc, up_ref, down_ref):
    res_f = src[...].astype(F32)
    normed_ref[...] = norm_parts(res_f)[0].astype(BF16)
    acc[...] = res_f

    def body(t, carry):
        sl = lanes(t, FWD_TILE)
        pre = dot_nn(normed_ref[...], up_ref[:, sl])
        act = (pre * gelu_parts(pre)[1]).astype(BF16)
        acc[...] += dot_nn(act, down_ref[sl, :])
        return carry
    lax.fori_loop(0, HID_TWO // FWD_TILE, body, 0)
    dst[...] = acc[...].astype(BF16)


def image_rows():
    image = lax.broadcasted_iota(jnp.int32, (8, ROWS), 0)
    row = lax.broadcasted_iota(jnp.int32, (8, ROWS), 1)
    inside = (row >= image * MERGED) & (row < (image + 1) * MERGED)
    return jnp.where(inside, 1.0, 0.0).astype(BF16)


def pooled_norm(resid):
    pooled = dot_nn(image_rows(), resid) * (1.0 / MERGED)
    return norm_parts(pooled)


UNIT = 1024
N_UNITS = 9
SHARE_ROWS = N_UNITS * UNIT
CLASS_PAD = 1024
DEVS = 8
SUBLANES = 8
LAST = N_UNITS - 1
PAIR_OUT, FIRST_OUT, SECOND_OUT, SECOND_BACK, FIRST_BACK, PAIR_BACK = range(6)


class Links:
    def __init__(self, own, final, land1, land2, sems):
        self.own, self.final, self.land1, self.land2, self.sems = own, final, land1, land2, sems
        me = lax.axis_index('data')
        self.me = me
        self.core, self.x, self.y = lax.rem(me, 2), lax.rem(me // 2, 2), me // 4
        self.pair = me + 1 - 2 * self.core
        self.x_peer = me + 2 - 4 * self.x
        self.y_peer = me + 4 - 8 * self.y

    def rows(self, unit, offset, size):
        return pl.ds(pl.multiple_of(unit * UNIT + offset, SHARD), size)

    def half(self, unit, offset, size):
        return self.rows(unit, self.core * WIDE + offset, size)

    def copy(self, unit, phase, lane, src, dst, peer):
        return pltpu.make_async_remote_copy(
            src_ref=src, dst_ref=dst, send_sem=self.sems.at[unit, phase, lane, 0], recv_sem=self.sems.at[unit, phase, lane, 1],
            device_id=(peer,), device_id_type=pl.DeviceIdType.MESH)

    def copies(self, unit, phase):
        x, y = self.x, self.y
        own, final = self.own, self.final
        if phase == PAIR_OUT:
            sl = self.rows(unit, (1 - self.core) * WIDE, WIDE)
            return [self.copy(unit, PAIR_OUT, 0, own.at[sl], final.at[sl], self.pair)]
        if phase == FIRST_OUT:
            land = lambda k: self.land1.at[pl.ds(pl.multiple_of(unit * TILE + k * WIDTH, WIDTH), WIDTH)]
            return [self.copy(unit, FIRST_OUT, 0, own.at[self.half(unit, (1 - x) * WIDTH, WIDTH)], land(0), self.x_peer),
                    self.copy(unit, FIRST_OUT, 1, own.at[self.half(unit, TILE + (1 - y) * WIDTH, WIDTH)], land(1), self.y_peer)]
        if phase == SECOND_OUT:
            land = lambda k: self.land2.at[pl.ds(pl.multiple_of(unit * WIDTH + k * SHARD, SHARD), SHARD)]
            return [self.copy(unit, SECOND_OUT, 0, own.at[self.half(unit, x * WIDTH + (1 - y) * SHARD, SHARD)], land(0), self.y_peer),
                    self.copy(unit, SECOND_OUT, 1, own.at[self.half(unit, TILE + y * WIDTH + (1 - x) * SHARD, SHARD)], land(1), self.x_peer)]
        if phase == SECOND_BACK:
            first = self.half(unit, x * WIDTH + y * SHARD, SHARD)
            second = self.half(unit, TILE + y * WIDTH + x * SHARD, SHARD)
            return [self.copy(unit, SECOND_BACK, 0, final.at[first], final.at[first], self.y_peer),
                    self.copy(unit, SECOND_BACK, 1, final.at[second], final.at[second], self.x_peer)]
        if phase == FIRST_BACK:
            first, second = self.half(unit, x * WIDTH, WIDTH), self.half(unit, TILE + y * WIDTH, WIDTH)
            return [self.copy(unit, FIRST_BACK, 0, final.at[first], final.at[first], self.x_peer),
                    self.copy(unit, FIRST_BACK, 1, final.at[second], final.at[second], self.y_peer)]
        sl = self.half(unit, 0, WIDE)
        return [self.copy(unit, PAIR_BACK, 0, final.at[sl], final.at[sl], self.pair)]

    def start(self, unit, phase):
        for copy in self.copies(unit, phase):
            copy.start()

    def wait(self, unit, phase):
        for copy in self.copies(unit, phase):
            copy.wait()

    def reduce_pair(self, unit):
        self.wait(unit, PAIR_OUT)
        x, y = self.x, self.y
        for offset in ((1 - x) * WIDTH, TILE + (1 - y) * WIDTH, x * WIDTH, TILE + y * WIDTH):
            sl = self.half(unit, offset, WIDTH)
            self.own[sl, :] = self.own[sl, :] + self.final[sl, :]
        self.start(unit, FIRST_OUT)

    def reduce_first(self, unit):
        self.wait(unit, FIRST_OUT)
        x, y = self.x, self.y
        for keep in (False, True):
            for lane, base, here, there in ((0, x * WIDTH, y, 0), (1, TILE + y * WIDTH, x, WIDTH)):
                part = here if keep else 1 - here
                sl = self.half(unit, base + part * SHARD, SHARD)
                land = pl.ds(pl.multiple_of(unit * TILE + there + part * SHARD, SHARD), SHARD)
                self.own[sl, :] = self.own[sl, :] + self.land1[land, :]
        self.start(unit, SECOND_OUT)

    def reduce_second(self, unit):
        self.wait(unit, SECOND_OUT)
        for lane, offset in ((0, self.x * WIDTH + self.y * SHARD), (1, TILE + self.y * WIDTH + self.x * SHARD)):
            sl = self.half(unit, offset, SHARD)
            land = pl.ds(pl.multiple_of(unit * WIDTH + lane * SHARD, SHARD), SHARD)
            self.final[sl, :] = self.own[sl, :] + self.land2[land, :]

    def forward(self, unit, phase):
        self.wait(unit, phase)
        self.start(unit, phase + 1)


def train_kernel(x_hbm, labels_ref, up1_hbm, dn1_hbm, mg_hbm, up2_hbm, dn2_hbm, hd_hbm,
                 sums_hbm, g_hd,
                 x_v, x_f32, st_up1, st_dn1, st_mg, st_up2, st_dn2,
                 up1, dn1, mg, up2, dn2, hd,
                 r0, r1, r2, s0, s1, normed_ref, acc, grad_a, grad_b, sems,
                 du1, dv1, own, final, land1, land2, factors, link_sems, factor_sems, out_sems):
    links = Links(own, final, land1, land2, link_sems)
    me = links.me
    st_hd = st_dn2.at[pl.ds(0, CLASSES)]
    copies = [pltpu.make_async_copy(src, dst, sems.at[i]) for i, (src, dst) in enumerate((
        (x_hbm, x_v), (up1_hbm, st_up1), (dn1_hbm, st_dn1), (mg_hbm, st_mg),
        (up2_hbm.at[0], st_up2), (dn2_hbm.at[0], st_dn2),
        (up2_hbm.at[1], st_up2), (dn2_hbm.at[1], st_dn2), (hd_hbm, st_hd)))]
    for i in range(6):
        copies[i].start()
    barrier = pltpu.get_barrier_semaphore()
    for k in range(1, DEVS):
        pl.semaphore_signal(barrier, inc=1, device_id=(lax.rem(me + k, DEVS),), device_id_type=pl.DeviceIdType.MESH)
    copies[0].wait()
    permute_tokens(x_v, x_f32, r0)
    copies[1].wait()
    copies[2].wait()
    for n in range(2):
        cast_rows(up1.at[n], st_up1.at[n], WIDTH, SHARD)
        cast_rows(dn1.at[n], st_dn1.at[n], WIDE, TILE)
    stage_one_forward(r0, r1, r2, up1, dn1)
    copies[3].wait()
    cast_rows(mg, st_mg, WIDE, SHARD)
    s0[...] = dot_nn(r2[...], mg[...]).astype(BF16)
    s2 = grad_a
    for n, (src, dst) in enumerate(((s0, s1), (s1, s2))):
        copies[4 + 2 * n].wait()
        cast_rows(up2.at[n], st_up2, WIDE, 16)
        if n == 0:
            copies[6].start()
        copies[5 + 2 * n].wait()
        cast_rows(dn2.at[n], st_dn2, 2048, SHARD)
        copies[7 + n].start()
        stage_two_block(src, dst, normed_ref, acc, up2.at[n], dn2.at[n])
    copies[8].wait()
    cast_rows(hd, st_hd, 992, 32)
    hd[992:CLASSES, :] = st_hd[992:CLASSES, :].astype(BF16)
    hd[CLASSES:, :] = jnp.zeros((CLASS_PAD - CLASSES, WIDE), BF16)
    head_normed, head_rstd = pooled_norm(s2[...])
    head_b = head_normed.astype(BF16)
    class_id = lax.broadcasted_iota(jnp.int32, (SUBLANES, CLASS_PAD), 1)
    real_row = lax.broadcasted_iota(jnp.int32, (SUBLANES, CLASS_PAD), 0) < IMGS
    logits = jnp.where(class_id < CLASSES, dot_nt(head_b, hd[...]), -jnp.inf)
    top = jnp.max(logits, axis=-1, keepdims=True)
    expd = jnp.exp(logits - top)
    probs = expd / jnp.sum(expd, axis=-1, keepdims=True)
    onehot = jnp.where(class_id == labels_ref[...], 1.0, 0.0)
    grad_logits = jnp.where(real_row, (probs - onehot) * (1.0 / (IMGS * DEVS)), 0.0).astype(BF16)
    factors[me, :, :WIDE] = head_b
    factors[me, :, WIDE:] = grad_logits
    grad_pooled = norm_back(dot_nn(grad_logits, hd[...]), head_normed, head_rstd) * (1.0 / MERGED)
    grad_a[...] = dot_tn(image_rows(), grad_pooled.astype(BF16)).astype(BF16)

    pl.semaphore_wait(barrier, DEVS - 1)

    def factor_copy(k):
        return pltpu.make_async_remote_copy(
            src_ref=factors.at[me], dst_ref=factors.at[me], send_sem=factor_sems.at[k, 0], recv_sem=factor_sems.at[k, 1],
            device_id=(lax.rem(me + k, DEVS),), device_id_type=pl.DeviceIdType.MESH)

    grads = (grad_a, grad_b)
    for step, n in enumerate((1, 0)):
        g_in, g_out = grads[step], grads[1 - step]
        src = (s0, s1)[n]
        normed_ref[...] = norm_parts(src[...].astype(F32))[0].astype(BF16)
        acc[...] = jnp.zeros_like(acc)

        def tile(t, row, n=n, g_in=g_in):
            sl = lanes(t, TILE)
            pre = dot_nn(normed_ref[...], up2[n, :, sl])
            square, half = gelu_parts(pre)
            act = (pre * half).astype(BF16)
            grad_pre = (gelu_slope(pre, square, half) * dot_nt(g_in[...], dn2[n, sl, :])).astype(BF16)
            own[pl.ds(row + TILE, TILE), :] = dot_tn(act, g_in[...]).astype(BF16)
            grad_up = dot_tn(normed_ref[...], grad_pre).astype(BF16)
            own[pl.ds(row, TILE), :TILE] = grad_up[:TILE]
            own[pl.ds(row, TILE), TILE:] = grad_up[TILE:]
            acc[...] += dot_nt(grad_pre, up2[n, :, sl])

        def body(p, carry, step=step, tile=tile):
            unit = step * 4 + p
            row = pl.multiple_of(unit * UNIT, UNIT)

            def guarded(lag, action):
                if step:
                    action(unit - lag)
                else:
                    @pl.when(p >= lag)
                    def _():
                        action(unit - lag)

            tile(2 * p, row)
            guarded(1, links.reduce_pair)
            tile(2 * p + 1, row + WIDE)
            guarded(3, links.reduce_second)
            guarded(2, links.reduce_first)
            links.start(unit, PAIR_OUT)
            return carry
        if step == 0:
            for k in range(1, DEVS):
                factor_copy(k).start()
        lax.fori_loop(0, N_TILES // 2, body, 0)
        normed_f, rstd = norm_parts(src[...].astype(F32))
        g_out[...] = (norm_back(acc[...], normed_f, rstd) + g_in[...].astype(F32)).astype(BF16)
    own[LAST * UNIT:LAST * UNIT + WIDE, :] = dot_tn(r2[...], grad_a[...]).astype(BF16)
    grad_b[...] = dot_nt(grad_a[...], mg[...]).astype(BF16)

    links.reduce_pair(7)
    for unit in range(5):
        links.start(unit, SECOND_BACK)

    def in_layer_one():
        links.reduce_second(5)
        links.reduce_first(6)
        links.start(5, SECOND_BACK)

    def in_layer_zero():
        links.reduce_second(6)
        links.reduce_first(7)
        links.start(6, SECOND_BACK)

    for n, src, g_in, g_out, between in ((1, r1, grad_b, grad_a, in_layer_one), (0, r0, grad_a, grad_b, in_layer_zero)):
        du1[...] = jnp.zeros_like(du1)
        dv1[...] = jnp.zeros_like(dv1)

        def body(j, carry, n=n, src=src, g_in=g_in, g_out=g_out, between=between):
            sl = lanes(j, WIDTH)
            normed_f, rstd = norm_parts(src[:, sl].astype(F32))
            normed = normed_f.astype(BF16)
            grad = g_in[:, sl]
            pre = dot_nn(normed, up1[n])
            square, half = gelu_parts(pre)
            act = (pre * half).astype(BF16)
            grad_pre = (gelu_slope(pre, square, half) * dot_nt(grad, dn1[n])).astype(BF16)
            dv1[...] += dot_tn(grad, act)
            du1[...] += dot_tn(normed, grad_pre)
            if n:
                back = norm_back(dot_nt(grad_pre, up1[n]), normed_f, rstd)
                g_out[:, sl] = (back + grad.astype(F32)).astype(BF16)
            pl.when(j == 1)(between)
            return carry
        lax.fori_loop(0, 4, body, 0)
        base = LAST * UNIT + WIDE + n * WIDTH
        own[base:base + WIDTH, :] = du1[...].astype(BF16)
        own[base + TILE:base + TILE + WIDTH, :] = dv1[...].astype(BF16)
        for unit in (range(2) if n else range(2, 4)):
            links.forward(unit, SECOND_BACK)
    links.start(LAST, PAIR_OUT)

    for k in range(1, DEVS):
        factor_copy(k).wait()

    def head_tile(c, carry):
        sl = pl.ds(pl.multiple_of(WIDE + c * WIDTH, WIDTH), WIDTH)
        total = jnp.zeros((WIDTH, WIDE), F32)
        for d in range(DEVS):
            total += dot_tn(factors[d, :, sl], factors[d, :, :WIDE]).astype(BF16).astype(F32)
        g_hd[pl.ds(pl.multiple_of(c * WIDTH, WIDTH), WIDTH), :] = total.astype(BF16)
        return carry
    lax.fori_loop(0, CLASS_PAD // WIDTH, head_tile, 0)

    def out_copy(unit):
        sl = pl.ds(unit * UNIT, UNIT)
        return pltpu.make_async_copy(final.at[sl], sums_hbm.at[sl], out_sems.at[unit])

    def finish(unit):
        links.wait(unit, PAIR_BACK)
        out_copy(unit).start()

    links.reduce_pair(LAST)
    links.reduce_second(7)
    links.forward(4, SECOND_BACK)
    links.forward(5, SECOND_BACK)
    links.start(7, SECOND_BACK)
    links.reduce_first(LAST)
    for unit in range(4):
        links.forward(unit, FIRST_BACK)
    links.forward(6, SECOND_BACK)
    links.reduce_second(LAST)
    links.forward(7, SECOND_BACK)
    links.start(LAST, SECOND_BACK)
    for unit in range(4, 6):
        links.forward(unit, FIRST_BACK)
    for unit in range(4):
        finish(unit)
    links.forward(6, FIRST_BACK)
    links.forward(LAST, SECOND_BACK)
    links.forward(7, FIRST_BACK)
    links.forward(LAST, FIRST_BACK)
    for unit in range(4, N_UNITS):
        finish(unit)
    for unit in range(N_UNITS):
        out_copy(unit).wait()


def sum_rows(tile):
    rows, cols = tile.shape
    return jnp.sum(tile.reshape(rows // 8, 8, cols), axis=0)


def lars_matrix(steps, piece, cols, tails=()):
    zero = jnp.zeros((8, cols), F32)

    def norms(i, carry):
        w, _, g, _ = piece(i)
        w, g = w[...], g[...].astype(F32)
        return carry[0] + sum_rows(w * w), carry[1] + sum_rows(g * g)
    w_acc, g_acc = lax.fori_loop(0, steps, norms, (zero, zero))
    for w, _, g, _ in tails:
        w, g = w[...], g[...].astype(F32)
        w_acc, g_acc = w_acc + sum_rows(w * w), g_acc + sum_rows(g * g)
    w_norm = jnp.sqrt(jnp.sum(jnp.sum(w_acc, axis=0, keepdims=True), axis=1, keepdims=True))
    g_norm = jnp.sqrt(jnp.sum(jnp.sum(g_acc, axis=0, keepdims=True), axis=1, keepdims=True))
    scale = TRUST * (w_norm / g_norm)

    def update_piece(w, v, g, b):
        new_v = MOMENTUM * v[...] + scale * g[...].astype(F32)
        new_w = w[...] - new_v
        v[...] = new_v
        w[...] = new_w
        b[...] = new_w.astype(BF16)

    def update(i, carry):
        update_piece(*piece(i))
        return carry
    lax.fori_loop(0, steps, update, 0)
    for tail in tails:
        update_piece(*tail)


def row_pieces(w, v, g, b, step):
    def piece(i):
        sl = pl.ds(pl.multiple_of(i * step, step), step)
        return w.at[sl], v.at[sl], g.at[sl], b.at[sl]
    return piece


def up_pieces(w, v, g, b):
    def piece(i):
        h, part = i // 2, lax.rem(i, 2)
        rows, cols = lanes(part, 256), lanes(h, 256)
        g_rows = pl.ds(pl.multiple_of(h * 512, 512), 256)
        return w.at[rows, cols], v.at[rows, cols], g.at[g_rows, rows], b.at[rows, cols]
    return piece


def down_pieces(w, v, g, b):
    def piece(i):
        h, part = i // 2, lax.rem(i, 2)
        rows = pl.ds(pl.multiple_of(i * 128, 128), 128)
        g_rows = pl.ds(pl.multiple_of(h * 512 + 256 + part * 128, 128), 128)
        return w.at[rows], v.at[rows], g.at[g_rows], b.at[rows]
    return piece


def next_kernel(x_hbm, up1_hbm, dn1_hbm, mg_hbm, up2_hbm, dn2_hbm, hd_hbm,
                vup1_hbm, vdn1_hbm, vmg_hbm, vup2_hbm, vdn2_hbm, vhd_hbm, sums_hbm, ghd_hbm,
                logits_ref, o_up1, o_dn1, o_mg, o_up2, o_dn2, o_hd, ov_up1, ov_dn1, ov_mg, ov_up2, ov_dn2, ov_hd,
                x_v, x_f32, wb_up1, wb_dn1, wb_mg, wb_up2, wb_dn2, wb_hd, vb_up1, vb_dn1, vb_mg, vb_up2, vb_dn2, vb_hd,
                gb_small, gb_turn, gb_two, gb_hd,
                up1, dn1, mg, up2, dn2, hd, r0, s0, s1, normed_ref, acc, sem_in, sem_out, sem_g):
    jobs = {}
    for n in range(2):
        jobs['up1', n] = (up1_hbm.at[n], vup1_hbm.at[n], o_up1.at[n], ov_up1.at[n], wb_up1.at[n], vb_up1.at[n])
        jobs['dn1', n] = (dn1_hbm.at[n], vdn1_hbm.at[n], o_dn1.at[n], ov_dn1.at[n], wb_dn1.at[n], vb_dn1.at[n])
        jobs['up2', n] = (up2_hbm.at[n], vup2_hbm.at[n], o_up2.at[n], ov_up2.at[n], wb_up2, vb_up2)
        jobs['dn2', n] = (dn2_hbm.at[n], vdn2_hbm.at[n], o_dn2.at[n], ov_dn2.at[n], wb_dn2, vb_dn2)
    jobs['mg', 0] = (mg_hbm, vmg_hbm, o_mg, ov_mg, wb_mg, vb_mg)
    jobs['hd', 0] = (hd_hbm, vhd_hbm, o_hd, ov_hd, wb_hd, vb_hd)
    order = {key: i for i, key in enumerate(jobs)}

    def loads(*key):
        w, v, _, _, wb, vb = jobs[key]
        return [pltpu.make_async_copy(w, wb, sem_in.at[order[key], 0]), pltpu.make_async_copy(v, vb, sem_in.at[order[key], 1])]

    def stores(*key):
        _, _, ow, ov, wb, vb = jobs[key]
        return [pltpu.make_async_copy(wb, ow, sem_out.at[order[key], 0]), pltpu.make_async_copy(vb, ov, sem_out.at[order[key], 1])]

    def each(copies, action):
        for copy in copies:
            getattr(copy, action)()

    small = pltpu.make_async_copy(sums_hbm.at[pl.ds(LAST * UNIT, UNIT)], gb_small, sem_g.at[0])
    two = [pltpu.make_async_copy(sums_hbm.at[pl.ds((1 - n) * 4 * UNIT, 4 * UNIT)], gb_two.at[n], sem_g.at[1 + n]) for n in range(2)]
    head = pltpu.make_async_copy(ghd_hbm, gb_hd, sem_g.at[3])
    x_copy = pltpu.make_async_copy(x_hbm, x_v, sem_g.at[4])
    x_copy.start()
    small.start()
    for key in (('up1', 0), ('dn1', 0), ('up1', 1), ('dn1', 1), ('mg', 0)):
        each(loads(*key), 'start')
    two[0].start()
    each(loads('up2', 0), 'start')
    each(loads('dn2', 0), 'start')
    two[1].start()
    head.start()
    each(loads('hd', 0), 'start')
    x_copy.wait()
    permute_tokens(x_v, x_f32, r0)
    small.wait()
    for n in range(2):
        each(loads('up1', n), 'wait')
        lars_matrix(2, row_pieces(wb_up1.at[n], vb_up1.at[n], gb_small.at[pl.ds(512 + n * 128, 128)], up1.at[n], 64), 512)
        each(stores('up1', n), 'start')
        each(loads('dn1', n), 'wait')
        gb_turn[...] = gb_small[pl.ds(768 + n * 128, 128), :].astype(F32).T
        lars_matrix(4, row_pieces(wb_dn1.at[n], vb_dn1.at[n], gb_turn, dn1.at[n], 128), 128)
        each(stores('dn1', n), 'start')
    stage_one_forward(r0, s0, s1, up1, dn1)
    each(loads('mg', 0), 'wait')
    lars_matrix(8, row_pieces(wb_mg, vb_mg, gb_small.at[pl.ds(0, 512)], mg, 64), 512)
    each(stores('mg', 0), 'start')
    s0[...] = dot_nn(s1[...], mg[...]).astype(BF16)

    def head_step():
        head.wait()
        each(loads('hd', 0), 'wait')
        tail = pl.ds(992, 8)
        lars_matrix(31, row_pieces(wb_hd, vb_hd, gb_hd, hd, 32), 512, [(wb_hd.at[tail], vb_hd.at[tail], gb_hd.at[tail], hd.at[tail])])
        each(stores('hd', 0), 'start')

    for n, (src, dst) in enumerate(((s0, s1), (s1, s0))):
        two[n].wait()
        each(loads('up2', n), 'wait')
        lars_matrix(16, up_pieces(wb_up2, vb_up2, gb_two.at[n], up2), 256)
        each(stores('up2', n), 'start')
        each(loads('dn2', n), 'wait')
        lars_matrix(16, down_pieces(wb_dn2, vb_dn2, gb_two.at[n], dn2), 512)
        each(stores('dn2', n), 'start')
        if n == 0:
            head_step()
            for name in ('up2', 'dn2'):
                each(stores(name, 0), 'wait')
                each(loads(name, 1), 'start')
        stage_two_block(src, dst, normed_ref, acc, up2, dn2)
    head_b = pooled_norm(s0[...])[0].astype(BF16)
    logits_ref[...] = dot_nt(head_b, hd[...])[:IMGS]
    for key in jobs:
        if key not in (('up2', 0), ('dn2', 0)):
            each(stores(*key), 'wait')


W_SHAPES = ((2, 128, 512), (2, 512, 128), (512, 512), (2, 512, 2048), (2, 2048, 512), (CLASSES, 512))
BUF_SHAPES = W_SHAPES[:3] + ((512, 2048), (2048, 512), (CLASSES, 512))


def vmem(shape, dtype):
    return pltpu.VMEM(shape, dtype)


ANY_SPEC = pl.BlockSpec(memory_space=pl.ANY)
VMEM_SPEC = pl.BlockSpec(memory_space=pltpu.VMEM)


def run_train(x_now, labels, params):
    act = lambda dt=BF16: vmem((ROWS, WIDE), dt)
    dma = pltpu.SemaphoreType.DMA
    return pl.pallas_call(
        train_kernel,
        out_shape=[jax.ShapeDtypeStruct((SHARE_ROWS, WIDE), BF16), jax.ShapeDtypeStruct((CLASS_PAD, WIDE), BF16)],
        in_specs=[ANY_SPEC, VMEM_SPEC] + [ANY_SPEC] * 6,
        out_specs=[ANY_SPEC, VMEM_SPEC],
        scratch_shapes=[vmem((ROWS * 4, WIDTH), BF16), vmem((ROWS * 4, WIDTH), F32)]
        + [vmem(shape, F32) for shape in BUF_SHAPES[:5]] + [vmem(shape, BF16) for shape in W_SHAPES[:5]] + [vmem((CLASS_PAD, WIDE), BF16)]
        + [act()] * 6 + [act(F32), act(), act(), dma((9,)), vmem((128, 512), F32), vmem((128, 512), F32)]
        + [vmem((SHARE_ROWS, WIDE), BF16), vmem((SHARE_ROWS, WIDE), BF16), vmem((N_UNITS * 256, WIDE), BF16), vmem((N_UNITS * 128, WIDE), BF16)]
        + [vmem((DEVS, 8, WIDE + CLASS_PAD), BF16), dma((N_UNITS, 6, 2, 2)), dma((DEVS, 2)), dma((N_UNITS,))],
        compiler_params=pltpu.CompilerParams(vmem_limit_bytes=66_000_000, collective_id=0, has_side_effects=True),
        cost_estimate=pl.CostEstimate(flops=30_000_000_000, bytes_accessed=40_000_000, transcendentals=0),
        name='train_part',
    )(x_now, labels, *params)


def run_next(x_next, params, velocities, sums, head_sum):
    act = lambda dt=BF16: vmem((ROWS, WIDE), dt)
    dma = pltpu.SemaphoreType.DMA
    outs = [jax.ShapeDtypeStruct((IMGS, CLASSES), F32)] + [jax.ShapeDtypeStruct(shape, F32) for shape in W_SHAPES] * 2
    return pl.pallas_call(
        next_kernel,
        out_shape=outs,
        in_specs=[ANY_SPEC] * 15,
        out_specs=[VMEM_SPEC] + [ANY_SPEC] * 12,
        scratch_shapes=[vmem((ROWS * 4, WIDTH), BF16), vmem((ROWS * 4, WIDTH), F32)]
        + [vmem(shape, F32) for shape in BUF_SHAPES] * 2
        + [vmem((UNIT, WIDE), BF16), vmem((512, 128), F32), vmem((2, 4 * UNIT, WIDE), BF16), vmem((CLASS_PAD, WIDE), BF16)]
        + [vmem(shape, BF16) for shape in BUF_SHAPES]
        + [act()] * 4 + [act(F32), dma((10, 2)), dma((10, 2)), dma((5,))],
        compiler_params=pltpu.CompilerParams(vmem_limit_bytes=VMEM_BYTES),
        cost_estimate=pl.CostEstimate(flops=10_000_000_000, bytes_accessed=100_000_000, transcendentals=0),
        name='next_part',
    )(x_next, *params, *velocities, sums, head_sum)


def turn_head(arrays):
    return tuple(arrays[:5]) + (arrays[5].T,)


def solution(mesh):
    def local_step(x_now, labels_now, x_next, *weights):
        params, velocities = turn_head(weights[:6]), turn_head(weights[6:])
        labels = jnp.pad(labels_now, (0, 8 - IMGS)).reshape(8, 1)
        sums, head_sum = run_train(x_now.reshape(ROWS * 4, WIDTH), labels, params)
        outs = run_next(x_next.reshape(ROWS * 4, WIDTH), params, velocities, sums, head_sum)
        return (outs[0],) + turn_head(outs[1:7]) + turn_head(outs[7:])

    split = P('data')
    in_specs = (split, split, split) + (P(),) * 12
    out_specs = (split,) + (P(),) * 12
    return jax.shard_map(local_step, mesh=mesh, in_specs=in_specs, out_specs=out_specs, check_vma=False)
```

```python
import jax
import jax.numpy as jnp
from jax import lax
from jax.experimental import pallas as pl
from jax.experimental.pallas import tpu as pltpu
from jax.sharding import PartitionSpec as P

MOMENTUM = 0.9
TRUST = 0.1
LN_EPS = 1e-6
GELU_A = 0.7978845608028654
GELU_B = 0.044715 * GELU_A
F32 = jnp.float32
BF16 = jnp.bfloat16
VMEM_BYTES = 62 * 1024 * 1024

IMGS, TOKENS, WIDTH = 4, 784, 128
MERGED = TOKENS // 4
ROWS = IMGS * MERGED
WIDE = 4 * WIDTH
HID_ONE, HID_TWO = 4 * WIDTH, 4 * WIDE
CLASSES = 1000
TILE = 256
SHARD = 64
N_TILES = HID_TWO // TILE
FWD_TILE = 512


def dot_nn(a, b):
    return lax.dot_general(a, b, (((1,), (0,)), ((), ())), preferred_element_type=F32)


def dot_nt(a, b):
    return lax.dot_general(a, b, (((1,), (1,)), ((), ())), preferred_element_type=F32)


def dot_tn(a, b):
    return lax.dot_general(a, b, (((0,), (0,)), ((), ())), preferred_element_type=F32)


def norm_parts(vals):
    centered = vals - jnp.mean(vals, axis=-1, keepdims=True)
    variance = jnp.mean(centered * centered, axis=-1, keepdims=True)
    rstd = lax.rsqrt(variance + LN_EPS)
    return centered * rstd, rstd


def norm_back(grad, normed, rstd):
    mean_g = jnp.mean(grad, axis=-1, keepdims=True)
    mean_gn = jnp.mean(grad * normed, axis=-1, keepdims=True)
    return rstd * (grad - mean_g - normed * mean_gn)


def gelu_parts(pre):
    square = pre * pre
    half = 0.5 * jnp.tanh(pre * (GELU_A + GELU_B * square)) + 0.5
    return square, half


def gelu_slope(pre, square, half):
    return half * (1.0 + pre * (1.0 - half) * (2.0 * GELU_A + 6.0 * GELU_B * square))


def cast_rows(dst, src, rows, step):
    def body(i, carry):
        sl = pl.ds(pl.multiple_of(i * step, step), step)
        dst[sl, :] = src[sl, :].astype(BF16)
        return carry
    lax.fori_loop(0, rows // step, body, 0)


def lanes(index, size):
    return pl.ds(pl.multiple_of(index * size, size), size)


def permute_tokens(x_ref, x_f32, r0):
    x_f32[...] = x_ref[...].astype(F32)
    for j in range(4):
        r0[:, j * WIDTH:(j + 1) * WIDTH] = x_f32[pl.ds(j, ROWS, stride=4), :].astype(BF16)


def stage_one_block(resid, w_up, w_down):
    res_f = resid.astype(F32)
    normed = norm_parts(res_f)[0].astype(BF16)
    pre = dot_nn(normed, w_up)
    act = (pre * gelu_parts(pre)[1]).astype(BF16)
    return (res_f + dot_nn(act, w_down)).astype(BF16)


def stage_one_forward(r0, r1, r2, up_one, down_one):
    def body(j, carry):
        sl = lanes(j, WIDTH)
        mid = stage_one_block(r0[:, sl], up_one[0], down_one[0])
        r1[:, sl] = mid
        r2[:, sl] = stage_one_block(mid, up_one[1], down_one[1])
        return carry
    lax.fori_loop(0, 4, body, 0)


def stage_two_block(src, dst, normed_ref, acc, up_ref, down_ref):
    res_f = src[...].astype(F32)
    normed_ref[...] = norm_parts(res_f)[0].astype(BF16)
    acc[...] = res_f

    def body(t, carry):
        sl = lanes(t, FWD_TILE)
        pre = dot_nn(normed_ref[...], up_ref[:, sl])
        act = (pre * gelu_parts(pre)[1]).astype(BF16)
        acc[...] += dot_nn(act, down_ref[sl, :])
        return carry
    lax.fori_loop(0, HID_TWO // FWD_TILE, body, 0)
    dst[...] = acc[...].astype(BF16)


def image_rows():
    image = lax.broadcasted_iota(jnp.int32, (8, ROWS), 0)
    row = lax.broadcasted_iota(jnp.int32, (8, ROWS), 1)
    inside = (row >= image * MERGED) & (row < (image + 1) * MERGED)
    return jnp.where(inside, 1.0, 0.0).astype(BF16)


def pooled_norm(resid):
    pooled = dot_nn(image_rows(), resid) * (1.0 / MERGED)
    return norm_parts(pooled)


UNIT = 1024
N_UNITS = 9
SHARE_ROWS = N_UNITS * UNIT
CLASS_PAD = 1024
DEVS = 8
SUBLANES = 8
LAST = N_UNITS - 1
HELD = 4
PAIR_OUT, FIRST_OUT, SECOND_OUT, SECOND_BACK, FIRST_BACK, PAIR_BACK = range(6)


class Links:
    def __init__(self, own, final, land1, land2, sems):
        self.own, self.final, self.land1, self.land2, self.sems = own, final, land1, land2, sems
        me = lax.axis_index('data')
        self.me = me
        self.core, self.x, self.y = lax.rem(me, 2), lax.rem(me // 2, 2), me // 4
        self.pair = me + 1 - 2 * self.core
        self.x_peer = me + 2 - 4 * self.x
        self.y_peer = me + 4 - 8 * self.y

    def rows(self, unit, offset, size):
        return pl.ds(pl.multiple_of(unit * UNIT + offset, SHARD), size)

    def half(self, unit, offset, size):
        return self.rows(unit, self.core * WIDE + offset, size)

    def copy(self, unit, phase, lane, src, dst, peer):
        return pltpu.make_async_remote_copy(
            src_ref=src, dst_ref=dst, send_sem=self.sems.at[unit, phase, lane, 0], recv_sem=self.sems.at[unit, phase, lane, 1],
            device_id=(peer,), device_id_type=pl.DeviceIdType.MESH)

    def copies(self, unit, phase):
        x, y = self.x, self.y
        own, final = self.own, self.final
        if phase == PAIR_OUT:
            sl = self.rows(unit, (1 - self.core) * WIDE, WIDE)
            return [self.copy(unit, PAIR_OUT, 0, own.at[sl], final.at[sl], self.pair)]
        if phase == FIRST_OUT:
            land = lambda k: self.land1.at[pl.ds(pl.multiple_of(unit * TILE + k * WIDTH, WIDTH), WIDTH)]
            return [self.copy(unit, FIRST_OUT, 0, own.at[self.half(unit, (1 - x) * WIDTH, WIDTH)], land(0), self.x_peer),
                    self.copy(unit, FIRST_OUT, 1, own.at[self.half(unit, TILE + (1 - y) * WIDTH, WIDTH)], land(1), self.y_peer)]
        if phase == SECOND_OUT:
            land = lambda k: self.land2.at[pl.ds(pl.multiple_of(unit * WIDTH + k * SHARD, SHARD), SHARD)]
            return [self.copy(unit, SECOND_OUT, 0, own.at[self.half(unit, x * WIDTH + (1 - y) * SHARD, SHARD)], land(0), self.y_peer),
                    self.copy(unit, SECOND_OUT, 1, own.at[self.half(unit, TILE + y * WIDTH + (1 - x) * SHARD, SHARD)], land(1), self.x_peer)]
        if phase == SECOND_BACK:
            first = self.half(unit, x * WIDTH + y * SHARD, SHARD)
            second = self.half(unit, TILE + y * WIDTH + x * SHARD, SHARD)
            return [self.copy(unit, SECOND_BACK, 0, final.at[first], final.at[first], self.y_peer),
                    self.copy(unit, SECOND_BACK, 1, final.at[second], final.at[second], self.x_peer)]
        if phase == FIRST_BACK:
            first, second = self.half(unit, x * WIDTH, WIDTH), self.half(unit, TILE + y * WIDTH, WIDTH)
            return [self.copy(unit, FIRST_BACK, 0, final.at[first], final.at[first], self.x_peer),
                    self.copy(unit, FIRST_BACK, 1, final.at[second], final.at[second], self.y_peer)]
        sl = self.half(unit, 0, WIDE)
        return [self.copy(unit, PAIR_BACK, 0, final.at[sl], final.at[sl], self.pair)]

    def start(self, unit, phase):
        for copy in self.copies(unit, phase):
            copy.start()

    def wait(self, unit, phase):
        for copy in self.copies(unit, phase):
            copy.wait()

    def reduce_pair(self, unit):
        self.wait(unit, PAIR_OUT)
        x, y = self.x, self.y
        for offset in ((1 - x) * WIDTH, TILE + (1 - y) * WIDTH, x * WIDTH, TILE + y * WIDTH):
            sl = self.half(unit, offset, WIDTH)
            self.own[sl, :] = self.own[sl, :] + self.final[sl, :]
        self.start(unit, FIRST_OUT)

    def reduce_first(self, unit):
        self.wait(unit, FIRST_OUT)
        x, y = self.x, self.y
        for keep in (False, True):
            for lane, base, here, there in ((0, x * WIDTH, y, 0), (1, TILE + y * WIDTH, x, WIDTH)):
                part = here if keep else 1 - here
                sl = self.half(unit, base + part * SHARD, SHARD)
                land = pl.ds(pl.multiple_of(unit * TILE + there + part * SHARD, SHARD), SHARD)
                self.own[sl, :] = self.own[sl, :] + self.land1[land, :]
        self.start(unit, SECOND_OUT)

    def reduce_second(self, unit):
        self.wait(unit, SECOND_OUT)
        for lane, offset in ((0, self.x * WIDTH + self.y * SHARD), (1, TILE + self.y * WIDTH + self.x * SHARD)):
            sl = self.half(unit, offset, SHARD)
            land = pl.ds(pl.multiple_of(unit * WIDTH + lane * SHARD, SHARD), SHARD)
            self.final[sl, :] = self.own[sl, :] + self.land2[land, :]

    def forward(self, unit, phase):
        self.wait(unit, phase)
        self.start(unit, phase + 1)


def train_kernel(x_hbm, labels_ref, up1_hbm, dn1_hbm, mg_hbm, up2_hbm, dn2_hbm, hd_hbm,
                 sums_hbm, first_hbm, second_hbm, head_hbm,
                 x_v, x_f32, st_up1, st_dn1, st_mg, st_up2, st_dn2,
                 up1, dn1, mg, up2, dn2, hd,
                 r0, r1, r2, s0, s1, normed_ref, acc, grad_a, grad_b, sems,
                 du1, dv1, own, final, land1, land2, factors, g_hd, link_sems, factor_sems, out_sems):
    links = Links(own, final, land1, land2, link_sems)
    me = links.me
    st_hd = st_dn2.at[pl.ds(0, CLASSES)]
    copies = [pltpu.make_async_copy(src, dst, sems.at[i]) for i, (src, dst) in enumerate((
        (x_hbm, x_v), (up1_hbm, st_up1), (dn1_hbm, st_dn1), (mg_hbm, st_mg),
        (up2_hbm.at[0], st_up2), (dn2_hbm.at[0], st_dn2),
        (up2_hbm.at[1], st_up2), (dn2_hbm.at[1], st_dn2), (hd_hbm, st_hd)))]
    for i in range(6):
        copies[i].start()
    barrier = pltpu.get_barrier_semaphore()
    for k in range(1, DEVS):
        pl.semaphore_signal(barrier, inc=1, device_id=(lax.rem(me + k, DEVS),), device_id_type=pl.DeviceIdType.MESH)
    copies[0].wait()
    permute_tokens(x_v, x_f32, r0)
    copies[1].wait()
    copies[2].wait()
    for n in range(2):
        cast_rows(up1.at[n], st_up1.at[n], WIDTH, SHARD)
        cast_rows(dn1.at[n], st_dn1.at[n], WIDE, TILE)
    stage_one_forward(r0, r1, r2, up1, dn1)
    copies[3].wait()
    cast_rows(mg, st_mg, WIDE, SHARD)
    s0[...] = dot_nn(r2[...], mg[...]).astype(BF16)
    s2 = grad_a
    for n, (src, dst) in enumerate(((s0, s1), (s1, s2))):
        copies[4 + 2 * n].wait()
        cast_rows(up2.at[n], st_up2, WIDE, 16)
        if n == 0:
            copies[6].start()
        copies[5 + 2 * n].wait()
        cast_rows(dn2.at[n], st_dn2, 2048, SHARD)
        copies[7 + n].start()
        stage_two_block(src, dst, normed_ref, acc, up2.at[n], dn2.at[n])
    copies[8].wait()
    cast_rows(hd, st_hd, 992, 32)
    hd[992:CLASSES, :] = st_hd[992:CLASSES, :].astype(BF16)
    hd[CLASSES:, :] = jnp.zeros((CLASS_PAD - CLASSES, WIDE), BF16)
    head_normed, head_rstd = pooled_norm(s2[...])
    head_b = head_normed.astype(BF16)
    class_id = lax.broadcasted_iota(jnp.int32, (SUBLANES, CLASS_PAD), 1)
    row_id = lax.broadcasted_iota(jnp.int32, (SUBLANES, CLASS_PAD), 0)
    logits = jnp.where(class_id < CLASSES, dot_nt(head_b, hd[...]), -jnp.inf)
    top = jnp.max(logits, axis=-1, keepdims=True)
    expd = jnp.exp(logits - top)
    probs = expd / jnp.sum(expd, axis=-1, keepdims=True)
    label = jnp.zeros((SUBLANES, CLASS_PAD), jnp.int32)
    for i in range(IMGS):
        label = jnp.where(row_id == i, labels_ref[i], label)
    onehot = jnp.where(class_id == label, 1.0, 0.0)
    grad_logits = jnp.where(row_id < IMGS, (probs - onehot) * (1.0 / (IMGS * DEVS)), 0.0).astype(BF16)
    factors[me, :, :WIDE] = head_b
    factors[me, :, WIDE:] = grad_logits
    grad_pooled = norm_back(dot_nn(grad_logits, hd[...]), head_normed, head_rstd) * (1.0 / MERGED)
    grad_a[...] = dot_tn(image_rows(), grad_pooled.astype(BF16)).astype(BF16)

    pl.semaphore_wait(barrier, DEVS - 1)

    def factor_copy(k):
        return pltpu.make_async_remote_copy(
            src_ref=factors.at[me], dst_ref=factors.at[me], send_sem=factor_sems.at[k, 0], recv_sem=factor_sems.at[k, 1],
            device_id=(lax.rem(me + k, DEVS),), device_id_type=pl.DeviceIdType.MESH)

    grads = (grad_a, grad_b)
    for step, n in enumerate((1, 0)):
        g_in, g_out = grads[step], grads[1 - step]
        src = (s0, s1)[n]
        normed_ref[...] = norm_parts(src[...].astype(F32))[0].astype(BF16)
        acc[...] = jnp.zeros_like(acc)

        def tile(t, row, n=n, g_in=g_in):
            sl = lanes(t, TILE)
            pre = dot_nn(normed_ref[...], up2[n, :, sl])
            square, half = gelu_parts(pre)
            act = (pre * half).astype(BF16)
            grad_pre = (gelu_slope(pre, square, half) * dot_nt(g_in[...], dn2[n, sl, :])).astype(BF16)
            own[pl.ds(row + TILE, TILE), :] = dot_tn(act, g_in[...]).astype(BF16)
            grad_up = dot_tn(normed_ref[...], grad_pre).astype(BF16)
            own[pl.ds(row, TILE), :TILE] = grad_up[:TILE]
            own[pl.ds(row, TILE), TILE:] = grad_up[TILE:]
            acc[...] += dot_nt(grad_pre, up2[n, :, sl])

        def body(p, carry, step=step, tile=tile):
            unit = step * 4 + p
            row = pl.multiple_of(unit * UNIT, UNIT)

            tile(2 * p, row)
            if step:
                links.reduce_pair(unit - 1)
            else:
                pl.when(p > 0)(lambda: links.reduce_pair(unit - 1))
            tile(2 * p + 1, row + WIDE)
            if step:
                links.reduce_first(unit - 4)
            links.start(unit, PAIR_OUT)
            return carry
        if step == 0:
            for k in range(1, DEVS):
                factor_copy(k).start()
        lax.fori_loop(0, N_TILES // 2, body, 0)
        normed_f, rstd = norm_parts(src[...].astype(F32))
        g_out[...] = (norm_back(acc[...], normed_f, rstd) + g_in[...].astype(F32)).astype(BF16)
    own[LAST * UNIT:LAST * UNIT + WIDE, :] = dot_tn(r2[...], grad_a[...]).astype(BF16)
    grad_b[...] = dot_nt(grad_a[...], mg[...]).astype(BF16)

    def first_copies(unit):
        sl = pl.ds(unit * WIDTH, WIDTH)
        return [pltpu.make_async_copy(final.at[links.half(unit, offset, WIDTH)], dst.at[sl], out_sems.at[unit, i])
                for i, (offset, dst) in enumerate(((links.x * WIDTH, first_hbm), (TILE + links.y * WIDTH, second_hbm)))]

    def out_copy(unit):
        rows = pl.ds((unit - HELD) * UNIT, UNIT)
        return [pltpu.make_async_copy(final.at[pl.ds(unit * UNIT, UNIT)], sums_hbm.at[rows], out_sems.at[unit, 0])]

    def reduced(unit):
        links.reduce_second(unit)
        links.start(unit, SECOND_BACK)

    def finish(unit):
        links.wait(unit, PAIR_BACK if unit >= HELD else SECOND_BACK)
        for copy in (out_copy(unit) if unit >= HELD else first_copies(unit)):
            copy.start()

    def back_first(unit):
        links.forward(unit, SECOND_BACK)

    def back_pair(unit):
        links.forward(unit, FIRST_BACK)

    def run_all(steps):
        for action, unit in steps:
            action(unit)

    links.reduce_pair(7)
    slots = {1: (((links.reduce_first, 4), (reduced, 0), (reduced, 1)), ((reduced, 2),), ((links.reduce_first, 5),), ((links.reduce_first, 6),)),
             0: (((reduced, 3),), ((reduced, 4),), ((finish, 0),), ((finish, 1),))}

    for n, src, g_in, g_out in ((1, r1, grad_b, grad_a), (0, r0, grad_a, grad_b)):
        du1[...] = jnp.zeros_like(du1)
        dv1[...] = jnp.zeros_like(dv1)

        def body(j, carry, n=n, src=src, g_in=g_in, g_out=g_out):
            sl = lanes(j, WIDTH)
            normed_f, rstd = norm_parts(src[:, sl].astype(F32))
            normed = normed_f.astype(BF16)
            grad = g_in[:, sl]
            pre = dot_nn(normed, up1[n])
            square, half = gelu_parts(pre)
            act = (pre * half).astype(BF16)
            grad_pre = (gelu_slope(pre, square, half) * dot_nt(grad, dn1[n])).astype(BF16)
            dv1[...] += dot_tn(grad, act)
            du1[...] += dot_tn(normed, grad_pre)
            if n:
                back = norm_back(dot_nt(grad_pre, up1[n]), normed_f, rstd)
                g_out[:, sl] = (back + grad.astype(F32)).astype(BF16)
            for k, steps in enumerate(slots[n]):
                pl.when(j == k)(lambda steps=steps: run_all(steps))
            return carry
        lax.fori_loop(0, 4, body, 0)
        base = LAST * UNIT + WIDE + n * WIDTH
        own[base:base + WIDTH, :] = du1[...].astype(BF16)
        own[base + TILE:base + TILE + WIDTH, :] = dv1[...].astype(BF16)
    links.start(LAST, PAIR_OUT)

    for k in range(1, DEVS):
        factor_copy(k).wait()

    def head_tile(c, carry):
        sl = pl.ds(pl.multiple_of(WIDE + c * WIDTH, WIDTH), WIDTH)
        total = jnp.zeros((WIDTH, WIDE), F32)
        for d in range(DEVS):
            total += dot_tn(factors[d, :, sl], factors[d, :, :WIDE]).astype(BF16).astype(F32)
        g_hd[pl.ds(pl.multiple_of(c * WIDTH, WIDTH), WIDTH), :] = total.astype(BF16)
        return carry
    half_tiles = CLASS_PAD // WIDTH // 2
    lax.fori_loop(0, half_tiles, head_tile, 0)
    run_all(((links.reduce_pair, LAST), (links.reduce_first, 7), (finish, 2)))
    lax.fori_loop(half_tiles, 2 * half_tiles, head_tile, 0)
    head_copy = pltpu.make_async_copy(g_hd, head_hbm, factor_sems.at[0, 0])
    head_copy.start()
    run_all(((reduced, 5), (reduced, 6), (finish, 3), (back_first, 4), (links.reduce_first, LAST), (reduced, 7), (back_first, 5),
             (back_first, 6), (back_pair, 4), (reduced, LAST), (finish, 4), (back_first, 7), (back_pair, 5), (back_pair, 6), (back_first, LAST),
             (finish, 5), (finish, 6), (back_pair, 7), (back_pair, LAST), (finish, 7), (finish, LAST)))
    for unit in range(N_UNITS):
        for copy in (out_copy(unit) if unit >= HELD else first_copies(unit)):
            copy.wait()
    head_copy.wait()


def sum_rows(tile):
    rows, cols = tile.shape
    return jnp.sum(tile.reshape(rows // 8, 8, cols), axis=0)


def lars_matrix(steps, piece, cols, tails=()):
    zero = jnp.zeros((8, cols), F32)

    def norms(i, carry):
        w, _, g, _ = piece(i)
        w, g = w[...], g[...].astype(F32)
        return carry[0] + sum_rows(w * w), carry[1] + sum_rows(g * g)
    w_acc, g_acc = lax.fori_loop(0, steps, norms, (zero, zero))
    for w, _, g, _ in tails:
        w, g = w[...], g[...].astype(F32)
        w_acc, g_acc = w_acc + sum_rows(w * w), g_acc + sum_rows(g * g)
    w_norm = jnp.sqrt(jnp.sum(jnp.sum(w_acc, axis=0, keepdims=True), axis=1, keepdims=True))
    g_norm = jnp.sqrt(jnp.sum(jnp.sum(g_acc, axis=0, keepdims=True), axis=1, keepdims=True))
    scale = TRUST * (w_norm / g_norm)

    def update_piece(w, v, g, b):
        new_v = MOMENTUM * v[...] + scale * g[...].astype(F32)
        new_w = w[...] - new_v
        v[...] = new_v
        w[...] = new_w
        b[...] = new_w.astype(BF16)

    def update(i, carry):
        update_piece(*piece(i))
        return carry
    lax.fori_loop(0, steps, update, 0)
    for tail in tails:
        update_piece(*tail)


def row_pieces(w, v, g, b, step):
    def piece(i):
        sl = pl.ds(pl.multiple_of(i * step, step), step)
        return w.at[sl], v.at[sl], g.at[sl], b.at[sl]
    return piece


def up_pieces(w, v, g, b):
    def piece(i):
        h, part = i // 2, lax.rem(i, 2)
        rows, cols = lanes(part, 256), lanes(h, 256)
        g_rows = pl.ds(pl.multiple_of(h * 512, 512), 256)
        return w.at[rows, cols], v.at[rows, cols], g.at[g_rows, rows], b.at[rows, cols]
    return piece


def down_pieces(w, v, g, b):
    def piece(i):
        h, part = i // 2, lax.rem(i, 2)
        rows = pl.ds(pl.multiple_of(i * 128, 128), 128)
        g_rows = pl.ds(pl.multiple_of(h * 512 + 256 + part * 128, 128), 128)
        return w.at[rows], v.at[rows], g.at[g_rows], b.at[rows]
    return piece


def start_all(copies):
    for copy in copies:
        copy.start()


def wait_all(copies):
    for copy in copies:
        copy.wait()


class Pair:
    def __init__(self, w, v, out_w, out_v, buf_w, buf_v, sems, slot):
        self.buf_w, self.buf_v = buf_w, buf_v
        ends = ((w, buf_w), (v, buf_v)), ((buf_w, out_w), (buf_v, out_v))
        self.loads, self.stores = ([pltpu.make_async_copy(src, dst, sems.at[slot, k, i]) for i, (src, dst) in enumerate(part)]
                                   for k, part in enumerate(ends))

    def update(self, steps, make, grad, cast, cols, *rest, tails=()):
        wait_all(self.loads)
        lars_matrix(steps, make(self.buf_w, self.buf_v, grad, cast, *rest), cols, tails)
        start_all(self.stores)


def early_kernel(x_hbm, up1_hbm, dn1_hbm, mg_hbm, up2_hbm, dn2_hbm, vup1_hbm, vdn1_hbm, vmg_hbm, vup2_hbm, vdn2_hbm, sums_hbm,
                 mid_ref, o_up1, o_dn1, o_mg, o_up2, o_dn2, ov_up1, ov_dn1, ov_mg, ov_up2, ov_dn2,
                 x_v, x_f32, wb_up1, wb_dn1, wb_mg, wb_up2, wb_dn2, vb_up1, vb_dn1, vb_mg, vb_up2, vb_dn2,
                 gb_small, gb_turn, gb_two, up1, dn1, mg, up2, dn2, r0, s0, s1, normed_ref, acc, sems, sem_g):
    ups = [Pair(up1_hbm.at[n], vup1_hbm.at[n], o_up1.at[n], ov_up1.at[n], wb_up1.at[n], vb_up1.at[n], sems, n) for n in range(2)]
    downs = [Pair(dn1_hbm.at[n], vdn1_hbm.at[n], o_dn1.at[n], ov_dn1.at[n], wb_dn1.at[n], vb_dn1.at[n], sems, 2 + n) for n in range(2)]
    merge = Pair(mg_hbm, vmg_hbm, o_mg, ov_mg, wb_mg, vb_mg, sems, 4)
    wide_up = Pair(up2_hbm.at[0], vup2_hbm.at[0], o_up2.at[0], ov_up2.at[0], wb_up2, vb_up2, sems, 5)
    wide_down = Pair(dn2_hbm.at[0], vdn2_hbm.at[0], o_dn2.at[0], ov_dn2.at[0], wb_dn2, vb_dn2, sems, 6)
    pairs = ups + downs + [merge, wide_up, wide_down]
    small = pltpu.make_async_copy(sums_hbm.at[pl.ds(HELD * UNIT, UNIT)], gb_small, sem_g.at[0])
    two = pltpu.make_async_copy(sums_hbm.at[pl.ds(0, HELD * UNIT)], gb_two, sem_g.at[1])
    x_copy = pltpu.make_async_copy(x_hbm, x_v, sem_g.at[2])
    x_copy.start()
    small.start()
    for pair in pairs[:5]:
        start_all(pair.loads)
    two.start()
    for pair in pairs[5:]:
        start_all(pair.loads)
    x_copy.wait()
    permute_tokens(x_v, x_f32, r0)
    small.wait()
    for n in range(2):
        ups[n].update(2, row_pieces, gb_small.at[pl.ds(WIDE + n * WIDTH, WIDTH)], up1.at[n], WIDE, SHARD)
        gb_turn[...] = gb_small[pl.ds(WIDE + TILE + n * WIDTH, WIDTH), :].astype(F32).T
        downs[n].update(4, row_pieces, gb_turn, dn1.at[n], WIDTH, WIDTH)
    merge.update(8, row_pieces, gb_small.at[pl.ds(0, WIDE)], mg, WIDE, SHARD)
    stage_one_forward(r0, s0, s1, up1, dn1)
    s0[...] = dot_nn(s1[...], mg[...]).astype(BF16)
    two.wait()
    wide_up.update(16, up_pieces, gb_two, up2, TILE)
    wide_down.update(16, down_pieces, gb_two, dn2, WIDE)
    stage_two_block(s0, mid_ref, normed_ref, acc, up2, dn2)
    for pair in pairs:
        wait_all(pair.stores)


def head_kernel(hd_hbm, vhd_hbm, ghd_hbm, hd, o_hd, ov_hd, wb_hd, vb_hd, gb_hd, sems, sem_g):
    pair = Pair(hd_hbm, vhd_hbm, o_hd, ov_hd, wb_hd, vb_hd, sems, 0)
    head = pltpu.make_async_copy(ghd_hbm, gb_hd, sem_g)
    head.start()
    start_all(pair.loads)
    head.wait()
    tail = pl.ds(992, SUBLANES)
    pair.update(31, row_pieces, gb_hd, hd, WIDE, 32, tails=[(wb_hd.at[tail], vb_hd.at[tail], gb_hd.at[tail], hd.at[tail])])
    wait_all(pair.stores)


def late_kernel(mid_hbm, hd_hbm, up2_hbm, dn2_hbm, vup2_hbm, vdn2_hbm,
                first, second, first_x, second_y, first_c, second_c, first_xc, second_yc, a_up2, a_dn2, a_vup2, a_vdn2,
                logits_ref, o_up2, o_dn2, ov_up2, ov_dn2,
                wb_up2, wb_dn2, vb_up2, vb_dn2, gb_two, up2, dn2, mid, hd, s0, normed_ref, acc, sems, sem_g, sem_m):
    me = lax.axis_index('data')
    core, x, y = lax.rem(me, 2), lax.rem(me // 2, 2), me // 4
    wide_up = Pair(up2_hbm.at[1], vup2_hbm.at[1], o_up2.at[1], ov_up2.at[1], wb_up2, vb_up2, sems, 0)
    wide_down = Pair(dn2_hbm.at[1], vdn2_hbm.at[1], o_dn2.at[1], ov_dn2.at[1], wb_dn2, vb_dn2, sems, 1)
    places = ((first, core, x * WIDTH), (second, core, TILE + y * WIDTH),
              (first_x, core, (1 - x) * WIDTH), (second_y, core, TILE + (1 - y) * WIDTH),
              (first_c, 1 - core, x * WIDTH), (second_c, 1 - core, TILE + y * WIDTH),
              (first_xc, 1 - core, (1 - x) * WIDTH), (second_yc, 1 - core, TILE + (1 - y) * WIDTH))
    pieces = []
    for k, (src, half, offset) in enumerate(places):
        for unit in range(HELD):
            rows = pl.ds(pl.multiple_of(unit * UNIT + half * WIDE + offset, WIDTH), WIDTH)
            pieces.append(pltpu.make_async_copy(src.at[pl.ds(unit * WIDTH, WIDTH)], gb_two.at[rows], sem_g.at[k, unit]))
    start_all(pieces)
    start_all(wide_up.loads)
    start_all(wide_down.loads)
    rest = [pltpu.make_async_copy(mid_hbm, mid, sem_m.at[0]), pltpu.make_async_copy(hd_hbm, hd, sem_m.at[1])]
    start_all(rest)
    wait_all(pieces)
    wide_up.update(16, up_pieces, gb_two, up2, TILE)
    wide_down.update(16, down_pieces, gb_two, dn2, WIDE)
    wait_all(rest)
    stage_two_block(mid, s0, normed_ref, acc, up2, dn2)
    head_b = pooled_norm(s0[...])[0].astype(BF16)
    logits_ref[...] = dot_nt(head_b, hd[...])[:IMGS]
    wait_all(wide_up.stores)
    wait_all(wide_down.stores)


W_SHAPES = ((2, 128, 512), (2, 512, 128), (512, 512), (2, 512, 2048), (2, 2048, 512), (CLASSES, 512))
BUF_SHAPES = W_SHAPES[:3] + ((512, 2048), (2048, 512), (CLASSES, 512))


def vmem(shape, dtype):
    return pltpu.VMEM(shape, dtype)


ANY_SPEC = pl.BlockSpec(memory_space=pl.ANY)
VMEM_SPEC = pl.BlockSpec(memory_space=pltpu.VMEM)


def act(dtype=BF16):
    return vmem((ROWS, WIDE), dtype)


def f32_outs(shapes):
    return [jax.ShapeDtypeStruct(shape, F32) for shape in shapes]


DMA = pltpu.SemaphoreType.DMA


def run_train(x_now, labels, params):
    return pl.pallas_call(
        train_kernel,
        out_shape=[jax.ShapeDtypeStruct((rows, WIDE), BF16) for rows in (SHARE_ROWS - HELD * UNIT, HELD * WIDTH, HELD * WIDTH, CLASS_PAD)],
        in_specs=[ANY_SPEC, pl.BlockSpec(memory_space=pltpu.SMEM)] + [ANY_SPEC] * 6,
        out_specs=[ANY_SPEC] * 4,
        scratch_shapes=[vmem((ROWS * 4, WIDTH), BF16), vmem((ROWS * 4, WIDTH), F32)]
        + [vmem(shape, F32) for shape in BUF_SHAPES[:5]] + [vmem(shape, BF16) for shape in W_SHAPES[:5]] + [vmem((CLASS_PAD, WIDE), BF16)]
        + [act()] * 6 + [act(F32), act(), act(), DMA((9,)), vmem((WIDTH, WIDE), F32), vmem((WIDTH, WIDE), F32)]
        + [vmem((rows, WIDE), BF16) for rows in (SHARE_ROWS, SHARE_ROWS, N_UNITS * TILE, N_UNITS * WIDTH)]
        + [vmem((DEVS, SUBLANES, WIDE + CLASS_PAD), BF16), vmem((CLASS_PAD, WIDE), BF16)]
        + [DMA((N_UNITS, 6, 2, 2)), DMA((DEVS, 2)), DMA((N_UNITS, 2))],
        compiler_params=pltpu.CompilerParams(vmem_limit_bytes=66_000_000, collective_id=0, has_side_effects=True),
        cost_estimate=pl.CostEstimate(flops=30_000_000_000, bytes_accessed=40_000_000, transcendentals=0),
        name='train_part',
    )(x_now, labels, *params)


def run_early(x_next, params, velocities, sums):
    return pl.pallas_call(
        early_kernel,
        out_shape=[jax.ShapeDtypeStruct((ROWS, WIDE), BF16)] + f32_outs(W_SHAPES[:5]) * 2,
        in_specs=[ANY_SPEC] * 12,
        out_specs=[VMEM_SPEC] + [ANY_SPEC] * 10,
        scratch_shapes=[vmem((ROWS * 4, WIDTH), BF16), vmem((ROWS * 4, WIDTH), F32)]
        + [vmem(shape, F32) for shape in BUF_SHAPES[:5]] * 2
        + [vmem((UNIT, WIDE), BF16), vmem((WIDE, WIDTH), F32), vmem((HELD * UNIT, WIDE), BF16)]
        + [vmem(shape, BF16) for shape in BUF_SHAPES[:5]]
        + [act()] * 4 + [act(F32), DMA((7, 2, 2)), DMA((3,))],
        compiler_params=pltpu.CompilerParams(vmem_limit_bytes=VMEM_BYTES),
        cost_estimate=pl.CostEstimate(flops=17_000_000_000, bytes_accessed=50_000_000, transcendentals=0),
        name='early_part',
    )(x_next, *params[:5], *velocities[:5], sums)


def run_head(weight, velocity, grad):
    shape = (CLASSES, WIDE)
    return pl.pallas_call(
        head_kernel,
        out_shape=[jax.ShapeDtypeStruct(shape, BF16)] + f32_outs([shape] * 2),
        in_specs=[ANY_SPEC] * 3,
        out_specs=[VMEM_SPEC] + [ANY_SPEC] * 2,
        scratch_shapes=[vmem(shape, F32)] * 2 + [vmem((CLASS_PAD, WIDE), BF16), DMA((1, 2, 2)), DMA],
        compiler_params=pltpu.CompilerParams(vmem_limit_bytes=VMEM_BYTES),
        cost_estimate=pl.CostEstimate(flops=4_000_000_000, bytes_accessed=11_000_000, transcendentals=0),
        name='head_part',
    )(weight, velocity, grad)


def run_late(mid, head, params, velocities, pieces, held):
    return pl.pallas_call(
        late_kernel,
        out_shape=f32_outs([(IMGS, CLASSES)] + [W_SHAPES[3], W_SHAPES[4]] * 2),
        in_specs=[ANY_SPEC] * 18,
        out_specs=[VMEM_SPEC] + [ANY_SPEC] * 4,
        scratch_shapes=[vmem(shape, F32) for shape in BUF_SHAPES[3:5]] * 2 + [vmem((HELD * UNIT, WIDE), BF16)]
        + [vmem(shape, BF16) for shape in BUF_SHAPES[3:5]] + [act(), vmem((CLASSES, WIDE), BF16), act(), act(), act(F32)]
        + [DMA((2, 2, 2)), DMA((8, HELD)), DMA((2,))],
        input_output_aliases={14 + i: 1 + i for i in range(4)},
        compiler_params=pltpu.CompilerParams(vmem_limit_bytes=VMEM_BYTES),
        cost_estimate=pl.CostEstimate(flops=15_000_000_000, bytes_accessed=40_000_000, transcendentals=0),
        name='late_part',
    )(mid, head, *params[3:5], *velocities[3:5], *pieces, *held)


def solution(mesh):
    def swap(array, bit):
        return lax.ppermute(array, 'data', [(d, d ^ bit) for d in range(DEVS)])

    def local_step(x_now, labels_now, x_next, *weights):
        up_one, down_one, merge, up_two, down_two = weights[:5]
        head, vel_head = weights[5].T, weights[11].T
        params, velocities = weights[:5], weights[6:11]
        sums, first, second, head_sum = run_train(x_now.reshape(ROWS * 4, WIDTH), labels_now, (*params, head))
        first_x, second_y, first_c, second_c = swap(first, 2), swap(second, 4), swap(first, 1), swap(second, 1)
        mid, *early = run_early(x_next.reshape(ROWS * 4, WIDTH), params, velocities, sums)
        first_x, second_y, mid, head_sum = lax.optimization_barrier((first_x, second_y, mid, head_sum))
        first_xc, second_yc = swap(first_x, 1), swap(second_y, 1)
        head_b, new_head, new_vel_head = run_head(head, vel_head, head_sum)
        pieces = (first, second, first_x, second_y, first_c, second_c, first_xc, second_yc)
        held = (early[3], early[4], early[8], early[9])
        logits, *late = run_late(mid, head_b, params, velocities, pieces, held)
        return (logits, *early[:3], late[0], late[1], new_head.T, *early[5:8], late[2], late[3], new_vel_head.T)

    split = P('data')
    in_specs = (split, split, split) + (P(),) * 12
    out_specs = (split,) + (P(),) * 12
    return jax.shard_map(local_step, mesh=mesh, in_specs=in_specs, out_specs=out_specs, check_vma=False)
```

```python
import jax
import jax.numpy as jnp
from jax import lax
from jax.experimental import pallas as pl
from jax.experimental.pallas import tpu as pltpu
from jax.sharding import PartitionSpec as P

MOMENTUM = 0.9
TRUST = 0.1
LN_EPS = 1e-6
GELU_A = 0.7978845608028654
GELU_B = 0.044715 * GELU_A
F32 = jnp.float32
BF16 = jnp.bfloat16
VMEM_BYTES = 66_000_000

IMGS, TOKENS, WIDTH = 4, 784, 128
MERGED = TOKENS // 4
ROWS = IMGS * MERGED
WIDE = 4 * WIDTH
HID_ONE, HID_TWO = 4 * WIDTH, 4 * WIDE
CLASSES = 1000
TILE = 256
SHARD = 64
N_TILES = HID_TWO // TILE
FWD_TILE = 512


def dot_nn(a, b):
    return lax.dot_general(a, b, (((1,), (0,)), ((), ())), preferred_element_type=F32)


def dot_nt(a, b):
    return lax.dot_general(a, b, (((1,), (1,)), ((), ())), preferred_element_type=F32)


def dot_tn(a, b):
    return lax.dot_general(a, b, (((0,), (0,)), ((), ())), preferred_element_type=F32)


def norm_parts(vals):
    centered = vals - jnp.mean(vals, axis=-1, keepdims=True)
    variance = jnp.mean(centered * centered, axis=-1, keepdims=True)
    rstd = lax.rsqrt(variance + LN_EPS)
    return centered * rstd, rstd


def norm_back(grad, normed, rstd):
    mean_g = jnp.mean(grad, axis=-1, keepdims=True)
    mean_gn = jnp.mean(grad * normed, axis=-1, keepdims=True)
    return rstd * (grad - mean_g - normed * mean_gn)


def gelu_parts(pre):
    square = pre * pre
    half = 0.5 * jnp.tanh(pre * (GELU_A + GELU_B * square)) + 0.5
    return square, half


def gelu_slope(pre, square, half):
    return half * (1.0 + pre * (1.0 - half) * (2.0 * GELU_A + 6.0 * GELU_B * square))


def cast_rows(dst, src, rows, step):
    def body(i, carry):
        sl = pl.ds(pl.multiple_of(i * step, step), step)
        dst[sl, :] = src[sl, :].astype(BF16)
        return carry
    lax.fori_loop(0, rows // step, body, 0)


def lanes(index, size):
    return pl.ds(pl.multiple_of(index * size, size), size)


def permute_tokens(x_ref, x_f32, r0):
    x_f32[...] = x_ref[...].astype(F32)
    for j in range(4):
        r0[:, j * WIDTH:(j + 1) * WIDTH] = x_f32[pl.ds(j, ROWS, stride=4), :].astype(BF16)


def stage_one_block(resid, w_up, w_down):
    res_f = resid.astype(F32)
    normed = norm_parts(res_f)[0].astype(BF16)
    pre = dot_nn(normed, w_up)
    act = (pre * gelu_parts(pre)[1]).astype(BF16)
    return (res_f + dot_nn(act, w_down)).astype(BF16)


def stage_one_forward(r0, r1, r2, up_one, down_one):
    def body(j, carry):
        sl = lanes(j, WIDTH)
        mid = stage_one_block(r0[:, sl], up_one[0], down_one[0])
        r1[:, sl] = mid
        r2[:, sl] = stage_one_block(mid, up_one[1], down_one[1])
        return carry
    lax.fori_loop(0, 4, body, 0)


def stage_two_block(src, dst, normed_ref, acc, up_ref, down_ref):
    res_f = src[...].astype(F32)
    normed_ref[...] = norm_parts(res_f)[0].astype(BF16)
    acc[...] = res_f

    def body(t, carry):
        sl = lanes(t, FWD_TILE)
        pre = dot_nn(normed_ref[...], up_ref[:, sl])
        act = (pre * gelu_parts(pre)[1]).astype(BF16)
        acc[...] += dot_nn(act, down_ref[sl, :])
        return carry
    lax.fori_loop(0, HID_TWO // FWD_TILE, body, 0)
    dst[...] = acc[...].astype(BF16)


def image_rows():
    image = lax.broadcasted_iota(jnp.int32, (8, ROWS), 0)
    row = lax.broadcasted_iota(jnp.int32, (8, ROWS), 1)
    inside = (row >= image * MERGED) & (row < (image + 1) * MERGED)
    return jnp.where(inside, 1.0, 0.0).astype(BF16)


def pooled_norm(resid):
    pooled = dot_nn(image_rows(), resid) * (1.0 / MERGED)
    return norm_parts(pooled)


UNIT = 1024
N_UNITS = 9
SHARE_ROWS = N_UNITS * UNIT
CLASS_PAD = 1024
DEVS = 8
SUBLANES = 8
LAST = N_UNITS - 1
HELD = 4
PAIR_OUT, FIRST_OUT, SECOND_OUT, SECOND_BACK, FIRST_BACK, PAIR_BACK = range(6)


class Links:
    def __init__(self, own, final, land1, land2, sems):
        self.own, self.final, self.land1, self.land2, self.sems = own, final, land1, land2, sems
        me = lax.axis_index('data')
        self.me = me
        self.core, self.x, self.y = lax.rem(me, 2), lax.rem(me // 2, 2), me // 4
        self.pair = me + 1 - 2 * self.core
        self.x_peer = me + 2 - 4 * self.x
        self.y_peer = me + 4 - 8 * self.y

    def rows(self, unit, offset, size):
        return pl.ds(pl.multiple_of(unit * UNIT + offset, SHARD), size)

    def half(self, unit, offset, size):
        return self.rows(unit, self.core * WIDE + offset, size)

    def copy(self, unit, phase, lane, src, dst, peer):
        return pltpu.make_async_remote_copy(
            src_ref=src, dst_ref=dst, send_sem=self.sems.at[unit, phase, lane, 0], recv_sem=self.sems.at[unit, phase, lane, 1],
            device_id=(peer,), device_id_type=pl.DeviceIdType.MESH)

    def copies(self, unit, phase):
        x, y = self.x, self.y
        own, final = self.own, self.final
        if phase == PAIR_OUT:
            sl = self.rows(unit, (1 - self.core) * WIDE, WIDE)
            return [self.copy(unit, PAIR_OUT, 0, own.at[sl], final.at[sl], self.pair)]
        if phase == FIRST_OUT:
            land = lambda k: self.land1.at[pl.ds(pl.multiple_of(unit * TILE + k * WIDTH, WIDTH), WIDTH)]
            return [self.copy(unit, FIRST_OUT, 0, own.at[self.half(unit, (1 - x) * WIDTH, WIDTH)], land(0), self.x_peer),
                    self.copy(unit, FIRST_OUT, 1, own.at[self.half(unit, TILE + (1 - y) * WIDTH, WIDTH)], land(1), self.y_peer)]
        if phase == SECOND_OUT:
            land = lambda k: self.land2.at[pl.ds(pl.multiple_of(unit * WIDTH + k * SHARD, SHARD), SHARD)]
            return [self.copy(unit, SECOND_OUT, 0, own.at[self.half(unit, x * WIDTH + (1 - y) * SHARD, SHARD)], land(0), self.y_peer),
                    self.copy(unit, SECOND_OUT, 1, own.at[self.half(unit, TILE + y * WIDTH + (1 - x) * SHARD, SHARD)], land(1), self.x_peer)]
        if phase == SECOND_BACK:
            first = self.half(unit, x * WIDTH + y * SHARD, SHARD)
            second = self.half(unit, TILE + y * WIDTH + x * SHARD, SHARD)
            return [self.copy(unit, SECOND_BACK, 0, final.at[first], final.at[first], self.y_peer),
                    self.copy(unit, SECOND_BACK, 1, final.at[second], final.at[second], self.x_peer)]
        if phase == FIRST_BACK:
            first, second = self.half(unit, x * WIDTH, WIDTH), self.half(unit, TILE + y * WIDTH, WIDTH)
            return [self.copy(unit, FIRST_BACK, 0, final.at[first], final.at[first], self.x_peer),
                    self.copy(unit, FIRST_BACK, 1, final.at[second], final.at[second], self.y_peer)]
        sl = self.half(unit, 0, WIDE)
        return [self.copy(unit, PAIR_BACK, 0, final.at[sl], final.at[sl], self.pair)]

    def start(self, unit, phase):
        for copy in self.copies(unit, phase):
            copy.start()

    def wait(self, unit, phase):
        for copy in self.copies(unit, phase):
            copy.wait()

    def reduce_pair(self, unit):
        self.wait(unit, PAIR_OUT)
        x, y = self.x, self.y
        for offset in ((1 - x) * WIDTH, TILE + (1 - y) * WIDTH, x * WIDTH, TILE + y * WIDTH):
            sl = self.half(unit, offset, WIDTH)
            self.own[sl, :] = self.own[sl, :] + self.final[sl, :]
        self.start(unit, FIRST_OUT)

    def reduce_first(self, unit):
        self.wait(unit, FIRST_OUT)
        x, y = self.x, self.y
        for keep in (False, True):
            for lane, base, here, there in ((0, x * WIDTH, y, 0), (1, TILE + y * WIDTH, x, WIDTH)):
                part = here if keep else 1 - here
                sl = self.half(unit, base + part * SHARD, SHARD)
                land = pl.ds(pl.multiple_of(unit * TILE + there + part * SHARD, SHARD), SHARD)
                self.own[sl, :] = self.own[sl, :] + self.land1[land, :]
        self.start(unit, SECOND_OUT)

    def reduce_second(self, unit):
        self.wait(unit, SECOND_OUT)
        for lane, offset in ((0, self.x * WIDTH + self.y * SHARD), (1, TILE + self.y * WIDTH + self.x * SHARD)):
            sl = self.half(unit, offset, SHARD)
            land = pl.ds(pl.multiple_of(unit * WIDTH + lane * SHARD, SHARD), SHARD)
            self.final[sl, :] = self.own[sl, :] + self.land2[land, :]

    def forward(self, unit, phase):
        self.wait(unit, phase)
        self.start(unit, phase + 1)


def train_kernel(x_hbm, labels_ref, up1_hbm, dn1_hbm, mg_hbm, up2_hbm, dn2_hbm, hd_hbm,
                 sums_hbm, head_hbm,
                 x_v, x_f32, st_up1, st_dn1, st_mg, st_up2, st_dn2,
                 up1, dn1, mg, up2, dn2, hd,
                 r0, r1, r2, s0, s1, normed_ref, acc, grad_a, grad_b, sems,
                 du1, dv1, own, final, land1, land2, factors, g_hd, link_sems, factor_sems, out_sems):
    links = Links(own, final, land1, land2, link_sems)
    me = links.me
    st_hd = st_dn2.at[pl.ds(0, CLASSES)]
    copies = [pltpu.make_async_copy(src, dst, sems.at[i]) for i, (src, dst) in enumerate((
        (x_hbm, x_v), (up1_hbm, st_up1), (dn1_hbm, st_dn1), (mg_hbm, st_mg),
        (up2_hbm.at[0], st_up2), (dn2_hbm.at[0], st_dn2),
        (up2_hbm.at[1], st_up2), (dn2_hbm.at[1], st_dn2), (hd_hbm, st_hd)))]
    for i in range(6):
        copies[i].start()
    barrier = pltpu.get_barrier_semaphore()
    for k in range(1, DEVS):
        pl.semaphore_signal(barrier, inc=1, device_id=(lax.rem(me + k, DEVS),), device_id_type=pl.DeviceIdType.MESH)
    copies[0].wait()
    permute_tokens(x_v, x_f32, r0)
    copies[1].wait()
    copies[2].wait()
    for n in range(2):
        cast_rows(up1.at[n], st_up1.at[n], WIDTH, SHARD)
        cast_rows(dn1.at[n], st_dn1.at[n], WIDE, TILE)
    stage_one_forward(r0, r1, r2, up1, dn1)
    copies[3].wait()
    cast_rows(mg, st_mg, WIDE, SHARD)
    s0[...] = dot_nn(r2[...], mg[...]).astype(BF16)
    s2 = grad_a
    for n, (src, dst) in enumerate(((s0, s1), (s1, s2))):
        copies[4 + 2 * n].wait()
        cast_rows(up2.at[n], st_up2, WIDE, 16)
        if n == 0:
            copies[6].start()
        copies[5 + 2 * n].wait()
        cast_rows(dn2.at[n], st_dn2, 2048, SHARD)
        copies[7 + n].start()
        stage_two_block(src, dst, normed_ref, acc, up2.at[n], dn2.at[n])
    copies[8].wait()
    cast_rows(hd, st_hd, 992, 32)
    hd[992:CLASSES, :] = st_hd[992:CLASSES, :].astype(BF16)
    hd[CLASSES:, :] = jnp.zeros((CLASS_PAD - CLASSES, WIDE), BF16)
    head_normed, head_rstd = pooled_norm(s2[...])
    head_b = head_normed.astype(BF16)
    class_id = lax.broadcasted_iota(jnp.int32, (SUBLANES, CLASS_PAD), 1)
    row_id = lax.broadcasted_iota(jnp.int32, (SUBLANES, CLASS_PAD), 0)
    logits = jnp.where(class_id < CLASSES, dot_nt(head_b, hd[...]), -jnp.inf)
    top = jnp.max(logits, axis=-1, keepdims=True)
    expd = jnp.exp(logits - top)
    probs = expd / jnp.sum(expd, axis=-1, keepdims=True)
    label = jnp.zeros((SUBLANES, CLASS_PAD), jnp.int32)
    for i in range(IMGS):
        label = jnp.where(row_id == i, labels_ref[i], label)
    onehot = jnp.where(class_id == label, 1.0, 0.0)
    grad_logits = jnp.where(row_id < IMGS, (probs - onehot) * (1.0 / (IMGS * DEVS)), 0.0).astype(BF16)
    factors[me, :, :WIDE] = head_b
    factors[me, :, WIDE:] = grad_logits
    grad_pooled = norm_back(dot_nn(grad_logits, hd[...]), head_normed, head_rstd) * (1.0 / MERGED)
    grad_a[...] = dot_tn(image_rows(), grad_pooled.astype(BF16)).astype(BF16)

    pl.semaphore_wait(barrier, DEVS - 1)

    def factor_copy(k):
        return pltpu.make_async_remote_copy(
            src_ref=factors.at[me], dst_ref=factors.at[me], send_sem=factor_sems.at[k, 0], recv_sem=factor_sems.at[k, 1],
            device_id=(lax.rem(me + k, DEVS),), device_id_type=pl.DeviceIdType.MESH)

    grads = (grad_a, grad_b)
    for step, n in enumerate((1, 0)):
        g_in, g_out = grads[step], grads[1 - step]
        src = (s0, s1)[n]
        normed_ref[...] = norm_parts(src[...].astype(F32))[0].astype(BF16)
        acc[...] = jnp.zeros_like(acc)

        def tile(t, row, n=n, g_in=g_in):
            sl = lanes(t, TILE)
            pre = dot_nn(normed_ref[...], up2[n, :, sl])
            square, half = gelu_parts(pre)
            act = (pre * half).astype(BF16)
            grad_pre = (gelu_slope(pre, square, half) * dot_nt(g_in[...], dn2[n, sl, :])).astype(BF16)
            own[pl.ds(row + TILE, TILE), :] = dot_tn(act, g_in[...]).astype(BF16)
            grad_up = dot_tn(normed_ref[...], grad_pre).astype(BF16)
            own[pl.ds(row, TILE), :TILE] = grad_up[:TILE]
            own[pl.ds(row, TILE), TILE:] = grad_up[TILE:]
            acc[...] += dot_nt(grad_pre, up2[n, :, sl])

        def body(p, carry, step=step, tile=tile):
            unit = step * 4 + p
            row = pl.multiple_of(unit * UNIT, UNIT)

            tile(2 * p, row)
            if step:
                links.reduce_pair(unit - 1)
            else:
                pl.when(p > 0)(lambda: links.reduce_pair(unit - 1))
            tile(2 * p + 1, row + WIDE)
            if step:
                links.reduce_first(unit - 4)
            links.start(unit, PAIR_OUT)
            return carry
        if step == 0:
            for k in range(1, DEVS):
                factor_copy(k).start()
        lax.fori_loop(0, N_TILES // 2, body, 0)
        normed_f, rstd = norm_parts(src[...].astype(F32))
        g_out[...] = (norm_back(acc[...], normed_f, rstd) + g_in[...].astype(F32)).astype(BF16)
    own[LAST * UNIT:LAST * UNIT + WIDE, :] = dot_tn(r2[...], grad_a[...]).astype(BF16)
    grad_b[...] = dot_nt(grad_a[...], mg[...]).astype(BF16)

    def out_copy(unit):
        rows = pl.ds(unit * UNIT, UNIT)
        return pltpu.make_async_copy(final.at[rows], sums_hbm.at[rows], out_sems.at[unit])

    def reduced(unit):
        links.reduce_second(unit)
        links.start(unit, SECOND_BACK)

    def finish(unit):
        links.wait(unit, PAIR_BACK)
        out_copy(unit).start()

    def back_first(unit):
        links.forward(unit, SECOND_BACK)

    def back_pair(unit):
        links.forward(unit, FIRST_BACK)

    def run_all(steps):
        for action, unit in steps:
            action(unit)

    links.reduce_pair(7)
    first = links.reduce_first
    slots = {1: (((reduced, 0), (reduced, 1), (reduced, 2), (first, 4)), ((first, 5),), ((reduced, 3),), ((first, 6), (back_first, 0))),
             0: (((back_first, 1),), ((back_first, 2),), ((reduced, 4),), ((first, 7),))}

    for n, src, g_in, g_out in ((1, r1, grad_b, grad_a), (0, r0, grad_a, grad_b)):
        du1[...] = jnp.zeros_like(du1)
        dv1[...] = jnp.zeros_like(dv1)

        def body(j, carry, n=n, src=src, g_in=g_in, g_out=g_out):
            sl = lanes(j, WIDTH)
            normed_f, rstd = norm_parts(src[:, sl].astype(F32))
            normed = normed_f.astype(BF16)
            grad = g_in[:, sl]
            pre = dot_nn(normed, up1[n])
            square, half = gelu_parts(pre)
            act = (pre * half).astype(BF16)
            grad_pre = (gelu_slope(pre, square, half) * dot_nt(grad, dn1[n])).astype(BF16)
            dv1[...] += dot_tn(grad, act)
            du1[...] += dot_tn(normed, grad_pre)
            if n:
                back = norm_back(dot_nt(grad_pre, up1[n]), normed_f, rstd)
                g_out[:, sl] = (back + grad.astype(F32)).astype(BF16)
            for k, steps in enumerate(slots[n]):
                pl.when(j == k)(lambda steps=steps: run_all(steps))
            return carry
        lax.fori_loop(0, 4, body, 0)
        base = LAST * UNIT + WIDE + n * WIDTH
        own[base:base + WIDTH, :] = du1[...].astype(BF16)
        own[base + TILE:base + TILE + WIDTH, :] = dv1[...].astype(BF16)
    links.start(LAST, PAIR_OUT)

    for k in range(1, DEVS):
        factor_copy(k).wait()

    def head_tile(c, carry):
        sl = pl.ds(pl.multiple_of(WIDE + c * WIDTH, WIDTH), WIDTH)
        total = jnp.zeros((WIDTH, WIDE), F32)
        for d in range(DEVS):
            total += dot_tn(factors[d, :, sl], factors[d, :, :WIDE]).astype(BF16).astype(F32)
        g_hd[pl.ds(pl.multiple_of(c * WIDTH, WIDTH), WIDTH), :] = total.astype(BF16)
        return carry
    half_tiles = CLASS_PAD // WIDTH // 2
    lax.fori_loop(0, half_tiles, head_tile, 0)
    run_all(((links.reduce_pair, LAST), (reduced, 5), (back_first, 3)))
    lax.fori_loop(half_tiles, 2 * half_tiles, head_tile, 0)
    head_copy = pltpu.make_async_copy(g_hd, head_hbm, factor_sems.at[0, 0])
    head_copy.start()
    run_all(((reduced, 6), (first, LAST), (back_pair, 0), (back_pair, 1), (finish, 0), (back_pair, 2), (finish, 1), (reduced, 7),
             (reduced, LAST), (back_first, 4), (finish, 2), (back_first, 5), (back_pair, 3), (back_first, 6), (back_first, LAST),
             (finish, 3), (back_pair, 4), (back_first, 7), (back_pair, 5), (finish, 4), (back_pair, LAST), (back_pair, 6), (finish, 5),
             (finish, LAST), (back_pair, 7), (finish, 6), (finish, 7)))
    for unit in range(N_UNITS):
        out_copy(unit).wait()
    head_copy.wait()


def sum_rows(tile):
    rows, cols = tile.shape
    return jnp.sum(tile.reshape(rows // 8, 8, cols), axis=0)


def lars_matrix(steps, piece, cols, tails=()):
    zero = jnp.zeros((8, cols), F32)

    def norms(i, carry):
        w, _, g, _ = piece(i)
        w, g = w[...], g[...].astype(F32)
        return carry[0] + sum_rows(w * w), carry[1] + sum_rows(g * g)
    w_acc, g_acc = lax.fori_loop(0, steps, norms, (zero, zero))
    for w, _, g, _ in tails:
        w, g = w[...], g[...].astype(F32)
        w_acc, g_acc = w_acc + sum_rows(w * w), g_acc + sum_rows(g * g)
    w_norm = jnp.sqrt(jnp.sum(jnp.sum(w_acc, axis=0, keepdims=True), axis=1, keepdims=True))
    g_norm = jnp.sqrt(jnp.sum(jnp.sum(g_acc, axis=0, keepdims=True), axis=1, keepdims=True))
    scale = TRUST * (w_norm / g_norm)

    def update_piece(w, v, g, b):
        new_v = MOMENTUM * v[...] + scale * g[...].astype(F32)
        new_w = w[...] - new_v
        v[...] = new_v
        w[...] = new_w
        b[...] = new_w.astype(BF16)

    def update(i, carry):
        update_piece(*piece(i))
        return carry
    lax.fori_loop(0, steps, update, 0)
    for tail in tails:
        update_piece(*tail)


def row_pieces(w, v, g, b, step):
    def piece(i):
        sl = pl.ds(pl.multiple_of(i * step, step), step)
        return w.at[sl], v.at[sl], g.at[sl], b.at[sl]
    return piece


def up_pieces(w, v, g, b):
    def piece(i):
        h, part = i // 2, lax.rem(i, 2)
        rows, cols = lanes(part, 256), lanes(h, 256)
        g_rows = pl.ds(pl.multiple_of(h * 512, 512), 256)
        return w.at[rows, cols], v.at[rows, cols], g.at[g_rows, rows], b.at[rows, cols]
    return piece


def down_pieces(w, v, g, b):
    def piece(i):
        h, part = i // 2, lax.rem(i, 2)
        rows = pl.ds(pl.multiple_of(i * 128, 128), 128)
        g_rows = pl.ds(pl.multiple_of(h * 512 + 256 + part * 128, 128), 128)
        return w.at[rows], v.at[rows], g.at[g_rows], b.at[rows]
    return piece


def start_all(copies):
    for copy in copies:
        copy.start()


def wait_all(copies):
    for copy in copies:
        copy.wait()


class Pair:
    def __init__(self, w, v, out_w, out_v, buf_w, buf_v, sems, slot):
        self.buf_w, self.buf_v = buf_w, buf_v
        ends = ((w, buf_w), (v, buf_v)), ((buf_w, out_w), (buf_v, out_v))
        self.loads, self.stores = ([pltpu.make_async_copy(src, dst, sems.at[slot, k, i]) for i, (src, dst) in enumerate(part)]
                                   for k, part in enumerate(ends))

    def update(self, steps, make, grad, cast, cols, *rest, tails=()):
        wait_all(self.loads)
        lars_matrix(steps, make(self.buf_w, self.buf_v, grad, cast, *rest), cols, tails)
        start_all(self.stores)


def next_kernel(x_hbm, up1_hbm, dn1_hbm, mg_hbm, up2_hbm, dn2_hbm, hd_hbm,
                vup1_hbm, vdn1_hbm, vmg_hbm, vup2_hbm, vdn2_hbm, vhd_hbm, sums_hbm, ghd_hbm,
                logits_ref, o_up1, o_dn1, o_mg, o_up2, o_dn2, o_hd, ov_up1, ov_dn1, ov_mg, ov_up2, ov_dn2, ov_hd,
                x_v, x_f32, wb_up1, wb_dn1, wb_mg, wb_up2, wb_dn2, vb_up1, vb_dn1, vb_mg, vb_up2, vb_dn2,
                gb_small, gb_turn, gb_two, gb_hd, up1, dn1, mg, up2, dn2, hd, r0, s0, s1, normed_ref, acc, sems, sem_g):
    def pair(n, slot, *refs):
        return Pair(*(ref.at[n] for ref in refs), sems, slot)

    ups = [pair(n, n, up1_hbm, vup1_hbm, o_up1, ov_up1, wb_up1, vb_up1) for n in range(2)]
    downs = [pair(n, 2 + n, dn1_hbm, vdn1_hbm, o_dn1, ov_dn1, wb_dn1, vb_dn1) for n in range(2)]
    merge = Pair(mg_hbm, vmg_hbm, o_mg, ov_mg, wb_mg, vb_mg, sems, 4)
    wide_ups = [pair(n, 5 + n, up2_hbm, vup2_hbm, o_up2, ov_up2, wb_up2, vb_up2) for n in range(2)]
    wide_downs = [pair(n, 7 + n, dn2_hbm, vdn2_hbm, o_dn2, ov_dn2, wb_dn2, vb_dn2) for n in range(2)]
    wb_hd, vb_hd = (buf.at[1, pl.ds(0, CLASSES)] for buf in (wb_dn2, vb_dn2))
    head = Pair(hd_hbm, vhd_hbm, o_hd, ov_hd, wb_hd, vb_hd, sems, 9)
    g_copies = [pltpu.make_async_copy(src, dst, sem_g.at[i]) for i, (src, dst) in enumerate((
        (x_hbm, x_v), (sums_hbm.at[pl.ds(LAST * UNIT, UNIT)], gb_small), (ghd_hbm, gb_hd),
        (sums_hbm.at[pl.ds(HELD * UNIT, HELD * UNIT)], gb_two), (sums_hbm.at[pl.ds(0, HELD * UNIT)], gb_two)))]
    x_copy, g_small, g_head, g_first, g_second = g_copies
    start_all((x_copy, g_small))
    for each in ups + downs + [merge]:
        start_all(each.loads)
    g_head.start()
    start_all(head.loads)
    g_first.start()
    for each in (wide_ups[0], wide_downs[0], wide_ups[1]):
        start_all(each.loads)
    x_copy.wait()
    permute_tokens(x_v, x_f32, r0)
    g_small.wait()
    for n in range(2):
        ups[n].update(2, row_pieces, gb_small.at[pl.ds(WIDE + n * WIDTH, WIDTH)], up1.at[n], WIDE, SHARD)
        gb_turn[...] = gb_small[pl.ds(WIDE + TILE + n * WIDTH, WIDTH), :].astype(F32).T
        downs[n].update(4, row_pieces, gb_turn, dn1.at[n], WIDTH, WIDTH)
    merge.update(8, row_pieces, gb_small.at[pl.ds(0, WIDE)], mg, WIDE, SHARD)
    g_head.wait()
    tail = pl.ds(992, SUBLANES)
    head.update(31, row_pieces, gb_hd, hd, WIDE, 32, tails=[(wb_hd.at[tail], vb_hd.at[tail], gb_hd.at[tail], hd.at[tail])])
    stage_one_forward(r0, s0, s1, up1, dn1)
    wait_all(head.stores)
    start_all(wide_downs[1].loads)
    s0[...] = dot_nn(s1[...], mg[...]).astype(BF16)
    for n, (src, dst) in enumerate(((s0, s1), (s1, s0))):
        g_copies[3 + n].wait()
        wide_ups[n].update(16, up_pieces, gb_two, up2, TILE)
        wide_downs[n].update(16, down_pieces, gb_two, dn2, WIDE)
        if n == 0:
            g_second.start()
        stage_two_block(src, dst, normed_ref, acc, up2, dn2)
    head_b = pooled_norm(s0[...])[0].astype(BF16)
    logits_ref[...] = dot_nt(head_b, hd[...])[:IMGS]
    for each in ups + downs + [merge] + wide_ups + wide_downs:
        wait_all(each.stores)


W_SHAPES = ((2, 128, 512), (2, 512, 128), (512, 512), (2, 512, 2048), (2, 2048, 512), (CLASSES, 512))
BUF_SHAPES = W_SHAPES[:3] + ((512, 2048), (2048, 512), (CLASSES, 512))


def vmem(shape, dtype):
    return pltpu.VMEM(shape, dtype)


ANY_SPEC = pl.BlockSpec(memory_space=pl.ANY)
VMEM_SPEC = pl.BlockSpec(memory_space=pltpu.VMEM)


def act(dtype=BF16):
    return vmem((ROWS, WIDE), dtype)


def f32_outs(shapes):
    return [jax.ShapeDtypeStruct(shape, F32) for shape in shapes]


DMA = pltpu.SemaphoreType.DMA


def run_train(x_now, labels, params):
    return pl.pallas_call(
        train_kernel,
        out_shape=[jax.ShapeDtypeStruct((rows, WIDE), BF16) for rows in (SHARE_ROWS, CLASS_PAD)],
        in_specs=[ANY_SPEC, pl.BlockSpec(memory_space=pltpu.SMEM)] + [ANY_SPEC] * 6,
        out_specs=[ANY_SPEC] * 2,
        scratch_shapes=[vmem((ROWS * 4, WIDTH), BF16), vmem((ROWS * 4, WIDTH), F32)]
        + [vmem(shape, F32) for shape in BUF_SHAPES[:5]] + [vmem(shape, BF16) for shape in W_SHAPES[:5]] + [vmem((CLASS_PAD, WIDE), BF16)]
        + [act()] * 6 + [act(F32), act(), act(), DMA((9,)), vmem((WIDTH, WIDE), F32), vmem((WIDTH, WIDE), F32)]
        + [vmem((rows, WIDE), BF16) for rows in (SHARE_ROWS, SHARE_ROWS, N_UNITS * TILE, N_UNITS * WIDTH)]
        + [vmem((DEVS, SUBLANES, WIDE + CLASS_PAD), BF16), vmem((CLASS_PAD, WIDE), BF16)]
        + [DMA((N_UNITS, 6, 2, 2)), DMA((DEVS, 2)), DMA((N_UNITS,))],
        compiler_params=pltpu.CompilerParams(vmem_limit_bytes=VMEM_BYTES, collective_id=0, has_side_effects=True),
        cost_estimate=pl.CostEstimate(flops=30_000_000_000, bytes_accessed=40_000_000, transcendentals=0),
        name='train_part',
    )(x_now, labels, *params)


def run_next(x_next, params, velocities, sums, head_sum):
    return pl.pallas_call(
        next_kernel,
        out_shape=f32_outs([(IMGS, CLASSES)] + list(W_SHAPES) * 2),
        in_specs=[ANY_SPEC] * 15,
        out_specs=[VMEM_SPEC] + [ANY_SPEC] * 12,
        scratch_shapes=[vmem((ROWS * 4, WIDTH), BF16), vmem((ROWS * 4, WIDTH), F32)]
        + [vmem(shape, F32) for shape in W_SHAPES[:5]] * 2
        + [vmem((UNIT, WIDE), BF16), vmem((WIDE, WIDTH), F32), vmem((HELD * UNIT, WIDE), BF16), vmem((CLASS_PAD, WIDE), BF16)]
        + [vmem(shape, BF16) for shape in BUF_SHAPES]
        + [act()] * 4 + [act(F32), DMA((10, 2, 2)), DMA((5,))],
        compiler_params=pltpu.CompilerParams(vmem_limit_bytes=VMEM_BYTES),
        cost_estimate=pl.CostEstimate(flops=10_000_000_000, bytes_accessed=100_000_000, transcendentals=0),
        name='next_part',
    )(x_next, *params, *velocities, sums, head_sum)


def turn_head(arrays):
    return (*arrays[:5], arrays[5].T)


def solution(mesh):
    def local_step(x_now, labels_now, x_next, *weights):
        params, velocities = turn_head(weights[:6]), turn_head(weights[6:])
        sums, head_sum = run_train(x_now.reshape(ROWS * 4, WIDTH), labels_now, params)
        outs = run_next(x_next.reshape(ROWS * 4, WIDTH), params, velocities, sums, head_sum)
        return (outs[0], *turn_head(outs[1:7]), *turn_head(outs[7:]))

    split = P('data')
    in_specs = (split, split, split) + (P(),) * 12
    out_specs = (split,) + (P(),) * 12
    return jax.shard_map(local_step, mesh=mesh, in_specs=in_specs, out_specs=out_specs, check_vma=False)
```

```python
import jax
import jax.numpy as jnp
from jax import lax
from jax.experimental import pallas as pl
from jax.experimental.pallas import tpu as pltpu
from jax.sharding import PartitionSpec as P

MOMENTUM = 0.9
TRUST = 0.1
LN_EPS = 1e-6
GELU_A = 0.7978845608028654
GELU_B = 0.044715 * GELU_A
F32 = jnp.float32
BF16 = jnp.bfloat16
VMEM_BYTES = 66_000_000

IMGS, TOKENS, WIDTH = 4, 784, 128
MERGED = TOKENS // 4
ROWS = IMGS * MERGED
WIDE = 4 * WIDTH
HID_ONE, HID_TWO = 4 * WIDTH, 4 * WIDE
CLASSES = 1000
TILE = 256
SHARD = 64
N_TILES = HID_TWO // TILE
FWD_TILE = 512


def dot_nn(a, b):
    return lax.dot_general(a, b, (((1,), (0,)), ((), ())), preferred_element_type=F32)


def dot_nt(a, b):
    return lax.dot_general(a, b, (((1,), (1,)), ((), ())), preferred_element_type=F32)


def dot_tn(a, b):
    return lax.dot_general(a, b, (((0,), (0,)), ((), ())), preferred_element_type=F32)


def norm_parts(vals):
    centered = vals - jnp.mean(vals, axis=-1, keepdims=True)
    variance = jnp.mean(centered * centered, axis=-1, keepdims=True)
    rstd = lax.rsqrt(variance + LN_EPS)
    return centered * rstd, rstd


def norm_back(grad, normed, rstd):
    mean_g = jnp.mean(grad, axis=-1, keepdims=True)
    mean_gn = jnp.mean(grad * normed, axis=-1, keepdims=True)
    return rstd * (grad - mean_g - normed * mean_gn)


def gelu_parts(pre):
    square = pre * pre
    half = 0.5 * jnp.tanh(pre * (GELU_A + GELU_B * square)) + 0.5
    return square, half


def gelu_slope(pre, square, half):
    return half * (1.0 + pre * (1.0 - half) * (2.0 * GELU_A + 6.0 * GELU_B * square))


def cast_rows(dst, src, rows, step):
    def body(i, carry):
        sl = pl.ds(pl.multiple_of(i * step, step), step)
        dst[sl, :] = src[sl, :].astype(BF16)
        return carry
    lax.fori_loop(0, rows // step, body, 0)


def lanes(index, size):
    return pl.ds(pl.multiple_of(index * size, size), size)


def permute_tokens(x_ref, x_f32, r0):
    x_f32[...] = x_ref[...].astype(F32)
    for j in range(4):
        r0[:, j * WIDTH:(j + 1) * WIDTH] = x_f32[pl.ds(j, ROWS, stride=4), :].astype(BF16)


def stage_one_block(resid, w_up, w_down):
    res_f = resid.astype(F32)
    normed = norm_parts(res_f)[0].astype(BF16)
    pre = dot_nn(normed, w_up)
    act = (pre * gelu_parts(pre)[1]).astype(BF16)
    return (res_f + dot_nn(act, w_down)).astype(BF16)


def stage_one_forward(r0, r1, r2, up_one, down_one):
    def body(j, carry):
        sl = lanes(j, WIDTH)
        mid = stage_one_block(r0[:, sl], up_one[0], down_one[0])
        r1[:, sl] = mid
        r2[:, sl] = stage_one_block(mid, up_one[1], down_one[1])
        return carry
    lax.fori_loop(0, 4, body, 0)


def stage_two_block(src, dst, normed_ref, acc, up_ref, down_ref):
    res_f = src[...].astype(F32)
    normed_ref[...] = norm_parts(res_f)[0].astype(BF16)
    acc[...] = res_f

    def body(t, carry):
        sl = lanes(t, FWD_TILE)
        pre = dot_nn(normed_ref[...], up_ref[:, sl])
        act = (pre * gelu_parts(pre)[1]).astype(BF16)
        acc[...] += dot_nn(act, down_ref[sl, :])
        return carry
    lax.fori_loop(0, HID_TWO // FWD_TILE, body, 0)
    dst[...] = acc[...].astype(BF16)


def image_rows():
    image = lax.broadcasted_iota(jnp.int32, (8, ROWS), 0)
    row = lax.broadcasted_iota(jnp.int32, (8, ROWS), 1)
    inside = (row >= image * MERGED) & (row < (image + 1) * MERGED)
    return jnp.where(inside, 1.0, 0.0).astype(BF16)


def pooled_norm(resid):
    pooled = dot_nn(image_rows(), resid) * (1.0 / MERGED)
    return norm_parts(pooled)


UNIT = 1024
N_UNITS = 9
SHARE_ROWS = N_UNITS * UNIT
CLASS_PAD = 1024
DEVS = 8
SUBLANES = 8
LAST = N_UNITS - 1
HELD = 4
PAIR_OUT, FIRST_OUT, SECOND_OUT, SECOND_BACK, FIRST_BACK, PAIR_BACK = range(6)


class Links:
    def __init__(self, own, final, land1, land2, sems):
        self.own, self.final, self.land1, self.land2, self.sems = own, final, land1, land2, sems
        me = lax.axis_index('data')
        self.me = me
        self.core, self.x, self.y = lax.rem(me, 2), lax.rem(me // 2, 2), me // 4
        self.pair = me + 1 - 2 * self.core
        self.x_peer = me + 2 - 4 * self.x
        self.y_peer = me + 4 - 8 * self.y

    def rows(self, unit, offset, size):
        return pl.ds(pl.multiple_of(unit * UNIT + offset, SHARD), size)

    def half(self, unit, offset, size):
        return self.rows(unit, self.core * WIDE + offset, size)

    def copy(self, unit, phase, lane, src, dst, peer):
        return pltpu.make_async_remote_copy(
            src_ref=src, dst_ref=dst, send_sem=self.sems.at[unit, phase, lane, 0], recv_sem=self.sems.at[unit, phase, lane, 1],
            device_id=(peer,), device_id_type=pl.DeviceIdType.MESH)

    def copies(self, unit, phase):
        x, y = self.x, self.y
        own, final = self.own, self.final
        if phase == PAIR_OUT:
            sl = self.rows(unit, (1 - self.core) * WIDE, WIDE)
            return [self.copy(unit, PAIR_OUT, 0, own.at[sl], final.at[sl], self.pair)]
        if phase == FIRST_OUT:
            land = lambda k: self.land1.at[pl.ds(pl.multiple_of(unit * TILE + k * WIDTH, WIDTH), WIDTH)]
            return [self.copy(unit, FIRST_OUT, 0, own.at[self.half(unit, (1 - x) * WIDTH, WIDTH)], land(0), self.x_peer),
                    self.copy(unit, FIRST_OUT, 1, own.at[self.half(unit, TILE + (1 - y) * WIDTH, WIDTH)], land(1), self.y_peer)]
        if phase == SECOND_OUT:
            land = lambda k: self.land2.at[pl.ds(pl.multiple_of(unit * WIDTH + k * SHARD, SHARD), SHARD)]
            return [self.copy(unit, SECOND_OUT, 0, own.at[self.half(unit, x * WIDTH + (1 - y) * SHARD, SHARD)], land(0), self.y_peer),
                    self.copy(unit, SECOND_OUT, 1, own.at[self.half(unit, TILE + y * WIDTH + (1 - x) * SHARD, SHARD)], land(1), self.x_peer)]
        if phase == SECOND_BACK:
            first = self.half(unit, x * WIDTH + y * SHARD, SHARD)
            second = self.half(unit, TILE + y * WIDTH + x * SHARD, SHARD)
            return [self.copy(unit, SECOND_BACK, 0, final.at[first], final.at[first], self.y_peer),
                    self.copy(unit, SECOND_BACK, 1, final.at[second], final.at[second], self.x_peer)]
        if phase == FIRST_BACK:
            first, second = self.half(unit, x * WIDTH, WIDTH), self.half(unit, TILE + y * WIDTH, WIDTH)
            return [self.copy(unit, FIRST_BACK, 0, final.at[first], final.at[first], self.x_peer),
                    self.copy(unit, FIRST_BACK, 1, final.at[second], final.at[second], self.y_peer)]
        sl = self.half(unit, 0, WIDE)
        return [self.copy(unit, PAIR_BACK, 0, final.at[sl], final.at[sl], self.pair)]

    def start(self, unit, phase):
        for copy in self.copies(unit, phase):
            copy.start()

    def wait(self, unit, phase):
        for copy in self.copies(unit, phase):
            copy.wait()

    def reduce_pair(self, unit):
        self.wait(unit, PAIR_OUT)
        x, y = self.x, self.y
        for offset in ((1 - x) * WIDTH, TILE + (1 - y) * WIDTH, x * WIDTH, TILE + y * WIDTH):
            sl = self.half(unit, offset, WIDTH)
            self.own[sl, :] = self.own[sl, :] + self.final[sl, :]
        self.start(unit, FIRST_OUT)

    def reduce_first(self, unit):
        self.wait(unit, FIRST_OUT)
        x, y = self.x, self.y
        for keep in (False, True):
            for lane, base, here, there in ((0, x * WIDTH, y, 0), (1, TILE + y * WIDTH, x, WIDTH)):
                part = here if keep else 1 - here
                sl = self.half(unit, base + part * SHARD, SHARD)
                land = pl.ds(pl.multiple_of(unit * TILE + there + part * SHARD, SHARD), SHARD)
                self.own[sl, :] = self.own[sl, :] + self.land1[land, :]
        self.start(unit, SECOND_OUT)

    def reduce_second(self, unit):
        self.wait(unit, SECOND_OUT)
        for lane, offset in ((0, self.x * WIDTH + self.y * SHARD), (1, TILE + self.y * WIDTH + self.x * SHARD)):
            sl = self.half(unit, offset, SHARD)
            land = pl.ds(pl.multiple_of(unit * WIDTH + lane * SHARD, SHARD), SHARD)
            self.final[sl, :] = self.own[sl, :] + self.land2[land, :]

    def forward(self, unit, phase):
        self.wait(unit, phase)
        self.start(unit, phase + 1)


def train_kernel(x_hbm, labels_ref, up1_hbm, dn1_hbm, mg_hbm, up2_hbm, dn2_hbm, hd_hbm,
                 sums_hbm, head_hbm,
                 x_v, x_f32, st_up1, st_dn1, st_mg, st_up2, st_dn2,
                 up1, dn1, mg, up2, dn2, hd,
                 r0, r1, r2, s0, s1, normed_ref, acc, grad_a, grad_b, sems,
                 du1, dv1, own, final, land1, land2, factors, g_hd, link_sems, factor_sems, out_sems):
    links = Links(own, final, land1, land2, link_sems)
    me = links.me
    st_hd = st_dn2.at[pl.ds(0, CLASSES)]
    copies = [pltpu.make_async_copy(src, dst, sems.at[i]) for i, (src, dst) in enumerate((
        (x_hbm, x_v), (up1_hbm, st_up1), (dn1_hbm, st_dn1), (mg_hbm, st_mg),
        (up2_hbm.at[0], st_up2), (dn2_hbm.at[0], st_dn2),
        (up2_hbm.at[1], st_up2), (dn2_hbm.at[1], st_dn2), (hd_hbm, st_hd)))]
    start_all(copies[:3])
    barrier = pltpu.get_barrier_semaphore()
    for k in range(1, DEVS):
        pl.semaphore_signal(barrier, inc=1, device_id=(lax.rem(me + k, DEVS),), device_id_type=pl.DeviceIdType.MESH)
    copies[0].wait()
    permute_tokens(x_v, x_f32, r0)
    wait_all(copies[1:3])
    start_all(copies[3:6])
    for n in range(2):
        cast_rows(up1.at[n], st_up1.at[n], WIDTH, SHARD)
        cast_rows(dn1.at[n], st_dn1.at[n], WIDE, TILE)
    stage_one_forward(r0, r1, r2, up1, dn1)
    copies[3].wait()
    cast_rows(mg, st_mg, WIDE, SHARD)
    s0[...] = dot_nn(r2[...], mg[...]).astype(BF16)
    s2 = grad_a
    for n, (src, dst) in enumerate(((s0, s1), (s1, s2))):
        copies[4 + 2 * n].wait()
        cast_rows(up2.at[n], st_up2, WIDE, 16)
        if n == 0:
            copies[6].start()
        copies[5 + 2 * n].wait()
        cast_rows(dn2.at[n], st_dn2, 2048, SHARD)
        copies[7 + n].start()
        stage_two_block(src, dst, normed_ref, acc, up2.at[n], dn2.at[n])
    copies[8].wait()
    cast_rows(hd, st_hd, 992, 32)
    hd[992:CLASSES, :] = st_hd[992:CLASSES, :].astype(BF16)
    hd[CLASSES:, :] = jnp.zeros((CLASS_PAD - CLASSES, WIDE), BF16)
    head_normed, head_rstd = pooled_norm(s2[...])
    head_b = head_normed.astype(BF16)
    class_id = lax.broadcasted_iota(jnp.int32, (SUBLANES, CLASS_PAD), 1)
    row_id = lax.broadcasted_iota(jnp.int32, (SUBLANES, CLASS_PAD), 0)
    logits = jnp.where(class_id < CLASSES, dot_nt(head_b, hd[...]), -jnp.inf)
    top = jnp.max(logits, axis=-1, keepdims=True)
    expd = jnp.exp(logits - top)
    probs = expd / jnp.sum(expd, axis=-1, keepdims=True)
    label = jnp.zeros((SUBLANES, CLASS_PAD), jnp.int32)
    for i in range(IMGS):
        label = jnp.where(row_id == i, labels_ref[i], label)
    onehot = jnp.where(class_id == label, 1.0, 0.0)
    grad_logits = jnp.where(row_id < IMGS, (probs - onehot) * (1.0 / (IMGS * DEVS)), 0.0).astype(BF16)
    factors[me, :, :WIDE] = head_b
    factors[me, :, WIDE:] = grad_logits
    grad_pooled = norm_back(dot_nn(grad_logits, hd[...]), head_normed, head_rstd) * (1.0 / MERGED)
    grad_a[...] = dot_tn(image_rows(), grad_pooled.astype(BF16)).astype(BF16)

    pl.semaphore_wait(barrier, DEVS - 1)

    def factor_copy(k):
        return pltpu.make_async_remote_copy(
            src_ref=factors.at[me], dst_ref=factors.at[me], send_sem=factor_sems.at[k, 0], recv_sem=factor_sems.at[k, 1],
            device_id=(lax.rem(me + k, DEVS),), device_id_type=pl.DeviceIdType.MESH)

    grads = (grad_a, grad_b)
    for step, n in enumerate((1, 0)):
        g_in, g_out = grads[step], grads[1 - step]
        src = (s0, s1)[n]
        normed_ref[...] = norm_parts(src[...].astype(F32))[0].astype(BF16)
        acc[...] = jnp.zeros_like(acc)

        def tile(t, row, n=n, g_in=g_in):
            sl = lanes(t, TILE)
            pre = dot_nn(normed_ref[...], up2[n, :, sl])
            square, half = gelu_parts(pre)
            act = (pre * half).astype(BF16)
            grad_pre = (gelu_slope(pre, square, half) * dot_nt(g_in[...], dn2[n, sl, :])).astype(BF16)
            own[pl.ds(row + TILE, TILE), :] = dot_tn(act, g_in[...]).astype(BF16)
            grad_up = dot_tn(normed_ref[...], grad_pre).astype(BF16)
            own[pl.ds(row, TILE), :TILE] = grad_up[:TILE]
            own[pl.ds(row, TILE), TILE:] = grad_up[TILE:]
            acc[...] += dot_nt(grad_pre, up2[n, :, sl])

        def body(p, carry, step=step, tile=tile):
            unit = step * 4 + p
            row = pl.multiple_of(unit * UNIT, UNIT)

            tile(2 * p, row)
            if step:
                links.reduce_pair(unit - 1)
            else:
                pl.when(p > 0)(lambda: links.reduce_pair(unit - 1))
            tile(2 * p + 1, row + WIDE)
            if step:
                links.reduce_first(unit - 4)
            links.start(unit, PAIR_OUT)
            return carry
        if step == 0:
            for k in range(1, DEVS):
                factor_copy(k).start()
        lax.fori_loop(0, N_TILES // 2, body, 0)
        normed_f, rstd = norm_parts(src[...].astype(F32))
        g_out[...] = (norm_back(acc[...], normed_f, rstd) + g_in[...].astype(F32)).astype(BF16)
    own[LAST * UNIT:LAST * UNIT + WIDE, :] = dot_tn(r2[...], grad_a[...]).astype(BF16)
    grad_b[...] = dot_nt(grad_a[...], mg[...]).astype(BF16)

    def out_copy(unit):
        rows = pl.ds(unit * UNIT, UNIT)
        return pltpu.make_async_copy(final.at[rows], sums_hbm.at[rows], out_sems.at[unit])

    def reduced(unit):
        links.reduce_second(unit)
        links.start(unit, SECOND_BACK)

    def finish(unit):
        links.wait(unit, PAIR_BACK)
        out_copy(unit).start()

    def back_first(unit):
        links.forward(unit, SECOND_BACK)

    def back_pair(unit):
        links.forward(unit, FIRST_BACK)

    def run_all(steps):
        for action, unit in steps:
            action(unit)

    links.reduce_pair(7)
    first = links.reduce_first
    slots = {1: (((reduced, 0), (reduced, 1), (reduced, 2), (first, 4)), ((first, 5),), ((reduced, 3),), ((first, 6), (back_first, 0))),
             0: (((back_first, 1),), ((back_first, 2),), ((reduced, 4),), ((first, 7),))}

    for n, src, g_in, g_out in ((1, r1, grad_b, grad_a), (0, r0, grad_a, grad_b)):
        du1[...] = jnp.zeros_like(du1)
        dv1[...] = jnp.zeros_like(dv1)

        def body(j, carry, n=n, src=src, g_in=g_in, g_out=g_out):
            sl = lanes(j, WIDTH)
            normed_f, rstd = norm_parts(src[:, sl].astype(F32))
            normed = normed_f.astype(BF16)
            grad = g_in[:, sl]
            pre = dot_nn(normed, up1[n])
            square, half = gelu_parts(pre)
            act = (pre * half).astype(BF16)
            grad_pre = (gelu_slope(pre, square, half) * dot_nt(grad, dn1[n])).astype(BF16)
            dv1[...] += dot_tn(grad, act)
            du1[...] += dot_tn(normed, grad_pre)
            if n:
                back = norm_back(dot_nt(grad_pre, up1[n]), normed_f, rstd)
                g_out[:, sl] = (back + grad.astype(F32)).astype(BF16)
            for k, steps in enumerate(slots[n]):
                pl.when(j == k)(lambda steps=steps: run_all(steps))
            return carry
        lax.fori_loop(0, 4, body, 0)
        base = LAST * UNIT + WIDE + n * WIDTH
        own[base:base + WIDTH, :] = du1[...].astype(BF16)
        own[base + TILE:base + TILE + WIDTH, :] = dv1[...].astype(BF16)
    links.start(LAST, PAIR_OUT)

    for k in range(1, DEVS):
        factor_copy(k).wait()

    def head_tile(c, carry):
        sl = pl.ds(pl.multiple_of(WIDE + c * WIDTH, WIDTH), WIDTH)
        total = jnp.zeros((WIDTH, WIDE), F32)
        for d in range(DEVS):
            total += dot_tn(factors[d, :, sl], factors[d, :, :WIDE]).astype(BF16).astype(F32)
        g_hd[pl.ds(pl.multiple_of(c * WIDTH, WIDTH), WIDTH), :] = total.astype(BF16)
        return carry
    half_tiles = CLASS_PAD // WIDTH // 2
    lax.fori_loop(0, half_tiles, head_tile, 0)
    run_all(((links.reduce_pair, LAST), (reduced, 5), (back_first, 3)))
    lax.fori_loop(half_tiles, 2 * half_tiles, head_tile, 0)
    head_copy = pltpu.make_async_copy(g_hd, head_hbm, factor_sems.at[0, 0])
    head_copy.start()
    run_all(((reduced, 6), (first, LAST), (back_pair, 0), (back_pair, 1), (finish, 0), (back_pair, 2), (finish, 1), (reduced, 7),
             (reduced, LAST), (back_first, 4), (finish, 2), (back_first, 5), (back_pair, 3), (back_first, 6), (back_first, LAST),
             (finish, 3), (back_pair, 4), (back_first, 7), (back_pair, 5), (finish, 4), (back_pair, LAST), (back_pair, 6), (finish, 5),
             (finish, LAST), (back_pair, 7), (finish, 6), (finish, 7)))
    for unit in range(N_UNITS):
        out_copy(unit).wait()
    head_copy.wait()


def sum_rows(tile):
    rows, cols = tile.shape
    return jnp.sum(tile.reshape(rows // 8, 8, cols), axis=0)


def lars_matrix(steps, piece, cols, tails=()):
    zero = jnp.zeros((8, cols), F32)

    def norms(i, carry):
        w, _, g, _ = piece(i)
        w, g = w[...], g[...].astype(F32)
        return carry[0] + sum_rows(w * w), carry[1] + sum_rows(g * g)
    w_acc, g_acc = lax.fori_loop(0, steps, norms, (zero, zero))
    for w, _, g, _ in tails:
        w, g = w[...], g[...].astype(F32)
        w_acc, g_acc = w_acc + sum_rows(w * w), g_acc + sum_rows(g * g)
    w_norm = jnp.sqrt(jnp.sum(jnp.sum(w_acc, axis=0, keepdims=True), axis=1, keepdims=True))
    g_norm = jnp.sqrt(jnp.sum(jnp.sum(g_acc, axis=0, keepdims=True), axis=1, keepdims=True))
    scale = TRUST * (w_norm / g_norm)

    def update_piece(w, v, g, b):
        new_v = MOMENTUM * v[...] + scale * g[...].astype(F32)
        new_w = w[...] - new_v
        v[...] = new_v
        w[...] = new_w
        b[...] = new_w.astype(BF16)

    def update(i, carry):
        update_piece(*piece(i))
        return carry
    lax.fori_loop(0, steps, update, 0)
    for tail in tails:
        update_piece(*tail)


def row_pieces(w, v, g, b, step):
    def piece(i):
        sl = pl.ds(pl.multiple_of(i * step, step), step)
        return w.at[sl], v.at[sl], g.at[sl], b.at[sl]
    return piece


def up_pieces(w, v, g, b):
    def piece(i):
        h, part = i // 2, lax.rem(i, 2)
        rows, cols = lanes(part, 256), lanes(h, 256)
        g_rows = pl.ds(pl.multiple_of(h * 512, 512), 256)
        return w.at[rows, cols], v.at[rows, cols], g.at[g_rows, rows], b.at[rows, cols]
    return piece


def down_pieces(w, v, g, b):
    def piece(i):
        h, part = i // 2, lax.rem(i, 2)
        rows = pl.ds(pl.multiple_of(i * 128, 128), 128)
        g_rows = pl.ds(pl.multiple_of(h * 512 + 256 + part * 128, 128), 128)
        return w.at[rows], v.at[rows], g.at[g_rows], b.at[rows]
    return piece


def start_all(copies):
    for copy in copies:
        copy.start()


def wait_all(copies):
    for copy in copies:
        copy.wait()


class Pair:
    def __init__(self, w, v, out_w, out_v, buf_w, buf_v, sems, slot):
        self.buf_w, self.buf_v = buf_w, buf_v
        ends = ((w, buf_w), (v, buf_v)), ((buf_w, out_w), (buf_v, out_v))
        self.loads, self.stores = ([pltpu.make_async_copy(src, dst, sems.at[slot, k, i]) for i, (src, dst) in enumerate(part)]
                                   for k, part in enumerate(ends))

    def update(self, steps, make, grad, cast, cols, *rest, tails=()):
        wait_all(self.loads)
        lars_matrix(steps, make(self.buf_w, self.buf_v, grad, cast, *rest), cols, tails)
        start_all(self.stores)


def next_kernel(x_hbm, up1_hbm, dn1_hbm, mg_hbm, up2_hbm, dn2_hbm, hd_hbm,
                vup1_hbm, vdn1_hbm, vmg_hbm, vup2_hbm, vdn2_hbm, vhd_hbm, sums_hbm, ghd_hbm,
                logits_ref, o_up1, o_dn1, o_mg, o_up2, o_dn2, o_hd, ov_up1, ov_dn1, ov_mg, ov_up2, ov_dn2, ov_hd,
                x_v, x_f32, wb_up1, wb_dn1, wb_mg, wb_up2, wb_dn2, vb_up1, vb_dn1, vb_mg, vb_up2, vb_dn2,
                gb_small, gb_turn, gb_two, gb_hd, up1, dn1, mg, up2, dn2, hd, r0, s0, s1, normed_ref, acc, sems, sem_g):
    def pair(n, slot, *refs):
        return Pair(*(ref.at[n] for ref in refs), sems, slot)

    ups = [pair(n, n, up1_hbm, vup1_hbm, o_up1, ov_up1, wb_up1, vb_up1) for n in range(2)]
    downs = [pair(n, 2 + n, dn1_hbm, vdn1_hbm, o_dn1, ov_dn1, wb_dn1, vb_dn1) for n in range(2)]
    merge = Pair(mg_hbm, vmg_hbm, o_mg, ov_mg, wb_mg, vb_mg, sems, 4)
    wide_ups = [pair(n, 5 + n, up2_hbm, vup2_hbm, o_up2, ov_up2, wb_up2, vb_up2) for n in range(2)]
    wide_downs = [pair(n, 7 + n, dn2_hbm, vdn2_hbm, o_dn2, ov_dn2, wb_dn2, vb_dn2) for n in range(2)]
    wb_hd, vb_hd = (buf.at[1, pl.ds(0, CLASSES)] for buf in (wb_dn2, vb_dn2))
    head = Pair(hd_hbm, vhd_hbm, o_hd, ov_hd, wb_hd, vb_hd, sems, 9)
    g_copies = [pltpu.make_async_copy(src, dst, sem_g.at[i]) for i, (src, dst) in enumerate((
        (x_hbm, x_v), (sums_hbm.at[pl.ds(LAST * UNIT, UNIT)], gb_small), (ghd_hbm, gb_hd),
        (sums_hbm.at[pl.ds(HELD * UNIT, HELD * UNIT)], gb_two), (sums_hbm.at[pl.ds(0, HELD * UNIT)], gb_two)))]
    x_copy, g_small, g_head, g_first, g_second = g_copies
    start_all((x_copy, g_small))
    for each in ups + downs:
        start_all(each.loads)
    x_copy.wait()
    start_all(merge.loads)
    permute_tokens(x_v, x_f32, r0)
    g_small.wait()
    g_head.start()
    start_all(head.loads)
    for n in range(2):
        ups[n].update(2, row_pieces, gb_small.at[pl.ds(WIDE + n * WIDTH, WIDTH)], up1.at[n], WIDE, SHARD)
        gb_turn[...] = gb_small[pl.ds(WIDE + TILE + n * WIDTH, WIDTH), :].astype(F32).T
        downs[n].update(4, row_pieces, gb_turn, dn1.at[n], WIDTH, WIDTH)
    merge.update(8, row_pieces, gb_small.at[pl.ds(0, WIDE)], mg, WIDE, SHARD)
    g_first.start()
    start_all(wide_ups[0].loads)
    g_head.wait()
    tail = pl.ds(992, SUBLANES)
    head.update(31, row_pieces, gb_hd, hd, WIDE, 32, tails=[(wb_hd.at[tail], vb_hd.at[tail], gb_hd.at[tail], hd.at[tail])])
    start_all(wide_downs[0].loads)
    stage_one_forward(r0, s0, s1, up1, dn1)
    wait_all(head.stores)
    start_all(wide_ups[1].loads)
    s0[...] = dot_nn(s1[...], mg[...]).astype(BF16)
    for n, (src, dst) in enumerate(((s0, s1), (s1, s0))):
        g_copies[3 + n].wait()
        wide_ups[n].update(16, up_pieces, gb_two, up2, TILE)
        if n == 0:
            start_all(wide_downs[1].loads)
        wide_downs[n].update(16, down_pieces, gb_two, dn2, WIDE)
        if n == 0:
            g_second.start()
        stage_two_block(src, dst, normed_ref, acc, up2, dn2)
    head_b = pooled_norm(s0[...])[0].astype(BF16)
    logits_ref[...] = dot_nt(head_b, hd[...])[:IMGS]
    for each in ups + downs + [merge] + wide_ups + wide_downs:
        wait_all(each.stores)


W_SHAPES = ((2, 128, 512), (2, 512, 128), (512, 512), (2, 512, 2048), (2, 2048, 512), (CLASSES, 512))
BUF_SHAPES = W_SHAPES[:3] + ((512, 2048), (2048, 512), (CLASSES, 512))


def vmem(shape, dtype):
    return pltpu.VMEM(shape, dtype)


ANY_SPEC = pl.BlockSpec(memory_space=pl.ANY)
VMEM_SPEC = pl.BlockSpec(memory_space=pltpu.VMEM)


def act(dtype=BF16):
    return vmem((ROWS, WIDE), dtype)


def f32_outs(shapes):
    return [jax.ShapeDtypeStruct(shape, F32) for shape in shapes]


DMA = pltpu.SemaphoreType.DMA


def run_train(x_now, labels, params):
    return pl.pallas_call(
        train_kernel,
        out_shape=[jax.ShapeDtypeStruct((rows, WIDE), BF16) for rows in (SHARE_ROWS, CLASS_PAD)],
        in_specs=[ANY_SPEC, pl.BlockSpec(memory_space=pltpu.SMEM)] + [ANY_SPEC] * 6,
        out_specs=[ANY_SPEC] * 2,
        scratch_shapes=[vmem((ROWS * 4, WIDTH), BF16), vmem((ROWS * 4, WIDTH), F32)]
        + [vmem(shape, F32) for shape in BUF_SHAPES[:5]] + [vmem(shape, BF16) for shape in W_SHAPES[:5]] + [vmem((CLASS_PAD, WIDE), BF16)]
        + [act()] * 6 + [act(F32), act(), act(), DMA((9,)), vmem((WIDTH, WIDE), F32), vmem((WIDTH, WIDE), F32)]
        + [vmem((rows, WIDE), BF16) for rows in (SHARE_ROWS, SHARE_ROWS, N_UNITS * TILE, N_UNITS * WIDTH)]
        + [vmem((DEVS, SUBLANES, WIDE + CLASS_PAD), BF16), vmem((CLASS_PAD, WIDE), BF16)]
        + [DMA((N_UNITS, 6, 2, 2)), DMA((DEVS, 2)), DMA((N_UNITS,))],
        compiler_params=pltpu.CompilerParams(vmem_limit_bytes=VMEM_BYTES, collective_id=0, has_side_effects=True),
        cost_estimate=pl.CostEstimate(flops=30_000_000_000, bytes_accessed=40_000_000, transcendentals=0),
        name='train_part',
    )(x_now, labels, *params)


def run_next(x_next, params, velocities, sums, head_sum):
    return pl.pallas_call(
        next_kernel,
        out_shape=f32_outs([(IMGS, CLASSES)] + list(W_SHAPES) * 2),
        in_specs=[ANY_SPEC] * 15,
        out_specs=[VMEM_SPEC] + [ANY_SPEC] * 12,
        scratch_shapes=[vmem((ROWS * 4, WIDTH), BF16), vmem((ROWS * 4, WIDTH), F32)]
        + [vmem(shape, F32) for shape in W_SHAPES[:5]] * 2
        + [vmem((UNIT, WIDE), BF16), vmem((WIDE, WIDTH), F32), vmem((HELD * UNIT, WIDE), BF16), vmem((CLASS_PAD, WIDE), BF16)]
        + [vmem(shape, BF16) for shape in BUF_SHAPES]
        + [act()] * 4 + [act(F32), DMA((10, 2, 2)), DMA((5,))],
        compiler_params=pltpu.CompilerParams(vmem_limit_bytes=VMEM_BYTES),
        cost_estimate=pl.CostEstimate(flops=10_000_000_000, bytes_accessed=100_000_000, transcendentals=0),
        name='next_part',
    )(x_next, *params, *velocities, sums, head_sum)


def turn_head(arrays):
    return (*arrays[:5], arrays[5].T)


def solution(mesh):
    def local_step(x_now, labels_now, x_next, *weights):
        params, velocities = turn_head(weights[:6]), turn_head(weights[6:])
        sums, head_sum = run_train(x_now.reshape(ROWS * 4, WIDTH), labels_now, params)
        outs = run_next(x_next.reshape(ROWS * 4, WIDTH), params, velocities, sums, head_sum)
        return (outs[0], *turn_head(outs[1:7]), *turn_head(outs[7:]))

    split = P('data')
    in_specs = (split, split, split) + (P(),) * 12
    out_specs = (split,) + (P(),) * 12
    return jax.shard_map(local_step, mesh=mesh, in_specs=in_specs, out_specs=out_specs, check_vma=False)
```

```python
import jax
import jax.numpy as jnp
from jax import lax
from jax.experimental import pallas as pl
from jax.experimental.pallas import tpu as pltpu
from jax.sharding import PartitionSpec as P

MOMENTUM = 0.9
TRUST = 0.1
LN_EPS = 1e-6
GELU_A = 0.7978845608028654
GELU_B = 0.044715 * GELU_A
F32 = jnp.float32
BF16 = jnp.bfloat16
VMEM_BYTES = 66_000_000

IMGS, TOKENS, WIDTH = 4, 784, 128
MERGED = TOKENS // 4
ROWS = IMGS * MERGED
WIDE = 4 * WIDTH
HID_ONE, HID_TWO = 4 * WIDTH, 4 * WIDE
CLASSES = 1000
TILE = 256
SHARD = 64
N_TILES = HID_TWO // TILE
FWD_TILE = 512


def dot_nn(a, b):
    return lax.dot_general(a, b, (((1,), (0,)), ((), ())), preferred_element_type=F32)


def dot_nt(a, b):
    return lax.dot_general(a, b, (((1,), (1,)), ((), ())), preferred_element_type=F32)


def dot_tn(a, b):
    return lax.dot_general(a, b, (((0,), (0,)), ((), ())), preferred_element_type=F32)


def norm_parts(vals):
    centered = vals - jnp.mean(vals, axis=-1, keepdims=True)
    variance = jnp.mean(centered * centered, axis=-1, keepdims=True)
    rstd = lax.rsqrt(variance + LN_EPS)
    return centered * rstd, rstd


def norm_back(grad, normed, rstd):
    mean_g = jnp.mean(grad, axis=-1, keepdims=True)
    mean_gn = jnp.mean(grad * normed, axis=-1, keepdims=True)
    return rstd * (grad - mean_g - normed * mean_gn)


def gelu_parts(pre):
    square = pre * pre
    half = 0.5 * jnp.tanh(pre * (GELU_A + GELU_B * square)) + 0.5
    return square, half


def gelu_slope(pre, square, half):
    return half * (1.0 + pre * (1.0 - half) * (2.0 * GELU_A + 6.0 * GELU_B * square))


def cast_rows(dst, src, rows, step):
    def body(i, carry):
        sl = pl.ds(pl.multiple_of(i * step, step), step)
        dst[sl, :] = src[sl, :].astype(BF16)
        return carry
    lax.fori_loop(0, rows // step, body, 0)


def lanes(index, size):
    return pl.ds(pl.multiple_of(index * size, size), size)


def permute_tokens(x_ref, x_f32, r0):
    x_f32[...] = x_ref[...].astype(F32)
    for j in range(4):
        r0[:, j * WIDTH:(j + 1) * WIDTH] = x_f32[pl.ds(j, ROWS, stride=4), :].astype(BF16)


def stage_one_block(resid, w_up, w_down):
    res_f = resid.astype(F32)
    normed = norm_parts(res_f)[0].astype(BF16)
    pre = dot_nn(normed, w_up)
    act = (pre * gelu_parts(pre)[1]).astype(BF16)
    return (res_f + dot_nn(act, w_down)).astype(BF16)


def stage_one_forward(r0, r1, r2, up_one, down_one):
    def body(j, carry):
        sl = lanes(j, WIDTH)
        mid = stage_one_block(r0[:, sl], up_one[0], down_one[0])
        r1[:, sl] = mid
        r2[:, sl] = stage_one_block(mid, up_one[1], down_one[1])
        return carry
    lax.fori_loop(0, 4, body, 0)


def stage_two_block(src, dst, normed_ref, acc, up_ref, down_ref):
    res_f = src[...].astype(F32)
    normed_ref[...] = norm_parts(res_f)[0].astype(BF16)
    acc[...] = res_f

    def body(t, carry):
        sl = lanes(t, FWD_TILE)
        pre = dot_nn(normed_ref[...], up_ref[:, sl])
        act = (pre * gelu_parts(pre)[1]).astype(BF16)
        acc[...] += dot_nn(act, down_ref[sl, :])
        return carry
    lax.fori_loop(0, HID_TWO // FWD_TILE, body, 0)
    dst[...] = acc[...].astype(BF16)


def image_rows():
    image = lax.broadcasted_iota(jnp.int32, (8, ROWS), 0)
    row = lax.broadcasted_iota(jnp.int32, (8, ROWS), 1)
    inside = (row >= image * MERGED) & (row < (image + 1) * MERGED)
    return jnp.where(inside, 1.0, 0.0).astype(BF16)


def pooled_norm(resid):
    pooled = dot_nn(image_rows(), resid) * (1.0 / MERGED)
    return norm_parts(pooled)


UNIT = 1024
N_UNITS = 9
SHARE_ROWS = N_UNITS * UNIT
CLASS_PAD = 1024
DEVS = 8
SUBLANES = 8
LAST = N_UNITS - 1
HELD = 4
MATRICES = 10
PAIR_OUT, FIRST_OUT, SECOND_OUT, SECOND_BACK, FIRST_BACK, PAIR_BACK = range(6)


def start_all(copies):
    for copy in copies:
        copy.start()


def wait_all(copies):
    for copy in copies:
        copy.wait()


def sum_rows(tile):
    rows, cols = tile.shape
    return jnp.sum(tile.reshape(rows // 8, 8, cols), axis=0)


def square_sum(ref, start, rows, step):
    def body(i, total):
        part = ref[pl.ds(pl.multiple_of(start + i * step, step), step), :].astype(F32)
        return total + sum_rows(part * part)
    return lax.fori_loop(0, rows // step, body, jnp.zeros((SUBLANES, ref.shape[1]), F32))


def total_of(tile):
    return jnp.sum(jnp.sum(tile, axis=0, keepdims=True), axis=1, keepdims=True)


class Links:
    def __init__(self, own, final, land1, land2, sems):
        self.own, self.final, self.land1, self.land2, self.sems = own, final, land1, land2, sems
        me = lax.axis_index('data')
        self.me = me
        self.core, self.x, self.y = lax.rem(me, 2), lax.rem(me // 2, 2), me // 4
        self.pair = me + 1 - 2 * self.core
        self.x_peer = me + 2 - 4 * self.x
        self.y_peer = me + 4 - 8 * self.y

    def rows(self, unit, offset, size):
        return pl.ds(pl.multiple_of(unit * UNIT + offset, SHARD), size)

    def half(self, unit, offset, size):
        return self.rows(unit, self.core * WIDE + offset, size)

    def copy(self, unit, phase, lane, src, dst, peer):
        return pltpu.make_async_remote_copy(
            src_ref=src, dst_ref=dst, send_sem=self.sems.at[unit, phase, lane, 0], recv_sem=self.sems.at[unit, phase, lane, 1],
            device_id=(peer,), device_id_type=pl.DeviceIdType.MESH)

    def copies(self, unit, phase):
        x, y = self.x, self.y
        own, final = self.own, self.final
        if phase == PAIR_OUT:
            sl = self.rows(unit, (1 - self.core) * WIDE, WIDE)
            return [self.copy(unit, PAIR_OUT, 0, own.at[sl], final.at[sl], self.pair)]
        if phase == FIRST_OUT:
            land = lambda k: self.land1.at[pl.ds(pl.multiple_of(unit * TILE + k * WIDTH, WIDTH), WIDTH)]
            return [self.copy(unit, FIRST_OUT, 0, own.at[self.half(unit, (1 - x) * WIDTH, WIDTH)], land(0), self.x_peer),
                    self.copy(unit, FIRST_OUT, 1, own.at[self.half(unit, TILE + (1 - y) * WIDTH, WIDTH)], land(1), self.y_peer)]
        if phase == SECOND_OUT:
            land = lambda k: self.land2.at[pl.ds(pl.multiple_of(unit * WIDTH + k * SHARD, SHARD), SHARD)]
            return [self.copy(unit, SECOND_OUT, 0, own.at[self.half(unit, x * WIDTH + (1 - y) * SHARD, SHARD)], land(0), self.y_peer),
                    self.copy(unit, SECOND_OUT, 1, own.at[self.half(unit, TILE + y * WIDTH + (1 - x) * SHARD, SHARD)], land(1), self.x_peer)]
        if phase == SECOND_BACK:
            first = self.half(unit, x * WIDTH + y * SHARD, SHARD)
            second = self.half(unit, TILE + y * WIDTH + x * SHARD, SHARD)
            return [self.copy(unit, SECOND_BACK, 0, final.at[first], final.at[first], self.y_peer),
                    self.copy(unit, SECOND_BACK, 1, final.at[second], final.at[second], self.x_peer)]
        if phase == FIRST_BACK:
            first, second = self.half(unit, x * WIDTH, WIDTH), self.half(unit, TILE + y * WIDTH, WIDTH)
            return [self.copy(unit, FIRST_BACK, 0, final.at[first], final.at[first], self.x_peer),
                    self.copy(unit, FIRST_BACK, 1, final.at[second], final.at[second], self.y_peer)]
        sl = self.half(unit, 0, WIDE)
        return [self.copy(unit, PAIR_BACK, 0, final.at[sl], final.at[sl], self.pair)]

    def start(self, unit, phase):
        for copy in self.copies(unit, phase):
            copy.start()

    def wait(self, unit, phase):
        for copy in self.copies(unit, phase):
            copy.wait()

    def reduce_pair(self, unit):
        self.wait(unit, PAIR_OUT)
        x, y = self.x, self.y
        for offset in ((1 - x) * WIDTH, TILE + (1 - y) * WIDTH, x * WIDTH, TILE + y * WIDTH):
            sl = self.half(unit, offset, WIDTH)
            self.own[sl, :] = self.own[sl, :] + self.final[sl, :]
        self.start(unit, FIRST_OUT)

    def reduce_first(self, unit):
        self.wait(unit, FIRST_OUT)
        x, y = self.x, self.y
        for keep in (False, True):
            for lane, base, here, there in ((0, x * WIDTH, y, 0), (1, TILE + y * WIDTH, x, WIDTH)):
                part = here if keep else 1 - here
                sl = self.half(unit, base + part * SHARD, SHARD)
                land = pl.ds(pl.multiple_of(unit * TILE + there + part * SHARD, SHARD), SHARD)
                self.own[sl, :] = self.own[sl, :] + self.land1[land, :]
        self.start(unit, SECOND_OUT)

    def reduce_second(self, unit):
        self.wait(unit, SECOND_OUT)
        for lane, offset in ((0, self.x * WIDTH + self.y * SHARD), (1, TILE + self.y * WIDTH + self.x * SHARD)):
            sl = self.half(unit, offset, SHARD)
            land = pl.ds(pl.multiple_of(unit * WIDTH + lane * SHARD, SHARD), SHARD)
            self.final[sl, :] = self.own[sl, :] + self.land2[land, :]

    def forward(self, unit, phase):
        self.wait(unit, phase)
        self.start(unit, phase + 1)


def train_kernel(x_hbm, labels_ref, up1_hbm, dn1_hbm, mg_hbm, up2_hbm, dn2_hbm, hd_hbm,
                 sums_hbm, head_hbm, scale_ref,
                 x_v, x_f32, st_up1, st_dn1, st_mg, st_up2, st_dn2,
                 up1, dn1, mg, up2, dn2, hd,
                 r0, r1, r2, s0, s1, normed_ref, acc, grad_a, grad_b, sems,
                 du1, dv1, own, final, land1, land2, factors, g_hd, w_sums, g_sums, link_sems, factor_sems, out_sems):
    links = Links(own, final, land1, land2, link_sems)
    me = links.me
    st_hd = st_dn2.at[pl.ds(0, CLASSES)]
    copies = [pltpu.make_async_copy(src, dst, sems.at[i]) for i, (src, dst) in enumerate((
        (x_hbm, x_v), (up1_hbm, st_up1), (dn1_hbm, st_dn1), (mg_hbm, st_mg),
        (up2_hbm.at[0], st_up2), (dn2_hbm.at[0], st_dn2),
        (up2_hbm.at[1], st_up2), (dn2_hbm.at[1], st_dn2), (hd_hbm, st_hd)))]
    start_all(copies[:3])
    barrier = pltpu.get_barrier_semaphore()
    for k in range(1, DEVS):
        pl.semaphore_signal(barrier, inc=1, device_id=(lax.rem(me + k, DEVS),), device_id_type=pl.DeviceIdType.MESH)
    copies[0].wait()
    permute_tokens(x_v, x_f32, r0)
    wait_all(copies[1:3])
    start_all(copies[3:6])
    for n in range(2):
        cast_rows(up1.at[n], st_up1.at[n], WIDTH, SHARD)
        cast_rows(dn1.at[n], st_dn1.at[n], WIDE, TILE)
    stage_one_forward(r0, r1, r2, up1, dn1)
    copies[3].wait()
    cast_rows(mg, st_mg, WIDE, SHARD)
    s0[...] = dot_nn(r2[...], mg[...]).astype(BF16)
    s2 = grad_a
    for n, (src, dst) in enumerate(((s0, s1), (s1, s2))):
        copies[4 + 2 * n].wait()
        cast_rows(up2.at[n], st_up2, WIDE, 16)
        if n == 0:
            copies[6].start()
        copies[5 + 2 * n].wait()
        cast_rows(dn2.at[n], st_dn2, 2048, SHARD)
        copies[7 + n].start()
        stage_two_block(src, dst, normed_ref, acc, up2.at[n], dn2.at[n])
    copies[8].wait()
    cast_rows(hd, st_hd, 992, 32)
    hd[992:CLASSES, :] = st_hd[992:CLASSES, :].astype(BF16)
    hd[CLASSES:, :] = jnp.zeros((CLASS_PAD - CLASSES, WIDE), BF16)
    head_normed, head_rstd = pooled_norm(s2[...])
    head_b = head_normed.astype(BF16)
    class_id = lax.broadcasted_iota(jnp.int32, (SUBLANES, CLASS_PAD), 1)
    row_id = lax.broadcasted_iota(jnp.int32, (SUBLANES, CLASS_PAD), 0)
    logits = jnp.where(class_id < CLASSES, dot_nt(head_b, hd[...]), -jnp.inf)
    top = jnp.max(logits, axis=-1, keepdims=True)
    expd = jnp.exp(logits - top)
    probs = expd / jnp.sum(expd, axis=-1, keepdims=True)
    label = jnp.zeros((SUBLANES, CLASS_PAD), jnp.int32)
    for i in range(IMGS):
        label = jnp.where(row_id == i, labels_ref[i], label)
    onehot = jnp.where(class_id == label, 1.0, 0.0)
    grad_logits = jnp.where(row_id < IMGS, (probs - onehot) * (1.0 / (IMGS * DEVS)), 0.0).astype(BF16)
    factors[me, :, :WIDE] = head_b
    factors[me, :, WIDE:] = grad_logits
    grad_pooled = norm_back(dot_nn(grad_logits, hd[...]), head_normed, head_rstd) * (1.0 / MERGED)
    grad_a[...] = dot_tn(image_rows(), grad_pooled.astype(BF16)).astype(BF16)

    pl.semaphore_wait(barrier, DEVS - 1)

    def factor_copy(k):
        return pltpu.make_async_remote_copy(
            src_ref=factors.at[me], dst_ref=factors.at[me], send_sem=factor_sems.at[k, 0], recv_sem=factor_sems.at[k, 1],
            device_id=(lax.rem(me + k, DEVS),), device_id_type=pl.DeviceIdType.MESH)

    grads = (grad_a, grad_b)
    for step, n in enumerate((1, 0)):
        g_in, g_out = grads[step], grads[1 - step]
        src = (s0, s1)[n]
        normed_ref[...] = norm_parts(src[...].astype(F32))[0].astype(BF16)
        acc[...] = jnp.zeros_like(acc)

        def tile(t, row, n=n, g_in=g_in):
            sl = lanes(t, TILE)
            pre = dot_nn(normed_ref[...], up2[n, :, sl])
            square, half = gelu_parts(pre)
            act = (pre * half).astype(BF16)
            grad_pre = (gelu_slope(pre, square, half) * dot_nt(g_in[...], dn2[n, sl, :])).astype(BF16)
            own[pl.ds(row + TILE, TILE), :] = dot_tn(act, g_in[...]).astype(BF16)
            grad_up = dot_tn(normed_ref[...], grad_pre).astype(BF16)
            own[pl.ds(row, TILE), :TILE] = grad_up[:TILE]
            own[pl.ds(row, TILE), TILE:] = grad_up[TILE:]
            acc[...] += dot_nt(grad_pre, up2[n, :, sl])

        def body(p, carry, step=step, tile=tile):
            unit = step * 4 + p
            row = pl.multiple_of(unit * UNIT, UNIT)

            tile(2 * p, row)
            if step:
                links.reduce_pair(unit - 1)
            else:
                pl.when(p > 0)(lambda: links.reduce_pair(unit - 1))
            tile(2 * p + 1, row + WIDE)
            if step:
                links.reduce_first(unit - 4)
            links.start(unit, PAIR_OUT)
            return carry
        if step == 0:
            for k in range(1, DEVS):
                factor_copy(k).start()
        lax.fori_loop(0, N_TILES // 2, body, 0)
        normed_f, rstd = norm_parts(src[...].astype(F32))
        g_out[...] = (norm_back(acc[...], normed_f, rstd) + g_in[...].astype(F32)).astype(BF16)
    own[LAST * UNIT:LAST * UNIT + WIDE, :] = dot_tn(r2[...], grad_a[...]).astype(BF16)
    grad_b[...] = dot_nt(grad_a[...], mg[...]).astype(BF16)

    def out_copy(unit):
        rows = pl.ds(unit * UNIT, UNIT)
        return pltpu.make_async_copy(final.at[rows], sums_hbm.at[rows], out_sems.at[unit])

    def reduced(unit):
        links.reduce_second(unit)
        links.start(unit, SECOND_BACK)

    def finish(unit):
        links.wait(unit, PAIR_BACK)
        out_copy(unit).start()
        start = unit * UNIT
        if unit < LAST:
            for k in range(4):
                matrix = (6 if unit < HELD else 5) + 2 * (k % 2)
                g_sums[matrix] += square_sum(final, start + k * TILE, TILE, SHARD)
        else:
            g_sums[4] = square_sum(final, start, WIDE, SHARD)
            for k in range(4):
                g_sums[k] = square_sum(final, start + WIDE + k * WIDTH, WIDTH, SHARD)

    def weigh(matrix, ref, rows, step):
        w_sums[pl.ds(matrix * SUBLANES, SUBLANES), :] = jnp.broadcast_to(total_of(square_sum(ref, 0, rows, step)), (SUBLANES, WIDTH))

    reloads = [pltpu.make_async_copy(src, dst, sems.at[9 + i]) for i, (src, dst) in enumerate((
        (up2_hbm.at[0], st_up2), (dn2_hbm.at[0], st_dn2), (dn2_hbm.at[1], st_dn2)))]

    def weigh_small(_):
        for n in range(2):
            weigh(n, st_up1.at[n], WIDTH, SHARD)
            weigh(2 + n, st_dn1.at[n], WIDE, WIDTH)
        weigh(4, st_mg, WIDE, SHARD)
        weigh(6, st_up2, WIDE, 16)
        w_hd = square_sum(st_dn2, 0, 992, 32) + square_sum(st_dn2, 992, SUBLANES, SUBLANES)
        w_sums[pl.ds(9 * SUBLANES, SUBLANES), :] = jnp.broadcast_to(total_of(w_hd), (SUBLANES, WIDTH))
        start_all(reloads[:2])

    def weigh_first(_):
        wait_all(reloads[:2])
        weigh(5, st_up2, WIDE, 16)
        weigh(7, st_dn2, HID_TWO, SHARD)
        reloads[2].start()

    def weigh_second(_):
        reloads[2].wait()
        weigh(8, st_dn2, HID_TWO, SHARD)
        g_sums[9] = square_sum(g_hd, 0, CLASS_PAD, SHARD)

    def back_first(unit):
        links.forward(unit, SECOND_BACK)

    def back_pair(unit):
        links.forward(unit, FIRST_BACK)

    def run_all(steps):
        for action, unit in steps:
            action(unit)

    g_sums[...] = jnp.zeros_like(g_sums)
    links.reduce_pair(7)
    first = links.reduce_first
    slots = {1: (((reduced, 0), (reduced, 1), (reduced, 2), (first, 4)), ((first, 5),), ((reduced, 3),), ((first, 6), (back_first, 0))),
             0: (((back_first, 1),), ((back_first, 2),), ((reduced, 4),), ((first, 7),))}

    for n, src, g_in, g_out in ((1, r1, grad_b, grad_a), (0, r0, grad_a, grad_b)):
        du1[...] = jnp.zeros_like(du1)
        dv1[...] = jnp.zeros_like(dv1)

        def body(j, carry, n=n, src=src, g_in=g_in, g_out=g_out):
            sl = lanes(j, WIDTH)
            normed_f, rstd = norm_parts(src[:, sl].astype(F32))
            normed = normed_f.astype(BF16)
            grad = g_in[:, sl]
            pre = dot_nn(normed, up1[n])
            square, half = gelu_parts(pre)
            act = (pre * half).astype(BF16)
            grad_pre = (gelu_slope(pre, square, half) * dot_nt(grad, dn1[n])).astype(BF16)
            dv1[...] += dot_tn(grad, act)
            du1[...] += dot_tn(normed, grad_pre)
            if n:
                back = norm_back(dot_nt(grad_pre, up1[n]), normed_f, rstd)
                g_out[:, sl] = (back + grad.astype(F32)).astype(BF16)
            for k, steps in enumerate(slots[n]):
                pl.when(j == k)(lambda steps=steps: run_all(steps))
            return carry
        lax.fori_loop(0, 4, body, 0)
        base = LAST * UNIT + WIDE + n * WIDTH
        own[base:base + WIDTH, :] = du1[...].astype(BF16)
        own[base + TILE:base + TILE + WIDTH, :] = dv1[...].astype(BF16)
    links.start(LAST, PAIR_OUT)

    for k in range(1, DEVS):
        factor_copy(k).wait()

    def head_tile(c, carry):
        sl = pl.ds(pl.multiple_of(WIDE + c * WIDTH, WIDTH), WIDTH)
        total = jnp.zeros((WIDTH, WIDE), F32)
        for d in range(DEVS):
            total += dot_tn(factors[d, :, sl], factors[d, :, :WIDE]).astype(BF16).astype(F32)
        g_hd[pl.ds(pl.multiple_of(c * WIDTH, WIDTH), WIDTH), :] = total.astype(BF16)
        return carry
    half_tiles = CLASS_PAD // WIDTH // 2
    lax.fori_loop(0, half_tiles, head_tile, 0)
    run_all(((links.reduce_pair, LAST), (reduced, 5), (back_first, 3)))
    lax.fori_loop(half_tiles, 2 * half_tiles, head_tile, 0)
    head_copy = pltpu.make_async_copy(g_hd, head_hbm, factor_sems.at[0, 0])
    head_copy.start()
    run_all(((reduced, 6), (weigh_small, 0), (first, LAST), (weigh_first, 0), (back_pair, 0), (back_pair, 1), (finish, 0), (weigh_second, 0), (back_pair, 2), (finish, 1), (reduced, 7),
             (reduced, LAST), (back_first, 4), (finish, 2), (back_first, 5), (back_pair, 3), (back_first, 6), (back_first, LAST),
             (finish, 3), (back_pair, 4), (back_first, 7), (back_pair, 5), (finish, 4), (back_pair, LAST), (back_pair, 6), (finish, 5),
             (finish, LAST), (back_pair, 7), (finish, 6), (finish, 7)))
    for matrix in range(MATRICES):
        sl = pl.ds(matrix * SUBLANES, SUBLANES)
        scale_ref[sl, :] = TRUST * (jnp.sqrt(w_sums[sl, :]) / jnp.sqrt(total_of(g_sums[matrix])))
    for unit in range(N_UNITS):
        out_copy(unit).wait()
    head_copy.wait()


def lars_matrix(steps, piece, scale, tails=()):
    def update_piece(w, v, g, b):
        new_v = MOMENTUM * v[...] + scale * g[...].astype(F32)
        new_w = w[...] - new_v
        v[...] = new_v
        w[...] = new_w
        b[...] = new_w.astype(BF16)

    def update(i, carry):
        update_piece(*piece(i))
        return carry
    lax.fori_loop(0, steps, update, 0)
    for tail in tails:
        update_piece(*tail)


def row_pieces(w, v, g, b, step):
    def piece(i):
        sl = pl.ds(pl.multiple_of(i * step, step), step)
        return w.at[sl], v.at[sl], g.at[sl], b.at[sl]
    return piece


def up_pieces(w, v, g, b):
    def piece(i):
        h, part = i // 2, lax.rem(i, 2)
        rows, cols = lanes(part, 256), lanes(h, 256)
        g_rows = pl.ds(pl.multiple_of(h * 512, 512), 256)
        return w.at[rows, cols], v.at[rows, cols], g.at[g_rows, rows], b.at[rows, cols]
    return piece


def down_pieces(w, v, g, b):
    def piece(i):
        h, part = i // 2, lax.rem(i, 2)
        rows = pl.ds(pl.multiple_of(i * 128, 128), 128)
        g_rows = pl.ds(pl.multiple_of(h * 512 + 256 + part * 128, 128), 128)
        return w.at[rows], v.at[rows], g.at[g_rows], b.at[rows]
    return piece


class Pair:
    def __init__(self, w, v, out_w, out_v, buf_w, buf_v, sems, scales, slot):
        self.buf_w, self.buf_v = buf_w, buf_v
        self.scale = scales.at[pl.ds(slot * SUBLANES, 1), pl.ds(0, 1)]
        ends = ((w, buf_w), (v, buf_v)), ((buf_w, out_w), (buf_v, out_v))
        self.loads, self.stores = ([pltpu.make_async_copy(src, dst, sems.at[slot, k, i]) for i, (src, dst) in enumerate(part)]
                                   for k, part in enumerate(ends))

    def update(self, steps, make, grad, cast, *rest, tails=()):
        wait_all(self.loads)
        lars_matrix(steps, make(self.buf_w, self.buf_v, grad, cast, *rest), self.scale[...], tails)
        start_all(self.stores)


def next_kernel(x_hbm, up1_hbm, dn1_hbm, mg_hbm, up2_hbm, dn2_hbm, hd_hbm,
                vup1_hbm, vdn1_hbm, vmg_hbm, vup2_hbm, vdn2_hbm, vhd_hbm, sums_hbm, ghd_hbm, scales,
                logits_ref, o_up1, o_dn1, o_mg, o_up2, o_dn2, o_hd, ov_up1, ov_dn1, ov_mg, ov_up2, ov_dn2, ov_hd,
                x_v, x_f32, wb_up1, wb_dn1, wb_mg, wb_up2, wb_dn2, vb_up1, vb_dn1, vb_mg, vb_up2, vb_dn2,
                gb_small, gb_turn, gb_two, gb_hd, up1, dn1, mg, up2, dn2, hd, r0, s0, s1, normed_ref, acc, sems, sem_g):
    def pair(n, slot, *refs):
        return Pair(*(ref.at[n] for ref in refs), sems, scales, slot)

    ups = [pair(n, n, up1_hbm, vup1_hbm, o_up1, ov_up1, wb_up1, vb_up1) for n in range(2)]
    downs = [pair(n, 2 + n, dn1_hbm, vdn1_hbm, o_dn1, ov_dn1, wb_dn1, vb_dn1) for n in range(2)]
    merge = Pair(mg_hbm, vmg_hbm, o_mg, ov_mg, wb_mg, vb_mg, sems, scales, 4)
    wide_ups = [pair(n, 5 + n, up2_hbm, vup2_hbm, o_up2, ov_up2, wb_up2, vb_up2) for n in range(2)]
    wide_downs = [pair(n, 7 + n, dn2_hbm, vdn2_hbm, o_dn2, ov_dn2, wb_dn2, vb_dn2) for n in range(2)]
    wb_hd, vb_hd = (buf.at[1, pl.ds(0, CLASSES)] for buf in (wb_dn2, vb_dn2))
    head = Pair(hd_hbm, vhd_hbm, o_hd, ov_hd, wb_hd, vb_hd, sems, scales, 9)
    g_copies = [pltpu.make_async_copy(src, dst, sem_g.at[i]) for i, (src, dst) in enumerate((
        (x_hbm, x_v), (sums_hbm.at[pl.ds(LAST * UNIT, UNIT)], gb_small), (ghd_hbm, gb_hd),
        (sums_hbm.at[pl.ds(HELD * UNIT, HELD * UNIT)], gb_two), (sums_hbm.at[pl.ds(0, HELD * UNIT)], gb_two)))]
    x_copy, g_small, g_head, g_first, g_second = g_copies
    start_all((x_copy, g_small))
    for each in ups + downs:
        start_all(each.loads)
    x_copy.wait()
    start_all(merge.loads)
    permute_tokens(x_v, x_f32, r0)
    g_small.wait()
    g_head.start()
    start_all(head.loads)
    for n in range(2):
        ups[n].update(2, row_pieces, gb_small.at[pl.ds(WIDE + n * WIDTH, WIDTH)], up1.at[n], SHARD)
        gb_turn[...] = gb_small[pl.ds(WIDE + TILE + n * WIDTH, WIDTH), :].astype(F32).T
        downs[n].update(4, row_pieces, gb_turn, dn1.at[n], WIDTH)
    merge.update(8, row_pieces, gb_small.at[pl.ds(0, WIDE)], mg, SHARD)
    g_first.start()
    start_all(wide_ups[0].loads)
    g_head.wait()
    tail = pl.ds(992, SUBLANES)
    head.update(31, row_pieces, gb_hd, hd, 32, tails=[(wb_hd.at[tail], vb_hd.at[tail], gb_hd.at[tail], hd.at[tail])])
    start_all(wide_downs[0].loads)
    stage_one_forward(r0, s0, s1, up1, dn1)
    wait_all(head.stores)
    start_all(wide_ups[1].loads)
    s0[...] = dot_nn(s1[...], mg[...]).astype(BF16)
    for n, (src, dst) in enumerate(((s0, s1), (s1, s0))):
        g_copies[3 + n].wait()
        wide_ups[n].update(16, up_pieces, gb_two, up2)
        if n == 0:
            start_all(wide_downs[1].loads)
        wide_downs[n].update(16, down_pieces, gb_two, dn2)
        if n == 0:
            g_second.start()
        stage_two_block(src, dst, normed_ref, acc, up2, dn2)
    head_b = pooled_norm(s0[...])[0].astype(BF16)
    logits_ref[...] = dot_nt(head_b, hd[...])[:IMGS]
    for each in ups + downs + [merge] + wide_ups + wide_downs:
        wait_all(each.stores)


W_SHAPES = ((2, 128, 512), (2, 512, 128), (512, 512), (2, 512, 2048), (2, 2048, 512), (CLASSES, 512))
BUF_SHAPES = W_SHAPES[:3] + ((512, 2048), (2048, 512), (CLASSES, 512))


def vmem(shape, dtype):
    return pltpu.VMEM(shape, dtype)


ANY_SPEC = pl.BlockSpec(memory_space=pl.ANY)
VMEM_SPEC = pl.BlockSpec(memory_space=pltpu.VMEM)


def act(dtype=BF16):
    return vmem((ROWS, WIDE), dtype)


def f32_outs(shapes):
    return [jax.ShapeDtypeStruct(shape, F32) for shape in shapes]


DMA = pltpu.SemaphoreType.DMA


def run_train(x_now, labels, params):
    return pl.pallas_call(
        train_kernel,
        out_shape=[jax.ShapeDtypeStruct((rows, WIDE), BF16) for rows in (SHARE_ROWS, CLASS_PAD)]
        + f32_outs([(MATRICES * SUBLANES, WIDTH)]),
        in_specs=[ANY_SPEC, pl.BlockSpec(memory_space=pltpu.SMEM)] + [ANY_SPEC] * 6,
        out_specs=[ANY_SPEC] * 2 + [VMEM_SPEC],
        scratch_shapes=[vmem((ROWS * 4, WIDTH), BF16), vmem((ROWS * 4, WIDTH), F32)]
        + [vmem(shape, F32) for shape in BUF_SHAPES[:5]] + [vmem(shape, BF16) for shape in W_SHAPES[:5]] + [vmem((CLASS_PAD, WIDE), BF16)]
        + [act()] * 6 + [act(F32), act(), act(), DMA((12,)), vmem((WIDTH, WIDE), F32), vmem((WIDTH, WIDE), F32)]
        + [vmem((rows, WIDE), BF16) for rows in (SHARE_ROWS, SHARE_ROWS, N_UNITS * TILE, N_UNITS * WIDTH)]
        + [vmem((DEVS, SUBLANES, WIDE + CLASS_PAD), BF16), vmem((CLASS_PAD, WIDE), BF16), vmem((MATRICES * SUBLANES, WIDTH), F32), vmem((MATRICES, SUBLANES, WIDE), F32)]
        + [DMA((N_UNITS, 6, 2, 2)), DMA((DEVS, 2)), DMA((N_UNITS,))],
        compiler_params=pltpu.CompilerParams(vmem_limit_bytes=VMEM_BYTES, collective_id=0, has_side_effects=True),
        cost_estimate=pl.CostEstimate(flops=30_000_000_000, bytes_accessed=40_000_000, transcendentals=0),
        name='train_part',
    )(x_now, labels, *params)


def run_next(x_next, params, velocities, *sums):
    return pl.pallas_call(
        next_kernel,
        out_shape=f32_outs([(IMGS, CLASSES)] + list(W_SHAPES) * 2),
        in_specs=[ANY_SPEC] * 15 + [VMEM_SPEC],
        out_specs=[VMEM_SPEC] + [ANY_SPEC] * 12,
        scratch_shapes=[vmem((ROWS * 4, WIDTH), BF16), vmem((ROWS * 4, WIDTH), F32)]
        + [vmem(shape, F32) for shape in W_SHAPES[:5]] * 2
        + [vmem((UNIT, WIDE), BF16), vmem((WIDE, WIDTH), F32), vmem((HELD * UNIT, WIDE), BF16), vmem((CLASS_PAD, WIDE), BF16)]
        + [vmem(shape, BF16) for shape in BUF_SHAPES]
        + [act()] * 4 + [act(F32), DMA((10, 2, 2)), DMA((5,))],
        compiler_params=pltpu.CompilerParams(vmem_limit_bytes=VMEM_BYTES),
        cost_estimate=pl.CostEstimate(flops=10_000_000_000, bytes_accessed=100_000_000, transcendentals=0),
        name='next_part',
    )(x_next, *params, *velocities, *sums)


def turn_head(arrays):
    return (*arrays[:5], arrays[5].T)


def solution(mesh):
    def local_step(x_now, labels_now, x_next, *weights):
        params, velocities = turn_head(weights[:6]), turn_head(weights[6:])
        sums = run_train(x_now.reshape(ROWS * 4, WIDTH), labels_now, params)
        outs = run_next(x_next.reshape(ROWS * 4, WIDTH), params, velocities, *sums)
        return (outs[0], *turn_head(outs[1:7]), *turn_head(outs[7:]))

    split = P('data')
    in_specs = (split, split, split) + (P(),) * 12
    out_specs = (split,) + (P(),) * 12
    return jax.shard_map(local_step, mesh=mesh, in_specs=in_specs, out_specs=out_specs, check_vma=False)
```

```python
import jax
import jax.numpy as jnp
from jax import lax
from jax.experimental import pallas as pl
from jax.experimental.pallas import tpu as pltpu
from jax.sharding import PartitionSpec as P

MOMENTUM = 0.9
TRUST = 0.1
LN_EPS = 1e-6
GELU_A = 0.7978845608028654
GELU_B = 0.044715 * GELU_A
F32 = jnp.float32
BF16 = jnp.bfloat16
VMEM_BYTES = 66_000_000

IMGS, TOKENS, WIDTH = 4, 784, 128
MERGED = TOKENS // 4
ROWS = IMGS * MERGED
WIDE = 4 * WIDTH
HID_ONE, HID_TWO = 4 * WIDTH, 4 * WIDE
CLASSES = 1000
TILE = 256
SHARD = 64
N_TILES = HID_TWO // TILE
FWD_TILE = 512


def dot_nn(a, b):
    return lax.dot_general(a, b, (((1,), (0,)), ((), ())), preferred_element_type=F32)


def dot_nt(a, b):
    return lax.dot_general(a, b, (((1,), (1,)), ((), ())), preferred_element_type=F32)


def dot_tn(a, b):
    return lax.dot_general(a, b, (((0,), (0,)), ((), ())), preferred_element_type=F32)


def norm_parts(vals):
    centered = vals - jnp.mean(vals, axis=-1, keepdims=True)
    variance = jnp.mean(centered * centered, axis=-1, keepdims=True)
    rstd = lax.rsqrt(variance + LN_EPS)
    return centered * rstd, rstd


def norm_back(grad, normed, rstd):
    mean_g = jnp.mean(grad, axis=-1, keepdims=True)
    mean_gn = jnp.mean(grad * normed, axis=-1, keepdims=True)
    return rstd * (grad - mean_g - normed * mean_gn)


def gelu_parts(pre):
    square = pre * pre
    half = 0.5 * jnp.tanh(pre * (GELU_A + GELU_B * square)) + 0.5
    return square, half


def gelu_slope(pre, square, half):
    return half * (1.0 + pre * (1.0 - half) * (2.0 * GELU_A + 6.0 * GELU_B * square))


def cast_rows(dst, src, rows, step):
    def body(i, carry):
        sl = pl.ds(pl.multiple_of(i * step, step), step)
        dst[sl, :] = src[sl, :].astype(BF16)
        return carry
    lax.fori_loop(0, rows // step, body, 0)


def lanes(index, size):
    return pl.ds(pl.multiple_of(index * size, size), size)


def permute_tokens(x_ref, x_f32, r0):
    x_f32[...] = x_ref[...].astype(F32)
    for j in range(4):
        r0[:, j * WIDTH:(j + 1) * WIDTH] = x_f32[pl.ds(j, ROWS, stride=4), :].astype(BF16)


def stage_one_block(resid, w_up, w_down):
    res_f = resid.astype(F32)
    normed = norm_parts(res_f)[0].astype(BF16)
    pre = dot_nn(normed, w_up)
    act = (pre * gelu_parts(pre)[1]).astype(BF16)
    return (res_f + dot_nn(act, w_down)).astype(BF16)


def stage_one_forward(r0, r1, r2, up_one, down_one):
    def body(j, carry):
        sl = lanes(j, WIDTH)
        mid = stage_one_block(r0[:, sl], up_one[0], down_one[0])
        r1[:, sl] = mid
        r2[:, sl] = stage_one_block(mid, up_one[1], down_one[1])
        return carry
    lax.fori_loop(0, 4, body, 0)


def stage_two_block(src, dst, normed_ref, acc, up_ref, down_ref):
    res_f = src[...].astype(F32)
    normed_ref[...] = norm_parts(res_f)[0].astype(BF16)
    acc[...] = res_f

    def body(t, carry):
        sl = lanes(t, FWD_TILE)
        pre = dot_nn(normed_ref[...], up_ref[:, sl])
        act = (pre * gelu_parts(pre)[1]).astype(BF16)
        acc[...] += dot_nn(act, down_ref[sl, :])
        return carry
    lax.fori_loop(0, HID_TWO // FWD_TILE, body, 0)
    dst[...] = acc[...].astype(BF16)


def image_rows():
    image = lax.broadcasted_iota(jnp.int32, (8, ROWS), 0)
    row = lax.broadcasted_iota(jnp.int32, (8, ROWS), 1)
    inside = (row >= image * MERGED) & (row < (image + 1) * MERGED)
    return jnp.where(inside, 1.0, 0.0).astype(BF16)


def pooled_norm(resid):
    pooled = dot_nn(image_rows(), resid) * (1.0 / MERGED)
    return norm_parts(pooled)


UNIT = 1024
N_UNITS = 9
SHARE_ROWS = N_UNITS * UNIT
CLASS_PAD = 1024
DEVS = 8
SUBLANES = 8
LAST = N_UNITS - 1
HELD = 4
MATRICES = 10
PAIR_OUT, FIRST_OUT, SECOND_OUT, SECOND_BACK, FIRST_BACK, PAIR_BACK = range(6)


def start_all(copies):
    for copy in copies:
        copy.start()


def wait_all(copies):
    for copy in copies:
        copy.wait()


def sum_rows(tile):
    rows, cols = tile.shape
    return jnp.sum(tile.reshape(rows // 8, 8, cols), axis=0)


def square_sum(ref, start, rows, step):
    def body(i, total):
        part = ref[pl.ds(pl.multiple_of(start + i * step, step), step), :].astype(F32)
        return total + sum_rows(part * part)
    return lax.fori_loop(0, rows // step, body, jnp.zeros((SUBLANES, ref.shape[1]), F32))


def total_of(tile):
    return jnp.sum(jnp.sum(tile, axis=0, keepdims=True), axis=1, keepdims=True)


class Links:
    def __init__(self, own, final, land1, land2, sems):
        self.own, self.final, self.land1, self.land2, self.sems = own, final, land1, land2, sems
        me = lax.axis_index('data')
        self.me = me
        self.core, self.x, self.y = lax.rem(me, 2), lax.rem(me // 2, 2), me // 4
        self.pair = me + 1 - 2 * self.core
        self.x_peer = me + 2 - 4 * self.x
        self.y_peer = me + 4 - 8 * self.y

    def rows(self, unit, offset, size):
        return pl.ds(pl.multiple_of(unit * UNIT + offset, SHARD), size)

    def half(self, unit, offset, size):
        return self.rows(unit, self.core * WIDE + offset, size)

    def copy(self, unit, phase, lane, src, dst, peer):
        return pltpu.make_async_remote_copy(
            src_ref=src, dst_ref=dst, send_sem=self.sems.at[unit, phase, lane, 0], recv_sem=self.sems.at[unit, phase, lane, 1],
            device_id=(peer,), device_id_type=pl.DeviceIdType.MESH)

    def copies(self, unit, phase):
        x, y = self.x, self.y
        own, final = self.own, self.final
        if phase == PAIR_OUT:
            sl = self.rows(unit, (1 - self.core) * WIDE, WIDE)
            return [self.copy(unit, PAIR_OUT, 0, own.at[sl], final.at[sl], self.pair)]
        if phase == FIRST_OUT:
            land = lambda k: self.land1.at[pl.ds(pl.multiple_of(unit * TILE + k * WIDTH, WIDTH), WIDTH)]
            return [self.copy(unit, FIRST_OUT, 0, own.at[self.half(unit, (1 - x) * WIDTH, WIDTH)], land(0), self.x_peer),
                    self.copy(unit, FIRST_OUT, 1, own.at[self.half(unit, TILE + (1 - y) * WIDTH, WIDTH)], land(1), self.y_peer)]
        if phase == SECOND_OUT:
            land = lambda k: self.land2.at[pl.ds(pl.multiple_of(unit * WIDTH + k * SHARD, SHARD), SHARD)]
            return [self.copy(unit, SECOND_OUT, 0, own.at[self.half(unit, x * WIDTH + (1 - y) * SHARD, SHARD)], land(0), self.y_peer),
                    self.copy(unit, SECOND_OUT, 1, own.at[self.half(unit, TILE + y * WIDTH + (1 - x) * SHARD, SHARD)], land(1), self.x_peer)]
        if phase == SECOND_BACK:
            first = self.half(unit, x * WIDTH + y * SHARD, SHARD)
            second = self.half(unit, TILE + y * WIDTH + x * SHARD, SHARD)
            return [self.copy(unit, SECOND_BACK, 0, final.at[first], final.at[first], self.y_peer),
                    self.copy(unit, SECOND_BACK, 1, final.at[second], final.at[second], self.x_peer)]
        if phase == FIRST_BACK:
            first, second = self.half(unit, x * WIDTH, WIDTH), self.half(unit, TILE + y * WIDTH, WIDTH)
            return [self.copy(unit, FIRST_BACK, 0, final.at[first], final.at[first], self.x_peer),
                    self.copy(unit, FIRST_BACK, 1, final.at[second], final.at[second], self.y_peer)]
        sl = self.half(unit, 0, WIDE)
        return [self.copy(unit, PAIR_BACK, 0, final.at[sl], final.at[sl], self.pair)]

    def start(self, unit, phase):
        for copy in self.copies(unit, phase):
            copy.start()

    def wait(self, unit, phase):
        for copy in self.copies(unit, phase):
            copy.wait()

    def reduce_pair(self, unit):
        self.wait(unit, PAIR_OUT)
        x, y = self.x, self.y
        for offset in ((1 - x) * WIDTH, TILE + (1 - y) * WIDTH, x * WIDTH, TILE + y * WIDTH):
            sl = self.half(unit, offset, WIDTH)
            self.own[sl, :] = self.own[sl, :] + self.final[sl, :]
        self.start(unit, FIRST_OUT)

    def reduce_first(self, unit):
        self.wait(unit, FIRST_OUT)
        x, y = self.x, self.y
        for keep in (False, True):
            for lane, base, here, there in ((0, x * WIDTH, y, 0), (1, TILE + y * WIDTH, x, WIDTH)):
                part = here if keep else 1 - here
                sl = self.half(unit, base + part * SHARD, SHARD)
                land = pl.ds(pl.multiple_of(unit * TILE + there + part * SHARD, SHARD), SHARD)
                self.own[sl, :] = self.own[sl, :] + self.land1[land, :]
        self.start(unit, SECOND_OUT)

    def reduce_second(self, unit):
        self.wait(unit, SECOND_OUT)
        for lane, offset in ((0, self.x * WIDTH + self.y * SHARD), (1, TILE + self.y * WIDTH + self.x * SHARD)):
            sl = self.half(unit, offset, SHARD)
            land = pl.ds(pl.multiple_of(unit * WIDTH + lane * SHARD, SHARD), SHARD)
            self.final[sl, :] = self.own[sl, :] + self.land2[land, :]

    def forward(self, unit, phase):
        self.wait(unit, phase)
        self.start(unit, phase + 1)


def train_kernel(x_hbm, x_next_hbm, labels_ref, up1_hbm, dn1_hbm, mg_hbm, up2_hbm, dn2_hbm, hd_hbm,
                 final, st_up1, st_dn1, st_mg, st_up2, st_dn2, r0, g_hd, scale_ref,
                 x_v, x_f32,
                 up1, dn1, mg, up2, dn2, hd,
                 r1, r2, s0, s1, normed_ref, acc, grad_a, grad_b, sems,
                 du1, dv1, own, land1, land2, factors, w_sums, g_sums, link_sems, factor_sems):
    links = Links(own, final, land1, land2, link_sems)
    me = links.me
    st_hd = st_dn2.at[pl.ds(0, CLASSES)]
    copies = [pltpu.make_async_copy(src, dst, sems.at[i]) for i, (src, dst) in enumerate((
        (x_hbm, x_v), (up1_hbm, st_up1), (dn1_hbm, st_dn1), (mg_hbm, st_mg),
        (up2_hbm.at[0], st_up2), (dn2_hbm.at[0], st_dn2),
        (up2_hbm.at[1], st_up2), (dn2_hbm.at[1], st_dn2), (hd_hbm, st_hd)))]
    start_all(copies[:3])
    barrier = pltpu.get_barrier_semaphore()
    for k in range(1, DEVS):
        pl.semaphore_signal(barrier, inc=1, device_id=(lax.rem(me + k, DEVS),), device_id_type=pl.DeviceIdType.MESH)
    copies[0].wait()
    permute_tokens(x_v, x_f32, r0)
    wait_all(copies[1:3])
    start_all(copies[3:6])
    for n in range(2):
        cast_rows(up1.at[n], st_up1.at[n], WIDTH, SHARD)
        cast_rows(dn1.at[n], st_dn1.at[n], WIDE, TILE)
    stage_one_forward(r0, r1, r2, up1, dn1)
    copies[3].wait()
    cast_rows(mg, st_mg, WIDE, SHARD)
    s0[...] = dot_nn(r2[...], mg[...]).astype(BF16)
    s2 = grad_a
    for n, (src, dst) in enumerate(((s0, s1), (s1, s2))):
        copies[4 + 2 * n].wait()
        cast_rows(up2.at[n], st_up2, WIDE, 16)
        if n == 0:
            copies[6].start()
        copies[5 + 2 * n].wait()
        cast_rows(dn2.at[n], st_dn2, 2048, SHARD)
        copies[7 + n].start()
        stage_two_block(src, dst, normed_ref, acc, up2.at[n], dn2.at[n])
    copies[8].wait()
    cast_rows(hd, st_hd, 992, 32)
    hd[992:CLASSES, :] = st_hd[992:CLASSES, :].astype(BF16)
    hd[CLASSES:, :] = jnp.zeros((CLASS_PAD - CLASSES, WIDE), BF16)
    head_normed, head_rstd = pooled_norm(s2[...])
    head_b = head_normed.astype(BF16)
    class_id = lax.broadcasted_iota(jnp.int32, (SUBLANES, CLASS_PAD), 1)
    row_id = lax.broadcasted_iota(jnp.int32, (SUBLANES, CLASS_PAD), 0)
    logits = jnp.where(class_id < CLASSES, dot_nt(head_b, hd[...]), -jnp.inf)
    top = jnp.max(logits, axis=-1, keepdims=True)
    expd = jnp.exp(logits - top)
    probs = expd / jnp.sum(expd, axis=-1, keepdims=True)
    label = jnp.zeros((SUBLANES, CLASS_PAD), jnp.int32)
    for i in range(IMGS):
        label = jnp.where(row_id == i, labels_ref[i], label)
    onehot = jnp.where(class_id == label, 1.0, 0.0)
    grad_logits = jnp.where(row_id < IMGS, (probs - onehot) * (1.0 / (IMGS * DEVS)), 0.0).astype(BF16)
    factors[me, :, :WIDE] = head_b
    factors[me, :, WIDE:] = grad_logits
    grad_pooled = norm_back(dot_nn(grad_logits, hd[...]), head_normed, head_rstd) * (1.0 / MERGED)
    grad_a[...] = dot_tn(image_rows(), grad_pooled.astype(BF16)).astype(BF16)

    pl.semaphore_wait(barrier, DEVS - 1)

    def factor_copy(k):
        return pltpu.make_async_remote_copy(
            src_ref=factors.at[me], dst_ref=factors.at[me], send_sem=factor_sems.at[k, 0], recv_sem=factor_sems.at[k, 1],
            device_id=(lax.rem(me + k, DEVS),), device_id_type=pl.DeviceIdType.MESH)

    grads = (grad_a, grad_b)
    for step, n in enumerate((1, 0)):
        g_in, g_out = grads[step], grads[1 - step]
        src = (s0, s1)[n]
        normed_ref[...] = norm_parts(src[...].astype(F32))[0].astype(BF16)
        acc[...] = jnp.zeros_like(acc)

        def tile(t, row, n=n, g_in=g_in):
            sl = lanes(t, TILE)
            pre = dot_nn(normed_ref[...], up2[n, :, sl])
            square, half = gelu_parts(pre)
            act = (pre * half).astype(BF16)
            grad_pre = (gelu_slope(pre, square, half) * dot_nt(g_in[...], dn2[n, sl, :])).astype(BF16)
            own[pl.ds(row + TILE, TILE), :] = dot_tn(act, g_in[...]).astype(BF16)
            grad_up = dot_tn(normed_ref[...], grad_pre).astype(BF16)
            own[pl.ds(row, TILE), :TILE] = grad_up[:TILE]
            own[pl.ds(row, TILE), TILE:] = grad_up[TILE:]
            acc[...] += dot_nt(grad_pre, up2[n, :, sl])

        def body(p, carry, step=step, tile=tile):
            unit = step * 4 + p
            row = pl.multiple_of(unit * UNIT, UNIT)

            tile(2 * p, row)
            if step:
                links.reduce_pair(unit - 1)
            else:
                pl.when(p > 0)(lambda: links.reduce_pair(unit - 1))
            tile(2 * p + 1, row + WIDE)
            if step:
                links.reduce_first(unit - 4)
            links.start(unit, PAIR_OUT)
            return carry
        if step == 0:
            for k in range(1, DEVS):
                factor_copy(k).start()
        lax.fori_loop(0, N_TILES // 2, body, 0)
        normed_f, rstd = norm_parts(src[...].astype(F32))
        g_out[...] = (norm_back(acc[...], normed_f, rstd) + g_in[...].astype(F32)).astype(BF16)
    own[LAST * UNIT:LAST * UNIT + WIDE, :] = dot_tn(r2[...], grad_a[...]).astype(BF16)
    grad_b[...] = dot_nt(grad_a[...], mg[...]).astype(BF16)

    def reduced(unit):
        links.reduce_second(unit)
        links.start(unit, SECOND_BACK)

    def finish(unit):
        links.wait(unit, PAIR_BACK)
        start = unit * UNIT
        if unit < LAST:
            for k in range(4):
                matrix = (6 if unit < HELD else 5) + 2 * (k % 2)
                g_sums[matrix] += square_sum(final, start + k * TILE, TILE, SHARD)
        else:
            g_sums[4] = square_sum(final, start, WIDE, SHARD)
            for k in range(4):
                g_sums[k] = square_sum(final, start + WIDE + k * WIDTH, WIDTH, SHARD)

    def weigh(matrix, ref, rows, step):
        w_sums[pl.ds(matrix * SUBLANES, SUBLANES), :] = jnp.broadcast_to(total_of(square_sum(ref, 0, rows, step)), (SUBLANES, WIDTH))

    reloads = [pltpu.make_async_copy(src, dst, sems.at[9 + i]) for i, (src, dst) in enumerate((
        (up2_hbm.at[0], st_up2), (dn2_hbm.at[1], st_dn2), (x_next_hbm, x_v), (dn2_hbm.at[0], st_dn2)))]

    def weigh_small(_):
        for n in range(2):
            weigh(n, st_up1.at[n], WIDTH, SHARD)
            weigh(2 + n, st_dn1.at[n], WIDE, WIDTH)
        weigh(4, st_mg, WIDE, SHARD)
        weigh(6, st_up2, WIDE, 16)
        w_hd = square_sum(st_dn2, 0, 992, 32) + square_sum(st_dn2, 992, SUBLANES, SUBLANES)
        w_sums[pl.ds(9 * SUBLANES, SUBLANES), :] = jnp.broadcast_to(total_of(w_hd), (SUBLANES, WIDTH))
        start_all(reloads[:3])

    def weigh_first(_):
        wait_all(reloads[:3])
        weigh(5, st_up2, WIDE, 16)
        weigh(8, st_dn2, HID_TWO, SHARD)
        reloads[3].start()
        permute_tokens(x_v, x_f32, r0)

    def weigh_second(_):
        reloads[3].wait()
        weigh(7, st_dn2, HID_TWO, SHARD)
        g_sums[9] = square_sum(g_hd, 0, CLASS_PAD, SHARD)

    def back_first(unit):
        links.forward(unit, SECOND_BACK)

    def back_pair(unit):
        links.forward(unit, FIRST_BACK)

    def run_all(steps):
        for action, unit in steps:
            action(unit)

    g_sums[...] = jnp.zeros_like(g_sums)
    links.reduce_pair(7)
    first = links.reduce_first
    slots = {1: (((reduced, 0), (reduced, 1), (reduced, 2), (first, 4)), ((first, 5),), ((reduced, 3),), ((first, 6), (back_first, 0))),
             0: (((back_first, 1),), ((back_first, 2),), ((reduced, 4),), ((first, 7),))}

    for n, src, g_in, g_out in ((1, r1, grad_b, grad_a), (0, r0, grad_a, grad_b)):
        du1[...] = jnp.zeros_like(du1)
        dv1[...] = jnp.zeros_like(dv1)

        def body(j, carry, n=n, src=src, g_in=g_in, g_out=g_out):
            sl = lanes(j, WIDTH)
            normed_f, rstd = norm_parts(src[:, sl].astype(F32))
            normed = normed_f.astype(BF16)
            grad = g_in[:, sl]
            pre = dot_nn(normed, up1[n])
            square, half = gelu_parts(pre)
            act = (pre * half).astype(BF16)
            grad_pre = (gelu_slope(pre, square, half) * dot_nt(grad, dn1[n])).astype(BF16)
            dv1[...] += dot_tn(grad, act)
            du1[...] += dot_tn(normed, grad_pre)
            if n:
                back = norm_back(dot_nt(grad_pre, up1[n]), normed_f, rstd)
                g_out[:, sl] = (back + grad.astype(F32)).astype(BF16)
            for k, steps in enumerate(slots[n]):
                pl.when(j == k)(lambda steps=steps: run_all(steps))
            return carry
        lax.fori_loop(0, 4, body, 0)
        base = LAST * UNIT + WIDE + n * WIDTH
        own[base:base + WIDTH, :] = du1[...].astype(BF16)
        own[base + TILE:base + TILE + WIDTH, :] = dv1[...].astype(BF16)
    links.start(LAST, PAIR_OUT)

    for k in range(1, DEVS):
        factor_copy(k).wait()

    def head_tile(c, carry):
        sl = pl.ds(pl.multiple_of(WIDE + c * WIDTH, WIDTH), WIDTH)
        total = jnp.zeros((WIDTH, WIDE), F32)
        for d in range(DEVS):
            total += dot_tn(factors[d, :, sl], factors[d, :, :WIDE]).astype(BF16).astype(F32)
        g_hd[pl.ds(pl.multiple_of(c * WIDTH, WIDTH), WIDTH), :] = total.astype(BF16)
        return carry
    half_tiles = CLASS_PAD // WIDTH // 2
    lax.fori_loop(0, half_tiles, head_tile, 0)
    run_all(((links.reduce_pair, LAST), (reduced, 5), (back_first, 3)))
    lax.fori_loop(half_tiles, 2 * half_tiles, head_tile, 0)
    run_all(((reduced, 6), (weigh_small, 0), (first, LAST), (weigh_first, 0), (back_pair, 0), (back_pair, 1), (finish, 0), (weigh_second, 0), (back_pair, 2), (finish, 1), (reduced, 7),
             (reduced, LAST), (back_first, 4), (finish, 2), (back_first, 5), (back_pair, 3), (back_first, 6), (back_first, LAST),
             (finish, 3), (back_pair, 4), (back_first, 7), (back_pair, 5), (finish, 4), (back_pair, LAST), (back_pair, 6), (finish, 5),
             (finish, LAST), (back_pair, 7), (finish, 6), (finish, 7)))
    for matrix in range(MATRICES):
        sl = pl.ds(matrix * SUBLANES, SUBLANES)
        scale_ref[sl, :] = TRUST * (jnp.sqrt(w_sums[sl, :]) / jnp.sqrt(total_of(g_sums[matrix])))


def lars_matrix(steps, piece, scale, tails=()):
    def update_piece(w, v, g, b):
        new_v = MOMENTUM * v[...] + scale * g[...].astype(F32)
        new_w = w[...] - new_v
        v[...] = new_v
        w[...] = new_w
        b[...] = new_w.astype(BF16)

    def update(i, carry):
        update_piece(*piece(i))
        return carry
    lax.fori_loop(0, steps, update, 0)
    for tail in tails:
        update_piece(*tail)


def row_pieces(w, v, g, b, step):
    def piece(i):
        sl = pl.ds(pl.multiple_of(i * step, step), step)
        return w.at[sl], v.at[sl], g.at[sl], b.at[sl]
    return piece


def up_pieces(w, v, g, b):
    def piece(i):
        h, part = i // 2, lax.rem(i, 2)
        rows, cols = lanes(part, 256), lanes(h, 256)
        g_rows = pl.ds(pl.multiple_of(h * 512, 512), 256)
        return w.at[rows, cols], v.at[rows, cols], g.at[g_rows, rows], b.at[rows, cols]
    return piece


def down_pieces(w, v, g, b):
    def piece(i):
        h, part = i // 2, lax.rem(i, 2)
        rows = pl.ds(pl.multiple_of(i * 128, 128), 128)
        g_rows = pl.ds(pl.multiple_of(h * 512 + 256 + part * 128, 128), 128)
        return w.at[rows], v.at[rows], g.at[g_rows], b.at[rows]
    return piece


class Pair:
    def __init__(self, w, v, out_w, out_v, buf_w, buf_v, sems, scales, slot):
        self.buf_w, self.buf_v = buf_w, buf_v
        self.scale = scales.at[pl.ds(slot * SUBLANES, 1), pl.ds(0, 1)]
        ins = ((v, buf_v),) if w is None else ((v, buf_v), (w, buf_w))
        self.loads, self.stores = ([pltpu.make_async_copy(src, dst, sems.at[slot, k, i]) for i, (src, dst) in enumerate(part)]
                                   for k, part in enumerate((ins, ((buf_w, out_w), (buf_v, out_v)))))

    def update(self, steps, make, grad, cast, *rest, tails=()):
        wait_all(self.loads)
        lars_matrix(steps, make(self.buf_w, self.buf_v, grad, cast, *rest), self.scale[...], tails)
        start_all(self.stores)


def next_kernel(up2_hbm, dn2_hbm, hd_hbm, vup1_hbm, vdn1_hbm, vmg_hbm, vup2_hbm, vdn2_hbm, vhd_hbm,
                sums, in_up1, in_dn1, in_mg, in_up2, in_dn2, r0, g_hd, scales,
                logits_ref, o_up1, o_dn1, o_mg, o_up2, o_dn2, o_hd, ov_up1, ov_dn1, ov_mg, ov_up2, ov_dn2, ov_hd,
                w_up1, w_dn1, w_mg, w_up2, w_dn2,
                vb_up1, vb_dn1, vb_mg, vb_up2, vb_dn2, wb_up2, wb_dn2,
                gb_turn, up1, dn1, mg, up2, dn2, hd, s0, s1, normed_ref, acc, sems):
    ups = [Pair(None, vup1_hbm.at[n], o_up1.at[n], ov_up1.at[n], w_up1.at[n], vb_up1.at[n], sems, scales, n) for n in range(2)]
    downs = [Pair(None, vdn1_hbm.at[n], o_dn1.at[n], ov_dn1.at[n], w_dn1.at[n], vb_dn1.at[n], sems, scales, 2 + n) for n in range(2)]
    merge = Pair(None, vmg_hbm, o_mg, ov_mg, w_mg, vb_mg, sems, scales, 4)
    wide_ups = [Pair((None, up2_hbm.at[1])[n], vup2_hbm.at[n], o_up2.at[n], ov_up2.at[n], (w_up2, wb_up2)[n], vb_up2.at[n],
                     sems, scales, 5 + n) for n in range(2)]
    wide_downs = [Pair((None, dn2_hbm.at[1])[n], vdn2_hbm.at[n], o_dn2.at[n], ov_dn2.at[n], (w_dn2, wb_dn2)[n], vb_dn2.at[n],
                       sems, scales, 7 + n) for n in range(2)]
    wb_hd, vb_hd = wb_dn2.at[pl.ds(0, CLASSES)], vb_dn2.at[1, pl.ds(0, CLASSES)]
    head = Pair(hd_hbm, vhd_hbm, o_hd, ov_hd, wb_hd, vb_hd, sems, scales, 9)
    for each in ups + downs + [merge, head] + wide_ups[:1]:
        start_all(each.loads)
    small = sums.at[pl.ds(LAST * UNIT, UNIT)]
    for n in range(2):
        ups[n].update(2, row_pieces, small.at[pl.ds(WIDE + n * WIDTH, WIDTH)], up1.at[n], SHARD)
        gb_turn[...] = small[pl.ds(WIDE + TILE + n * WIDTH, WIDTH), :].astype(F32).T
        downs[n].update(4, row_pieces, gb_turn, dn1.at[n], WIDTH)
    start_all(wide_downs[0].loads)
    merge.update(8, row_pieces, small.at[pl.ds(0, WIDE)], mg, SHARD)
    tail = pl.ds(992, SUBLANES)
    head.update(31, row_pieces, g_hd, hd, 32, tails=[(wb_hd.at[tail], vb_hd.at[tail], g_hd.at[tail], hd.at[tail])])
    start_all(wide_ups[1].loads)
    wide_ups[0].update(16, up_pieces, sums.at[pl.ds(HELD * UNIT, HELD * UNIT)], up2)
    wide_downs[0].update(16, down_pieces, sums.at[pl.ds(HELD * UNIT, HELD * UNIT)], dn2)
    wait_all(head.stores)
    start_all(wide_downs[1].loads)
    stage_one_forward(r0, s0, s1, up1, dn1)
    s0[...] = dot_nn(s1[...], mg[...]).astype(BF16)
    for n, (src, dst) in enumerate(((s0, s1), (s1, s0))):
        if n:
            wide_ups[n].update(16, up_pieces, sums.at[pl.ds(0, HELD * UNIT)], up2)
            wide_downs[n].update(16, down_pieces, sums.at[pl.ds(0, HELD * UNIT)], dn2)
        stage_two_block(src, dst, normed_ref, acc, up2, dn2)
    head_b = pooled_norm(s0[...])[0].astype(BF16)
    logits_ref[...] = dot_nt(head_b, hd[...])[:IMGS]
    for each in ups + downs + [merge] + wide_ups + wide_downs:
        wait_all(each.stores)


W_SHAPES = ((2, 128, 512), (2, 512, 128), (512, 512), (2, 512, 2048), (2, 2048, 512), (CLASSES, 512))
BUF_SHAPES = W_SHAPES[:3] + ((512, 2048), (2048, 512), (CLASSES, 512))


def vmem(shape, dtype):
    return pltpu.VMEM(shape, dtype)


ANY_SPEC = pl.BlockSpec(memory_space=pl.ANY)
VMEM_SPEC = pl.BlockSpec(memory_space=pltpu.VMEM)


def act(dtype=BF16):
    return vmem((ROWS, WIDE), dtype)


def f32_outs(shapes):
    return [jax.ShapeDtypeStruct(shape, F32) for shape in shapes]


DMA = pltpu.SemaphoreType.DMA


HANDED = ((SHARE_ROWS, WIDE), BF16), *((shape, F32) for shape in BUF_SHAPES[:5]), ((ROWS, WIDE), BF16), ((CLASS_PAD, WIDE), BF16)
HANDED_BYTES = 22_000_000


def run_train(x_now, x_next, labels, params):
    return pl.pallas_call(
        train_kernel,
        out_shape=[vmem(*each) for each in HANDED] + f32_outs([(MATRICES * SUBLANES, WIDTH)]),
        in_specs=[ANY_SPEC] * 2 + [pl.BlockSpec(memory_space=pltpu.SMEM)] + [ANY_SPEC] * 6,
        out_specs=[VMEM_SPEC] * 9,
        scratch_shapes=[vmem((ROWS * 4, WIDTH), BF16), vmem((ROWS * 4, WIDTH), F32)]
        + [vmem(shape, BF16) for shape in W_SHAPES[:5]] + [vmem((CLASS_PAD, WIDE), BF16)]
        + [act()] * 5 + [act(F32), act(), act(), DMA((13,)), vmem((WIDTH, WIDE), F32), vmem((WIDTH, WIDE), F32)]
        + [vmem((rows, WIDE), BF16) for rows in (SHARE_ROWS, N_UNITS * TILE, N_UNITS * WIDTH)]
        + [vmem((DEVS, SUBLANES, WIDE + CLASS_PAD), BF16), vmem((MATRICES * SUBLANES, WIDTH), F32), vmem((MATRICES, SUBLANES, WIDE), F32)]
        + [DMA((N_UNITS, 6, 2, 2)), DMA((DEVS, 2))],
        compiler_params=pltpu.CompilerParams(vmem_limit_bytes=VMEM_BYTES - HANDED_BYTES, collective_id=0, has_side_effects=True),
        cost_estimate=pl.CostEstimate(flops=30_000_000_000, bytes_accessed=40_000_000, transcendentals=0),
        name='train_part',
    )(x_now, x_next, labels, *params)


def run_next(params, velocities, handed):
    held = [vmem(*each) for each in HANDED[1:6]]
    handed = [pltpu.with_memory_space_constraint(each, pltpu.VMEM) for each in handed[:8]] + list(handed[8:])
    outs = pl.pallas_call(
        next_kernel,
        out_shape=f32_outs([(IMGS, CLASSES)] + list(W_SHAPES) * 2) + held,
        in_specs=[ANY_SPEC] * 9 + [VMEM_SPEC] * 9,
        out_specs=[VMEM_SPEC] + [ANY_SPEC] * 12 + [VMEM_SPEC] * 5,
        scratch_shapes=[vmem(shape, F32) for shape in W_SHAPES[:5] + BUF_SHAPES[3:5]] + [vmem((WIDE, WIDTH), F32)]
        + [vmem(shape, BF16) for shape in BUF_SHAPES]
        + [act()] * 3 + [act(F32), DMA((10, 2, 2))],
        input_output_aliases={10 + i: 13 + i for i in range(5)},
        compiler_params=pltpu.CompilerParams(vmem_limit_bytes=VMEM_BYTES - HANDED_BYTES),
        cost_estimate=pl.CostEstimate(flops=10_000_000_000, bytes_accessed=100_000_000, transcendentals=0),
        name='next_part',
    )(*params[3:], *velocities, *handed)
    return outs[:13]


def turn_head(arrays):
    return (*arrays[:5], arrays[5].T)


def solution(mesh):
    def local_step(x_now, labels_now, x_next, *weights):
        params, velocities = turn_head(weights[:6]), turn_head(weights[6:])
        handed = run_train(x_now.reshape(ROWS * 4, WIDTH), x_next.reshape(ROWS * 4, WIDTH), labels_now, params)
        outs = run_next(params, velocities, handed)
        return (outs[0], *turn_head(outs[1:7]), *turn_head(outs[7:]))

    split = P('data')
    in_specs = (split, split, split) + (P(),) * 12
    out_specs = (split,) + (P(),) * 12
    return jax.shard_map(local_step, mesh=mesh, in_specs=in_specs, out_specs=out_specs, check_vma=False)
```

```python
import jax
import jax.numpy as jnp
from jax import lax
from jax.experimental import pallas as pl
from jax.experimental.pallas import tpu as pltpu
from jax.sharding import PartitionSpec as P

MOMENTUM = 0.9
TRUST = 0.1
LN_EPS = 1e-6
GELU_A = 0.7978845608028654
GELU_B = 0.044715 * GELU_A
F32 = jnp.float32
BF16 = jnp.bfloat16
VMEM_BYTES = 66_000_000

IMGS, TOKENS, WIDTH = 4, 784, 128
MERGED = TOKENS // 4
ROWS = IMGS * MERGED
WIDE = 4 * WIDTH
HID_ONE, HID_TWO = 4 * WIDTH, 4 * WIDE
CLASSES = 1000
TILE = 256
SHARD = 64
N_TILES = HID_TWO // TILE
FWD_TILE = 512


def dot_nn(a, b):
    return lax.dot_general(a, b, (((1,), (0,)), ((), ())), preferred_element_type=F32)


def dot_nt(a, b):
    return lax.dot_general(a, b, (((1,), (1,)), ((), ())), preferred_element_type=F32)


def dot_tn(a, b):
    return lax.dot_general(a, b, (((0,), (0,)), ((), ())), preferred_element_type=F32)


def norm_parts(vals):
    centered = vals - jnp.mean(vals, axis=-1, keepdims=True)
    variance = jnp.mean(centered * centered, axis=-1, keepdims=True)
    rstd = lax.rsqrt(variance + LN_EPS)
    return centered * rstd, rstd


def norm_back(grad, normed, rstd):
    mean_g = jnp.mean(grad, axis=-1, keepdims=True)
    mean_gn = jnp.mean(grad * normed, axis=-1, keepdims=True)
    return rstd * (grad - mean_g - normed * mean_gn)


def gelu_parts(pre):
    square = pre * pre
    half = 0.5 * jnp.tanh(pre * (GELU_A + GELU_B * square)) + 0.5
    return square, half


def gelu_slope(pre, square, half):
    return half * (1.0 + pre * (1.0 - half) * (2.0 * GELU_A + 6.0 * GELU_B * square))


def cast_rows(dst, src, rows, step):
    def body(i, carry):
        sl = pl.ds(pl.multiple_of(i * step, step), step)
        dst[sl, :] = src[sl, :].astype(BF16)
        return carry
    lax.fori_loop(0, rows // step, body, 0)


def lanes(index, size):
    return pl.ds(pl.multiple_of(index * size, size), size)


def permute_tokens(x_ref, x_f32, r0):
    x_f32[...] = x_ref[...].astype(F32)
    for j in range(4):
        r0[:, j * WIDTH:(j + 1) * WIDTH] = x_f32[pl.ds(j, ROWS, stride=4), :].astype(BF16)


def stage_one_block(resid, w_up, w_down):
    res_f = resid.astype(F32)
    normed = norm_parts(res_f)[0].astype(BF16)
    pre = dot_nn(normed, w_up)
    act = (pre * gelu_parts(pre)[1]).astype(BF16)
    return (res_f + dot_nn(act, w_down)).astype(BF16)


def stage_one_forward(r0, r1, r2, up_one, down_one, slots=()):
    def body(j, carry):
        for k, steps in enumerate(slots):
            pl.when(j == k)(lambda steps=steps: run_all(steps))
        sl = lanes(j, WIDTH)
        mid = stage_one_block(r0[:, sl], up_one[0], down_one[0])
        r1[:, sl] = mid
        r2[:, sl] = stage_one_block(mid, up_one[1], down_one[1])
        return carry
    lax.fori_loop(0, 4, body, 0)


def stage_two_block(src, dst, normed_ref, acc, up_ref, down_ref):
    res_f = src[...].astype(F32)
    normed_ref[...] = norm_parts(res_f)[0].astype(BF16)
    acc[...] = res_f

    def body(t, carry):
        sl = lanes(t, FWD_TILE)
        pre = dot_nn(normed_ref[...], up_ref[:, sl])
        act = (pre * gelu_parts(pre)[1]).astype(BF16)
        acc[...] += dot_nn(act, down_ref[sl, :])
        return carry
    lax.fori_loop(0, HID_TWO // FWD_TILE, body, 0)
    dst[...] = acc[...].astype(BF16)


def image_rows():
    image = lax.broadcasted_iota(jnp.int32, (8, ROWS), 0)
    row = lax.broadcasted_iota(jnp.int32, (8, ROWS), 1)
    inside = (row >= image * MERGED) & (row < (image + 1) * MERGED)
    return jnp.where(inside, 1.0, 0.0).astype(BF16)


def pooled_norm(resid):
    pooled = dot_nn(image_rows(), resid) * (1.0 / MERGED)
    return norm_parts(pooled)


UNIT = 1024
N_UNITS = 9
SHARE_ROWS = N_UNITS * UNIT
CLASS_PAD = 1024
DEVS = 8
SUBLANES = 8
LAST = N_UNITS - 1
HELD = 4
MATRICES = 10
SENT = 5
PAIR_OUT, FIRST_OUT, SECOND_OUT, SECOND_BACK, FIRST_BACK, PAIR_BACK = range(6)


def start_all(copies):
    for copy in copies:
        copy.start()


def wait_all(copies):
    for copy in copies:
        copy.wait()


def sum_rows(tile):
    rows, cols = tile.shape
    return jnp.sum(tile.reshape(rows // 8, 8, cols), axis=0)


def square_sum(ref, start, rows, step):
    def body(i, total):
        part = ref[pl.ds(pl.multiple_of(start + i * step, step), step), :].astype(F32)
        return total + sum_rows(part * part)
    return lax.fori_loop(0, rows // step, body, jnp.zeros((SUBLANES, ref.shape[1]), F32))


def total_of(tile):
    return jnp.sum(jnp.sum(tile, axis=0, keepdims=True), axis=1, keepdims=True)


def run_all(steps):
    for action, unit in steps:
        action(unit)


class Links:
    def __init__(self, own, final, land1, land2, sems):
        self.own, self.final, self.land1, self.land2, self.sems = own, final, land1, land2, sems
        me = lax.axis_index('data')
        self.me = me
        self.core, self.x, self.y = lax.rem(me, 2), lax.rem(me // 2, 2), me // 4
        self.pair = me + 1 - 2 * self.core
        self.x_peer = me + 2 - 4 * self.x
        self.y_peer = me + 4 - 8 * self.y

    def rows(self, unit, offset, size):
        return pl.ds(pl.multiple_of(unit * UNIT + offset, SHARD), size)

    def half(self, unit, offset, size):
        return self.rows(unit, self.core * WIDE + offset, size)

    def copy(self, unit, phase, lane, src, dst, peer):
        return pltpu.make_async_remote_copy(
            src_ref=src, dst_ref=dst, send_sem=self.sems.at[unit, phase, lane, 0], recv_sem=self.sems.at[unit, phase, lane, 1],
            device_id=(peer,), device_id_type=pl.DeviceIdType.MESH)

    def copies(self, unit, phase):
        x, y = self.x, self.y
        own, final = self.own, self.final
        if phase == PAIR_OUT:
            sl = self.rows(unit, (1 - self.core) * WIDE, WIDE)
            return [self.copy(unit, PAIR_OUT, 0, own.at[sl], final.at[sl], self.pair)]
        if phase == FIRST_OUT:
            land = lambda k: self.land1.at[pl.ds(pl.multiple_of(unit * TILE + k * WIDTH, WIDTH), WIDTH)]
            return [self.copy(unit, FIRST_OUT, 0, own.at[self.half(unit, (1 - x) * WIDTH, WIDTH)], land(0), self.x_peer),
                    self.copy(unit, FIRST_OUT, 1, own.at[self.half(unit, TILE + (1 - y) * WIDTH, WIDTH)], land(1), self.y_peer)]
        if phase == SECOND_OUT:
            land = lambda k: self.land2.at[pl.ds(pl.multiple_of(unit * WIDTH + k * SHARD, SHARD), SHARD)]
            return [self.copy(unit, SECOND_OUT, 0, own.at[self.half(unit, x * WIDTH + (1 - y) * SHARD, SHARD)], land(0), self.y_peer),
                    self.copy(unit, SECOND_OUT, 1, own.at[self.half(unit, TILE + y * WIDTH + (1 - x) * SHARD, SHARD)], land(1), self.x_peer)]
        if phase == SECOND_BACK:
            first = self.half(unit, x * WIDTH + y * SHARD, SHARD)
            second = self.half(unit, TILE + y * WIDTH + x * SHARD, SHARD)
            return [self.copy(unit, SECOND_BACK, 0, final.at[first], final.at[first], self.y_peer),
                    self.copy(unit, SECOND_BACK, 1, final.at[second], final.at[second], self.x_peer)]
        if phase == FIRST_BACK:
            first, second = self.half(unit, x * WIDTH, WIDTH), self.half(unit, TILE + y * WIDTH, WIDTH)
            return [self.copy(unit, FIRST_BACK, 0, final.at[first], final.at[first], self.x_peer),
                    self.copy(unit, FIRST_BACK, 1, final.at[second], final.at[second], self.y_peer)]
        sl = self.half(unit, 0, WIDE)
        return [self.copy(unit, PAIR_BACK, 0, final.at[sl], final.at[sl], self.pair)]

    def start(self, unit, phase):
        for copy in self.copies(unit, phase):
            copy.start()

    def wait(self, unit, phase):
        for copy in self.copies(unit, phase):
            copy.wait()

    def reduce_pair(self, unit):
        self.wait(unit, PAIR_OUT)
        x, y = self.x, self.y
        for offset in ((1 - x) * WIDTH, TILE + (1 - y) * WIDTH, x * WIDTH, TILE + y * WIDTH):
            sl = self.half(unit, offset, WIDTH)
            self.own[sl, :] = self.own[sl, :] + self.final[sl, :]
        self.start(unit, FIRST_OUT)

    def reduce_first(self, unit):
        self.wait(unit, FIRST_OUT)
        x, y = self.x, self.y
        for keep in (False, True):
            for lane, base, here, there in ((0, x * WIDTH, y, 0), (1, TILE + y * WIDTH, x, WIDTH)):
                part = here if keep else 1 - here
                sl = self.half(unit, base + part * SHARD, SHARD)
                land = pl.ds(pl.multiple_of(unit * TILE + there + part * SHARD, SHARD), SHARD)
                self.own[sl, :] = self.own[sl, :] + self.land1[land, :]
        self.start(unit, SECOND_OUT)

    def reduce_second(self, unit):
        self.wait(unit, SECOND_OUT)
        for lane, offset in ((0, self.x * WIDTH + self.y * SHARD), (1, TILE + self.y * WIDTH + self.x * SHARD)):
            sl = self.half(unit, offset, SHARD)
            land = pl.ds(pl.multiple_of(unit * WIDTH + lane * SHARD, SHARD), SHARD)
            self.final[sl, :] = self.own[sl, :] + self.land2[land, :]

    def back_first(self, unit):
        self.forward(unit, SECOND_BACK)

    def back_pair(self, unit):
        self.forward(unit, FIRST_BACK)

    def forward(self, unit, phase):
        self.wait(unit, phase)
        self.start(unit, phase + 1)


def train_kernel(x_hbm, labels_ref, up1_hbm, dn1_hbm, mg_hbm, up2_hbm, dn2_hbm, hd_hbm,
                 final, g_hd,
                 x_v, x_f32, st_up1, st_dn1, st_mg, st_up2, st_dn2, r0,
                 up1, dn1, mg, up2, dn2, hd,
                 r1, r2, s0, s1, normed_ref, acc, grad_a, grad_b, sems,
                 du1, dv1, own, land1, land2, factors, link_sems, factor_sems):
    links = Links(own, final, land1, land2, link_sems)
    me = links.me
    st_hd = st_dn2.at[pl.ds(0, CLASSES)]
    copies = [pltpu.make_async_copy(src, dst, sems.at[i]) for i, (src, dst) in enumerate((
        (x_hbm, x_v), (up1_hbm, st_up1), (dn1_hbm, st_dn1), (mg_hbm, st_mg),
        (up2_hbm.at[0], st_up2), (dn2_hbm.at[0], st_dn2),
        (up2_hbm.at[1], st_up2), (dn2_hbm.at[1], st_dn2), (hd_hbm, st_hd)))]
    start_all(copies[:3])
    barrier = pltpu.get_barrier_semaphore()
    for k in range(1, DEVS):
        pl.semaphore_signal(barrier, inc=1, device_id=(lax.rem(me + k, DEVS),), device_id_type=pl.DeviceIdType.MESH)
    copies[0].wait()
    permute_tokens(x_v, x_f32, r0)
    wait_all(copies[1:3])
    start_all(copies[3:6])
    for n in range(2):
        cast_rows(up1.at[n], st_up1.at[n], WIDTH, SHARD)
        cast_rows(dn1.at[n], st_dn1.at[n], WIDE, TILE)
    stage_one_forward(r0, r1, r2, up1, dn1)
    copies[3].wait()
    cast_rows(mg, st_mg, WIDE, SHARD)
    s0[...] = dot_nn(r2[...], mg[...]).astype(BF16)
    s2 = grad_a
    for n, (src, dst) in enumerate(((s0, s1), (s1, s2))):
        copies[4 + 2 * n].wait()
        cast_rows(up2.at[n], st_up2, WIDE, 16)
        if n == 0:
            copies[6].start()
        copies[5 + 2 * n].wait()
        cast_rows(dn2.at[n], st_dn2, 2048, SHARD)
        copies[7 + n].start()
        stage_two_block(src, dst, normed_ref, acc, up2.at[n], dn2.at[n])
    copies[8].wait()
    cast_rows(hd, st_hd, 992, 32)
    hd[992:CLASSES, :] = st_hd[992:CLASSES, :].astype(BF16)
    hd[CLASSES:, :] = jnp.zeros((CLASS_PAD - CLASSES, WIDE), BF16)
    head_normed, head_rstd = pooled_norm(s2[...])
    head_b = head_normed.astype(BF16)
    class_id = lax.broadcasted_iota(jnp.int32, (SUBLANES, CLASS_PAD), 1)
    row_id = lax.broadcasted_iota(jnp.int32, (SUBLANES, CLASS_PAD), 0)
    logits = jnp.where(class_id < CLASSES, dot_nt(head_b, hd[...]), -jnp.inf)
    top = jnp.max(logits, axis=-1, keepdims=True)
    expd = jnp.exp(logits - top)
    probs = expd / jnp.sum(expd, axis=-1, keepdims=True)
    label = jnp.zeros((SUBLANES, CLASS_PAD), jnp.int32)
    for i in range(IMGS):
        label = jnp.where(row_id == i, labels_ref[i], label)
    onehot = jnp.where(class_id == label, 1.0, 0.0)
    grad_logits = jnp.where(row_id < IMGS, (probs - onehot) * (1.0 / (IMGS * DEVS)), 0.0).astype(BF16)
    factors[me, :, :WIDE] = head_b
    factors[me, :, WIDE:] = grad_logits
    grad_pooled = norm_back(dot_nn(grad_logits, hd[...]), head_normed, head_rstd) * (1.0 / MERGED)
    grad_a[...] = dot_tn(image_rows(), grad_pooled.astype(BF16)).astype(BF16)

    pl.semaphore_wait(barrier, DEVS - 1)

    def factor_copy(k):
        return pltpu.make_async_remote_copy(
            src_ref=factors.at[me], dst_ref=factors.at[me], send_sem=factor_sems.at[k, 0], recv_sem=factor_sems.at[k, 1],
            device_id=(lax.rem(me + k, DEVS),), device_id_type=pl.DeviceIdType.MESH)

    grads = (grad_a, grad_b)
    for step, n in enumerate((1, 0)):
        g_in, g_out = grads[step], grads[1 - step]
        src = (s0, s1)[n]
        normed_ref[...] = norm_parts(src[...].astype(F32))[0].astype(BF16)
        acc[...] = jnp.zeros_like(acc)

        def tile(t, row, n=n, g_in=g_in):
            sl = lanes(t, TILE)
            pre = dot_nn(normed_ref[...], up2[n, :, sl])
            square, half = gelu_parts(pre)
            act = (pre * half).astype(BF16)
            grad_pre = (gelu_slope(pre, square, half) * dot_nt(g_in[...], dn2[n, sl, :])).astype(BF16)
            own[pl.ds(row + TILE, TILE), :] = dot_tn(act, g_in[...]).astype(BF16)
            grad_up = dot_tn(normed_ref[...], grad_pre).astype(BF16)
            own[pl.ds(row, TILE), :TILE] = grad_up[:TILE]
            own[pl.ds(row, TILE), TILE:] = grad_up[TILE:]
            acc[...] += dot_nt(grad_pre, up2[n, :, sl])

        def body(p, carry, step=step, tile=tile):
            unit = step * 4 + p
            row = pl.multiple_of(unit * UNIT, UNIT)

            tile(2 * p, row)
            if step:
                links.reduce_pair(unit - 1)
            else:
                pl.when(p > 0)(lambda: links.reduce_pair(unit - 1))
            tile(2 * p + 1, row + WIDE)
            if step:
                links.reduce_first(unit - 4)
            links.start(unit, PAIR_OUT)
            return carry
        if step == 0:
            for k in range(1, DEVS):
                factor_copy(k).start()
        lax.fori_loop(0, N_TILES // 2, body, 0)
        normed_f, rstd = norm_parts(src[...].astype(F32))
        g_out[...] = (norm_back(acc[...], normed_f, rstd) + g_in[...].astype(F32)).astype(BF16)
    own[LAST * UNIT:LAST * UNIT + WIDE, :] = dot_tn(r2[...], grad_a[...]).astype(BF16)
    grad_b[...] = dot_nt(grad_a[...], mg[...]).astype(BF16)

    def reduced(unit):
        links.reduce_second(unit)
        links.start(unit, SECOND_BACK)

    links.reduce_pair(7)
    first = links.reduce_first
    slots = {1: (((reduced, 0), (reduced, 1), (reduced, 2), (first, 4)), ((first, 5),), ((reduced, 3),), ((first, 6),)),
             0: ((), (), ((reduced, 4),), ((first, 7),))}

    for n, src, g_in, g_out in ((1, r1, grad_b, grad_a), (0, r0, grad_a, grad_b)):
        du1[...] = jnp.zeros_like(du1)
        dv1[...] = jnp.zeros_like(dv1)

        def body(j, carry, n=n, src=src, g_in=g_in, g_out=g_out):
            sl = lanes(j, WIDTH)
            normed_f, rstd = norm_parts(src[:, sl].astype(F32))
            normed = normed_f.astype(BF16)
            grad = g_in[:, sl]
            pre = dot_nn(normed, up1[n])
            square, half = gelu_parts(pre)
            act = (pre * half).astype(BF16)
            grad_pre = (gelu_slope(pre, square, half) * dot_nt(grad, dn1[n])).astype(BF16)
            dv1[...] += dot_tn(grad, act)
            du1[...] += dot_tn(normed, grad_pre)
            if n:
                back = norm_back(dot_nt(grad_pre, up1[n]), normed_f, rstd)
                g_out[:, sl] = (back + grad.astype(F32)).astype(BF16)
            for k, steps in enumerate(slots[n]):
                pl.when(j == k)(lambda steps=steps: run_all(steps))
            return carry
        lax.fori_loop(0, 4, body, 0)
        base = LAST * UNIT + WIDE + n * WIDTH
        own[base:base + WIDTH, :] = du1[...].astype(BF16)
        own[base + TILE:base + TILE + WIDTH, :] = dv1[...].astype(BF16)
    links.start(LAST, PAIR_OUT)

    for k in range(1, DEVS):
        factor_copy(k).wait()

    def head_tile(c, carry):
        sl = pl.ds(pl.multiple_of(WIDE + c * WIDTH, WIDTH), WIDTH)
        total = jnp.zeros((WIDTH, WIDE), F32)
        for d in range(DEVS):
            total += dot_tn(factors[d, :, sl], factors[d, :, :WIDE]).astype(BF16).astype(F32)
        g_hd[pl.ds(pl.multiple_of(c * WIDTH, WIDTH), WIDTH), :] = total.astype(BF16)
        return carry
    half_tiles = CLASS_PAD // WIDTH // 2
    lax.fori_loop(0, half_tiles, head_tile, 0)
    run_all(((links.reduce_pair, LAST), (links.reduce_second, 5)))
    lax.fori_loop(half_tiles, 2 * half_tiles, head_tile, 0)
    run_all(((links.reduce_second, 6), (first, LAST)))
    for unit in range(SENT):
        links.wait(unit, SECOND_BACK)
    run_all(((links.reduce_second, 7), (links.reduce_second, LAST)))


def lars_matrix(steps, piece, scale, tails=()):
    def update_piece(w, v, g, b):
        new_v = MOMENTUM * v[...] + scale * g[...].astype(F32)
        new_w = w[...] - new_v
        v[...] = new_v
        w[...] = new_w
        b[...] = new_w.astype(BF16)

    def update(i, carry):
        update_piece(*piece(i))
        return carry
    lax.fori_loop(0, steps, update, 0)
    for tail in tails:
        update_piece(*tail)


def row_pieces(w, v, g, b, step):
    def piece(i):
        sl = pl.ds(pl.multiple_of(i * step, step), step)
        return w.at[sl], v.at[sl], g.at[sl], b.at[sl]
    return piece


def up_pieces(w, v, g, b):
    def piece(i):
        h, part = i // 2, lax.rem(i, 2)
        rows, cols = lanes(part, 256), lanes(h, 256)
        g_rows = pl.ds(pl.multiple_of(h * 512, 512), 256)
        return w.at[rows, cols], v.at[rows, cols], g.at[g_rows, rows], b.at[rows, cols]
    return piece


def down_pieces(w, v, g, b):
    def piece(i):
        h, part = i // 2, lax.rem(i, 2)
        rows = pl.ds(pl.multiple_of(i * 128, 128), 128)
        g_rows = pl.ds(pl.multiple_of(h * 512 + 256 + part * 128, 128), 128)
        return w.at[rows], v.at[rows], g.at[g_rows], b.at[rows]
    return piece


class Pair:
    def __init__(self, w, v, out_w, out_v, buf_w, buf_v, sems, scales, slot):
        self.buf_w, self.buf_v = buf_w, buf_v
        self.scale = scales.at[pl.ds(slot * SUBLANES, 1), pl.ds(0, 1)]
        ins = () if w is None else ((v, buf_v), (w, buf_w))
        self.loads, self.stores = ([pltpu.make_async_copy(src, dst, sems.at[slot, k, i]) for i, (src, dst) in enumerate(part)]
                                   for k, part in enumerate((ins, ((buf_w, out_w), (buf_v, out_v)))))

    def update(self, steps, make, grad, cast, *rest, tails=()):
        wait_all(self.loads)
        lars_matrix(steps, make(self.buf_w, self.buf_v, grad, cast, *rest), self.scale[...], tails)
        start_all(self.stores)


def gather_kernel(in_final, x_hbm, up1_hbm, dn1_hbm, mg_hbm, up2_hbm, dn2_hbm, vup1_hbm, vdn1_hbm, vmg_hbm, vup2_hbm, vdn2_hbm, g_hd, hd_hbm,
                  final, w_up1, w_dn1, w_mg, w_up2, w_dn2, v_up1, v_dn1, v_mg, v_up2, v_dn2, mid, scale_ref,
                  x_v, x_f32, r0, s1, up1, dn1, mg, gb_turn, st_hd, w_sums, g_sums, link_sems, sems):
    links = Links(None, final, None, None, link_sems)
    barrier = pltpu.get_barrier_semaphore()
    peers = (links.pair, links.x_peer, links.y_peer)
    for peer in peers:
        pl.semaphore_signal(barrier, inc=1, device_id=(peer,), device_id_type=pl.DeviceIdType.MESH)
    copies = [pltpu.make_async_copy(src, dst, sems.at[i]) for i, (src, dst) in enumerate((
        (x_hbm, x_v), (up1_hbm, w_up1), (dn1_hbm, w_dn1), (mg_hbm, w_mg), (vup1_hbm, v_up1), (vdn1_hbm, v_dn1), (vmg_hbm, v_mg),
        (up2_hbm, w_up2), (dn2_hbm, w_dn2), (hd_hbm, st_hd), (vup2_hbm, v_up2), (vdn2_hbm, v_dn2)))]
    start_all(copies[:7])
    pl.semaphore_wait(barrier, len(peers))
    links.start(LAST, SECOND_BACK)
    links.start(4, FIRST_BACK)
    g_sums[...] = jnp.zeros_like(g_sums)

    def finish(unit):
        links.wait(unit, PAIR_BACK)
        start = unit * UNIT
        if unit < LAST:
            for k in range(4):
                matrix = (6 if unit < HELD else 5) + 2 * (k % 2)
                g_sums[matrix] += square_sum(final, start + k * TILE, TILE, SHARD)
        else:
            g_sums[4] = square_sum(final, start, WIDE, SHARD)
            for k in range(4):
                g_sums[k] = square_sum(final, start + WIDE + k * WIDTH, WIDTH, SHARD)

    def weigh(matrix, total):
        w_sums[pl.ds(matrix * SUBLANES, SUBLANES), :] = jnp.broadcast_to(total_of(total), (SUBLANES, WIDTH))

    def scale_matrix(matrix):
        sl = pl.ds(matrix * SUBLANES, SUBLANES)
        scale = TRUST * (jnp.sqrt(w_sums[sl, :]) / jnp.sqrt(total_of(g_sums[matrix])))
        scale_ref[sl, :] = scale
        return scale[:1, :1]

    copies[0].wait()
    start_all(copies[7:])
    permute_tokens(x_v, x_f32, r0)
    wait_all(copies[1:7])
    for n in range(2):
        weigh(n, square_sum(w_up1.at[n], 0, WIDTH, SHARD))
        weigh(2 + n, square_sum(w_dn1.at[n], 0, WIDE, WIDTH))
    weigh(4, square_sum(w_mg, 0, WIDE, SHARD))
    links.back_first(LAST)
    for unit in range(SENT, LAST):
        links.start(unit, SECOND_BACK)
    run_all(((links.back_pair, 4), (links.back_pair, LAST), (links.back_first, 5), (finish, LAST), (links.back_first, 6)))
    small = final.at[pl.ds(LAST * UNIT, UNIT)]
    for n in range(2):
        grad = small.at[pl.ds(WIDE + n * WIDTH, WIDTH)]
        lars_matrix(2, row_pieces(w_up1.at[n], v_up1.at[n], grad, up1.at[n], SHARD), scale_matrix(n))
        gb_turn[...] = small[pl.ds(WIDE + TILE + n * WIDTH, WIDTH), :].astype(F32).T
        lars_matrix(4, row_pieces(w_dn1.at[n], v_dn1.at[n], gb_turn, dn1.at[n], WIDTH), scale_matrix(2 + n))
    lars_matrix(8, row_pieces(w_mg, v_mg, small.at[pl.ds(0, WIDE)], mg, SHARD), scale_matrix(4))
    links.back_first(7)
    for unit in range(HELD):
        links.start(unit, FIRST_BACK)
    stage_one_forward(r0, mid, s1, up1, dn1, slots=((), ((links.back_pair, 5), (finish, 4)), ((links.back_pair, 6),), ((links.back_pair, 7), (finish, 5))))
    mid[...] = dot_nn(s1[...], mg[...]).astype(BF16)
    wait_all(copies[7:])
    run_all(((finish, 6), (links.back_pair, 0), (finish, 7)))
    for n in range(2):
        weigh(5 + n, square_sum(w_up2.at[n], 0, WIDE, 16))
        weigh(7 + n, square_sum(w_dn2.at[n], 0, HID_TWO, SHARD))
        scale_matrix(5) if n else None
        links.back_pair(1 + n)
    weigh(9, square_sum(st_hd, 0, 992, 32) + square_sum(st_hd, 992, SUBLANES, SUBLANES))
    g_sums[9] = square_sum(g_hd, 0, CLASS_PAD, SHARD)
    run_all(((finish, 0), (links.back_pair, 3), (finish, 1), (finish, 2), (finish, 3)))
    for matrix in range(6, MATRICES):
        scale_matrix(matrix)


def next_kernel(hd_hbm, vhd_hbm, sums, g_hd, mid, scales, w_up1, w_dn1, w_mg, v_up1, v_dn1, v_mg, in_wu, in_wd, in_vu, in_vd,
                logits_ref, o_up1, o_dn1, o_mg, o_up2, o_dn2, o_hd, ov_up1, ov_dn1, ov_mg, ov_up2, ov_dn2, ov_hd,
                w_up2, w_dn2, v_up2, v_dn2,
                wb_hd, vb_hd, up2, dn2, hd, s1, normed_ref, acc, sems, small_sems):
    wide_ups = [Pair(None, None, o_up2.at[n], ov_up2.at[n], w_up2.at[n], v_up2.at[n], sems, scales, 5 + n) for n in range(2)]
    wide_downs = [Pair(None, None, o_dn2.at[n], ov_dn2.at[n], w_dn2.at[n], v_dn2.at[n], sems, scales, 7 + n) for n in range(2)]
    head = Pair(hd_hbm, vhd_hbm, o_hd, ov_hd, wb_hd, vb_hd, sems, scales, 9)
    start_all(head.loads)
    done = [pltpu.make_async_copy(src, dst, small_sems.at[i]) for i, (src, dst) in enumerate((
        (w_up1, o_up1), (w_dn1, o_dn1), (w_mg, o_mg), (v_up1, ov_up1), (v_dn1, ov_dn1), (v_mg, ov_mg)))]
    start_all(done)
    for n, (src, dst) in enumerate(((mid, s1), (s1, s1))):
        grads = sums.at[pl.ds((1 - n) * HELD * UNIT, HELD * UNIT)]
        wide_ups[n].update(16, up_pieces, grads, up2)
        wide_downs[n].update(16, down_pieces, grads, dn2)
        if n == 0:
            tail = pl.ds(992, SUBLANES)
            head.update(31, row_pieces, g_hd, hd, 32, tails=[(wb_hd.at[tail], vb_hd.at[tail], g_hd.at[tail], hd.at[tail])])
        stage_two_block(src, dst, normed_ref, acc, up2, dn2)
    head_b = pooled_norm(s1[...])[0].astype(BF16)
    logits_ref[...] = dot_nt(head_b, hd[...])[:IMGS]
    wait_all(done)
    for each in [head] + wide_ups + wide_downs:
        wait_all(each.stores)


W_SHAPES = ((2, 128, 512), (2, 512, 128), (512, 512), (2, 512, 2048), (2, 2048, 512), (CLASSES, 512))
BUF_SHAPES = W_SHAPES[:3] + ((512, 2048), (2048, 512), (CLASSES, 512))


def vmem(shape, dtype):
    return pltpu.VMEM(shape, dtype)


ANY_SPEC = pl.BlockSpec(memory_space=pl.ANY)
VMEM_SPEC = pl.BlockSpec(memory_space=pltpu.VMEM)


def act(dtype=BF16):
    return vmem((ROWS, WIDE), dtype)


def f32_outs(shapes):
    return [jax.ShapeDtypeStruct(shape, F32) for shape in shapes]


DMA = pltpu.SemaphoreType.DMA


SUMS = (SHARE_ROWS, WIDE), BF16
HEAD_SUM = (CLASS_PAD, WIDE), BF16
ROW_BLOCK = (ROWS, WIDE), BF16
WEIGHTS = tuple((shape, F32) for shape in W_SHAPES[:5])


def keep(arrays):
    return [pltpu.with_memory_space_constraint(each, pltpu.VMEM) for each in arrays]


def run_train(x_now, labels, params):
    return pl.pallas_call(
        train_kernel,
        out_shape=[vmem(*SUMS), vmem(*HEAD_SUM)],
        in_specs=[ANY_SPEC] + [pl.BlockSpec(memory_space=pltpu.SMEM)] + [ANY_SPEC] * 6,
        out_specs=[VMEM_SPEC] * 2,
        scratch_shapes=[vmem((ROWS * 4, WIDTH), BF16), vmem((ROWS * 4, WIDTH), F32)]
        + [vmem(shape, F32) for shape in BUF_SHAPES[:5]] + [act()]
        + [vmem(shape, BF16) for shape in W_SHAPES[:5]] + [vmem((CLASS_PAD, WIDE), BF16)]
        + [act()] * 5 + [act(F32), act(), act(), DMA((9,)), vmem((WIDTH, WIDE), F32), vmem((WIDTH, WIDE), F32)]
        + [vmem((rows, WIDE), BF16) for rows in (SHARE_ROWS, N_UNITS * TILE, N_UNITS * WIDTH)]
        + [vmem((DEVS, SUBLANES, WIDE + CLASS_PAD), BF16)]
        + [DMA((N_UNITS, 6, 2, 2)), DMA((DEVS, 2))],
        compiler_params=pltpu.CompilerParams(vmem_limit_bytes=VMEM_BYTES - 11_000_000, collective_id=0, has_side_effects=True),
        cost_estimate=pl.CostEstimate(flops=30_000_000_000, bytes_accessed=40_000_000, transcendentals=0),
        name='train_part',
    )(x_now, labels, *params)


def run_gather(sums, head_sum, x_next, params, velocities):
    sums, head_sum = keep((sums, head_sum))
    return pl.pallas_call(
        gather_kernel,
        out_shape=[vmem(*each) for each in (SUMS, *WEIGHTS, *WEIGHTS, ROW_BLOCK)] + f32_outs([(MATRICES * SUBLANES, WIDTH)]),
        in_specs=[VMEM_SPEC] + [ANY_SPEC] * 11 + [VMEM_SPEC, ANY_SPEC],
        out_specs=[VMEM_SPEC] * 13,
        scratch_shapes=[vmem((ROWS * 4, WIDTH), BF16), vmem((ROWS * 4, WIDTH), F32), act(), act()]
        + [vmem(shape, BF16) for shape in BUF_SHAPES[:3]] + [vmem((WIDE, WIDTH), F32), vmem((CLASSES, WIDE), F32)]
        + [vmem((MATRICES * SUBLANES, WIDTH), F32), vmem((MATRICES, SUBLANES, WIDE), F32), DMA((N_UNITS, 6, 2, 2)), DMA((12,))],
        input_output_aliases={0: 0},
        compiler_params=pltpu.CompilerParams(vmem_limit_bytes=GATHER_BYTES, collective_id=1, has_side_effects=True),
        cost_estimate=pl.CostEstimate(flops=10_000_000_000, bytes_accessed=40_000_000, transcendentals=0),
        name='gather_part',
    )(sums, x_next, *params[:5], *velocities[:5], head_sum, params[5])


GATHER_BYTES = 17_000_000
NEXT_BYTES = 17_500_000


def run_next(head, vel_head, head_sum, gathered):
    sums, w_up1, w_dn1, w_mg, w_up2, w_dn2, v_up1, v_dn1, v_mg, v_up2, v_dn2, mid, scales = gathered
    held = keep((w_up2, w_dn2, v_up2, v_dn2))
    outs = pl.pallas_call(
        next_kernel,
        out_shape=f32_outs([(IMGS, CLASSES)] + list(W_SHAPES) * 2) + [vmem(*each) for each in WEIGHTS[3:] * 2],
        in_specs=[ANY_SPEC] * 2 + [VMEM_SPEC] * 14,
        out_specs=[VMEM_SPEC] + [ANY_SPEC] * 12 + [VMEM_SPEC] * 4,
        scratch_shapes=[vmem((CLASSES, WIDE), F32)] * 2 + [vmem(shape, BF16) for shape in BUF_SHAPES[3:]]
        + [act()] * 2 + [act(F32), DMA((10, 2, 2)), DMA((6,))],
        input_output_aliases={12 + i: 13 + i for i in range(4)},
        compiler_params=pltpu.CompilerParams(vmem_limit_bytes=NEXT_BYTES),
        cost_estimate=pl.CostEstimate(flops=10_000_000_000, bytes_accessed=50_000_000, transcendentals=0),
        name='next_part',
    )(head, vel_head, *keep((sums, head_sum, mid)), scales, *keep((w_up1, w_dn1, w_mg, v_up1, v_dn1, v_mg)), *held)
    return outs[:13]


def turn_head(arrays):
    return (*arrays[:5], arrays[5].T)


def solution(mesh):
    def local_step(x_now, labels_now, x_next, *weights):
        params, velocities = turn_head(weights[:6]), turn_head(weights[6:])
        sums, head_sum = run_train(x_now.reshape(ROWS * 4, WIDTH), labels_now, params)
        gathered = run_gather(sums, head_sum, x_next.reshape(ROWS * 4, WIDTH), params, velocities)
        outs = run_next(params[5], velocities[5], head_sum, gathered)
        return (outs[0], *turn_head(outs[1:7]), *turn_head(outs[7:]))

    split = P('data')
    in_specs = (split, split, split) + (P(),) * 12
    out_specs = (split,) + (P(),) * 12
    return jax.shard_map(local_step, mesh=mesh, in_specs=in_specs, out_specs=out_specs, check_vma=False)
```

```python
import jax
import jax.numpy as jnp
from jax import lax
from jax.experimental import pallas as pl
from jax.experimental.pallas import tpu as pltpu
from jax.sharding import PartitionSpec as P

MOMENTUM = 0.9
TRUST = 0.1
LN_EPS = 1e-6
GELU_A = 0.7978845608028654
GELU_B = 0.044715 * GELU_A
F32 = jnp.float32
BF16 = jnp.bfloat16
VMEM_BYTES = 66_000_000

IMGS, TOKENS, WIDTH = 4, 784, 128
MERGED = TOKENS // 4
ROWS = IMGS * MERGED
WIDE = 4 * WIDTH
HID_ONE, HID_TWO = 4 * WIDTH, 4 * WIDE
CLASSES = 1000
TILE = 256
SHARD = 64
N_TILES = HID_TWO // TILE
FWD_TILE = 512


def dot_nn(a, b):
    return lax.dot_general(a, b, (((1,), (0,)), ((), ())), preferred_element_type=F32)


def dot_nt(a, b):
    return lax.dot_general(a, b, (((1,), (1,)), ((), ())), preferred_element_type=F32)


def dot_tn(a, b):
    return lax.dot_general(a, b, (((0,), (0,)), ((), ())), preferred_element_type=F32)


def norm_parts(vals):
    centered = vals - jnp.mean(vals, axis=-1, keepdims=True)
    variance = jnp.mean(centered * centered, axis=-1, keepdims=True)
    rstd = lax.rsqrt(variance + LN_EPS)
    return centered * rstd, rstd


def norm_back(grad, normed, rstd):
    mean_g = jnp.mean(grad, axis=-1, keepdims=True)
    mean_gn = jnp.mean(grad * normed, axis=-1, keepdims=True)
    return rstd * (grad - mean_g - normed * mean_gn)


def gelu_parts(pre):
    square = pre * pre
    half = 0.5 * jnp.tanh(pre * (GELU_A + GELU_B * square)) + 0.5
    return square, half


def gelu_slope(pre, square, half):
    return half * (1.0 + pre * (1.0 - half) * (2.0 * GELU_A + 6.0 * GELU_B * square))


def cast_rows(dst, src, rows, step):
    def body(i, carry):
        sl = pl.ds(pl.multiple_of(i * step, step), step)
        dst[sl, :] = src[sl, :].astype(BF16)
        return carry
    lax.fori_loop(0, rows // step, body, 0)


def lanes(index, size):
    return pl.ds(pl.multiple_of(index * size, size), size)


def permute_tokens(x_ref, x_f32, r0):
    x_f32[...] = x_ref[...].astype(F32)
    for j in range(4):
        r0[:, j * WIDTH:(j + 1) * WIDTH] = x_f32[pl.ds(j, ROWS, stride=4), :].astype(BF16)


def stage_one_block(resid, w_up, w_down):
    res_f = resid.astype(F32)
    normed = norm_parts(res_f)[0].astype(BF16)
    pre = dot_nn(normed, w_up)
    act = (pre * gelu_parts(pre)[1]).astype(BF16)
    return (res_f + dot_nn(act, w_down)).astype(BF16)


def stage_one_forward(r0, r1, r2, up_one, down_one):
    def body(j, carry):
        cuts = [lanes(2 * j + k, WIDTH) for k in range(2)]
        mids = [stage_one_block(r0[:, sl], up_one[0], down_one[0]) for sl in cuts]
        for sl, mid in zip(cuts, mids):
            r1[:, sl] = mid
        for sl, mid in zip(cuts, mids):
            r2[:, sl] = stage_one_block(mid, up_one[1], down_one[1])
        return carry
    lax.fori_loop(0, 2, body, 0)


def stage_two_block(src, dst, normed_ref, acc, up_ref, down_ref):
    res_f = src[...].astype(F32)
    normed_ref[...] = norm_parts(res_f)[0].astype(BF16)
    acc[...] = res_f

    def body(t, carry):
        sl = lanes(t, FWD_TILE)
        pre = dot_nn(normed_ref[...], up_ref[:, sl])
        act = (pre * gelu_parts(pre)[1]).astype(BF16)
        acc[...] += dot_nn(act, down_ref[sl, :])
        return carry
    lax.fori_loop(0, HID_TWO // FWD_TILE, body, 0)
    dst[...] = acc[...].astype(BF16)


def image_rows():
    image = lax.broadcasted_iota(jnp.int32, (8, ROWS), 0)
    row = lax.broadcasted_iota(jnp.int32, (8, ROWS), 1)
    inside = (row >= image * MERGED) & (row < (image + 1) * MERGED)
    return jnp.where(inside, 1.0, 0.0).astype(BF16)


def pooled_norm(resid):
    pooled = dot_nn(image_rows(), resid) * (1.0 / MERGED)
    return norm_parts(pooled)


UNIT = 1024
N_UNITS = 9
SHARE_ROWS = N_UNITS * UNIT
CLASS_PAD = 1024
DEVS = 8
SUBLANES = 8
LAST = N_UNITS - 1
HELD = 4
MATRICES = 10
PAIR_OUT, FIRST_OUT, SECOND_OUT, SECOND_BACK, FIRST_BACK, PAIR_BACK = range(6)


def start_all(copies):
    for copy in copies:
        copy.start()


def wait_all(copies):
    for copy in copies:
        copy.wait()


def sum_rows(tile):
    rows, cols = tile.shape
    return jnp.sum(tile.reshape(rows // 8, 8, cols), axis=0)


def square_sum(ref, start, rows, step):
    def body(i, total):
        part = ref[pl.ds(pl.multiple_of(start + i * step, step), step), :].astype(F32)
        return total + sum_rows(part * part)
    return lax.fori_loop(0, rows // step, body, jnp.zeros((SUBLANES, ref.shape[1]), F32))


def total_of(tile):
    return jnp.sum(jnp.sum(tile, axis=0, keepdims=True), axis=1, keepdims=True)


class Links:
    def __init__(self, own, final, land1, land2, sems):
        self.own, self.final, self.land1, self.land2, self.sems = own, final, land1, land2, sems
        me = lax.axis_index('data')
        self.me = me
        self.core, self.x, self.y = lax.rem(me, 2), lax.rem(me // 2, 2), me // 4
        self.pair = me + 1 - 2 * self.core
        self.x_peer = me + 2 - 4 * self.x
        self.y_peer = me + 4 - 8 * self.y

    def rows(self, unit, offset, size):
        return pl.ds(pl.multiple_of(unit * UNIT + offset, SHARD), size)

    def half(self, unit, offset, size):
        return self.rows(unit, self.core * WIDE + offset, size)

    def copy(self, unit, phase, lane, src, dst, peer):
        return pltpu.make_async_remote_copy(
            src_ref=src, dst_ref=dst, send_sem=self.sems.at[unit, phase, lane, 0], recv_sem=self.sems.at[unit, phase, lane, 1],
            device_id=(peer,), device_id_type=pl.DeviceIdType.MESH)

    def copies(self, unit, phase):
        x, y = self.x, self.y
        own, final = self.own, self.final
        if phase == PAIR_OUT:
            sl = self.rows(unit, (1 - self.core) * WIDE, WIDE)
            return [self.copy(unit, PAIR_OUT, 0, own.at[sl], final.at[sl], self.pair)]
        if phase == FIRST_OUT:
            land = lambda k: self.land1.at[pl.ds(pl.multiple_of(unit * TILE + k * WIDTH, WIDTH), WIDTH)]
            return [self.copy(unit, FIRST_OUT, 0, own.at[self.half(unit, (1 - x) * WIDTH, WIDTH)], land(0), self.x_peer),
                    self.copy(unit, FIRST_OUT, 1, own.at[self.half(unit, TILE + (1 - y) * WIDTH, WIDTH)], land(1), self.y_peer)]
        if phase == SECOND_OUT:
            land = lambda k: self.land2.at[pl.ds(pl.multiple_of(unit * WIDTH + k * SHARD, SHARD), SHARD)]
            return [self.copy(unit, SECOND_OUT, 0, own.at[self.half(unit, x * WIDTH + (1 - y) * SHARD, SHARD)], land(0), self.y_peer),
                    self.copy(unit, SECOND_OUT, 1, own.at[self.half(unit, TILE + y * WIDTH + (1 - x) * SHARD, SHARD)], land(1), self.x_peer)]
        if phase == SECOND_BACK:
            first = self.half(unit, x * WIDTH + y * SHARD, SHARD)
            second = self.half(unit, TILE + y * WIDTH + x * SHARD, SHARD)
            return [self.copy(unit, SECOND_BACK, 0, final.at[first], final.at[first], self.y_peer),
                    self.copy(unit, SECOND_BACK, 1, final.at[second], final.at[second], self.x_peer)]
        if phase == FIRST_BACK:
            first, second = self.half(unit, x * WIDTH, WIDTH), self.half(unit, TILE + y * WIDTH, WIDTH)
            return [self.copy(unit, FIRST_BACK, 0, final.at[first], final.at[first], self.x_peer),
                    self.copy(unit, FIRST_BACK, 1, final.at[second], final.at[second], self.y_peer)]
        sl = self.half(unit, 0, WIDE)
        return [self.copy(unit, PAIR_BACK, 0, final.at[sl], final.at[sl], self.pair)]

    def start(self, unit, phase):
        for copy in self.copies(unit, phase):
            copy.start()

    def wait(self, unit, phase):
        for copy in self.copies(unit, phase):
            copy.wait()

    def reduce_pair(self, unit):
        self.wait(unit, PAIR_OUT)
        x, y = self.x, self.y
        for offset in ((1 - x) * WIDTH, TILE + (1 - y) * WIDTH, x * WIDTH, TILE + y * WIDTH):
            sl = self.half(unit, offset, WIDTH)
            self.own[sl, :] = self.own[sl, :] + self.final[sl, :]
        self.start(unit, FIRST_OUT)

    def reduce_first(self, unit):
        self.wait(unit, FIRST_OUT)
        x, y = self.x, self.y
        for keep in (False, True):
            for lane, base, here, there in ((0, x * WIDTH, y, 0), (1, TILE + y * WIDTH, x, WIDTH)):
                part = here if keep else 1 - here
                sl = self.half(unit, base + part * SHARD, SHARD)
                land = pl.ds(pl.multiple_of(unit * TILE + there + part * SHARD, SHARD), SHARD)
                self.own[sl, :] = self.own[sl, :] + self.land1[land, :]
        self.start(unit, SECOND_OUT)

    def reduce_second(self, unit):
        self.wait(unit, SECOND_OUT)
        for lane, offset in ((0, self.x * WIDTH + self.y * SHARD), (1, TILE + self.y * WIDTH + self.x * SHARD)):
            sl = self.half(unit, offset, SHARD)
            land = pl.ds(pl.multiple_of(unit * WIDTH + lane * SHARD, SHARD), SHARD)
            self.final[sl, :] = self.own[sl, :] + self.land2[land, :]

    def forward(self, unit, phase):
        self.wait(unit, phase)
        self.start(unit, phase + 1)


def train_kernel(x_hbm, x_next_hbm, labels_ref, up1_hbm, dn1_hbm, mg_hbm, up2_hbm, dn2_hbm, hd_hbm,
                 final, st_up1, st_dn1, st_mg, st_up2, st_dn2, r0, g_hd, scale_ref,
                 x_v, x_f32,
                 up1, dn1, mg, up2, dn2, hd,
                 r1, r2, s0, s1, normed_ref, acc, grad_a, grad_b, sems,
                 du1, dv1, own, land1, land2, factors, w_sums, g_sums, link_sems, factor_sems):
    links = Links(own, final, land1, land2, link_sems)
    me = links.me
    st_hd = st_dn2.at[pl.ds(0, CLASSES)]
    copies = [pltpu.make_async_copy(src, dst, sems.at[i]) for i, (src, dst) in enumerate((
        (x_hbm, x_v), (up1_hbm, st_up1), (dn1_hbm, st_dn1), (mg_hbm, st_mg),
        (up2_hbm.at[0], st_up2), (dn2_hbm.at[0], st_dn2),
        (up2_hbm.at[1], st_up2), (dn2_hbm.at[1], st_dn2), (hd_hbm, st_hd)))]
    start_all(copies[:3])
    barrier = pltpu.get_barrier_semaphore()
    for k in range(1, DEVS):
        pl.semaphore_signal(barrier, inc=1, device_id=(lax.rem(me + k, DEVS),), device_id_type=pl.DeviceIdType.MESH)
    copies[0].wait()
    permute_tokens(x_v, x_f32, r0)
    wait_all(copies[1:3])
    start_all(copies[3:6])
    for n in range(2):
        cast_rows(up1.at[n], st_up1.at[n], WIDTH, SHARD)
        cast_rows(dn1.at[n], st_dn1.at[n], WIDE, TILE)
    stage_one_forward(r0, r1, r2, up1, dn1)
    copies[3].wait()
    cast_rows(mg, st_mg, WIDE, SHARD)
    s0[...] = dot_nn(r2[...], mg[...]).astype(BF16)
    s2 = grad_a
    for n, (src, dst) in enumerate(((s0, s1), (s1, s2))):
        copies[4 + 2 * n].wait()
        cast_rows(up2.at[n], st_up2, WIDE, 16)
        if n == 0:
            copies[6].start()
        copies[5 + 2 * n].wait()
        cast_rows(dn2.at[n], st_dn2, 2048, SHARD)
        copies[7 + n].start()
        stage_two_block(src, dst, normed_ref, acc, up2.at[n], dn2.at[n])
    copies[8].wait()
    cast_rows(hd, st_hd, 992, 32)
    hd[992:CLASSES, :] = st_hd[992:CLASSES, :].astype(BF16)
    hd[CLASSES:, :] = jnp.zeros((CLASS_PAD - CLASSES, WIDE), BF16)
    head_normed, head_rstd = pooled_norm(s2[...])
    head_b = head_normed.astype(BF16)
    class_id = lax.broadcasted_iota(jnp.int32, (SUBLANES, CLASS_PAD), 1)
    row_id = lax.broadcasted_iota(jnp.int32, (SUBLANES, CLASS_PAD), 0)
    logits = jnp.where(class_id < CLASSES, dot_nt(head_b, hd[...]), -jnp.inf)
    top = jnp.max(logits, axis=-1, keepdims=True)
    expd = jnp.exp(logits - top)
    probs = expd / jnp.sum(expd, axis=-1, keepdims=True)
    label = jnp.zeros((SUBLANES, CLASS_PAD), jnp.int32)
    for i in range(IMGS):
        label = jnp.where(row_id == i, labels_ref[i], label)
    onehot = jnp.where(class_id == label, 1.0, 0.0)
    grad_logits = jnp.where(row_id < IMGS, (probs - onehot) * (1.0 / (IMGS * DEVS)), 0.0).astype(BF16)
    factors[me, :, :WIDE] = head_b
    factors[me, :, WIDE:] = grad_logits
    grad_pooled = norm_back(dot_nn(grad_logits, hd[...]), head_normed, head_rstd) * (1.0 / MERGED)
    grad_a[...] = dot_tn(image_rows(), grad_pooled.astype(BF16)).astype(BF16)

    pl.semaphore_wait(barrier, DEVS - 1)

    def factor_copy(k):
        return pltpu.make_async_remote_copy(
            src_ref=factors.at[me], dst_ref=factors.at[me], send_sem=factor_sems.at[k, 0], recv_sem=factor_sems.at[k, 1],
            device_id=(lax.rem(me + k, DEVS),), device_id_type=pl.DeviceIdType.MESH)

    grads = (grad_a, grad_b)
    for step, n in enumerate((1, 0)):
        g_in, g_out = grads[step], grads[1 - step]
        src = (s0, s1)[n]
        normed_ref[...] = norm_parts(src[...].astype(F32))[0].astype(BF16)
        acc[...] = jnp.zeros_like(acc)

        def tile(t, row, n=n, g_in=g_in):
            sl = lanes(t, TILE)
            pre = dot_nn(normed_ref[...], up2[n, :, sl])
            square, half = gelu_parts(pre)
            act = (pre * half).astype(BF16)
            grad_pre = (gelu_slope(pre, square, half) * dot_nt(g_in[...], dn2[n, sl, :])).astype(BF16)
            own[pl.ds(row + TILE, TILE), :] = dot_tn(act, g_in[...]).astype(BF16)
            grad_up = dot_tn(normed_ref[...], grad_pre).astype(BF16)
            own[pl.ds(row, TILE), :TILE] = grad_up[:TILE]
            own[pl.ds(row, TILE), TILE:] = grad_up[TILE:]
            acc[...] += dot_nt(grad_pre, up2[n, :, sl])

        def body(p, carry, step=step, tile=tile):
            unit = step * 4 + p
            row = pl.multiple_of(unit * UNIT, UNIT)

            tile(2 * p, row)
            if step:
                links.reduce_pair(unit - 1)
            else:
                pl.when(p > 0)(lambda: links.reduce_pair(unit - 1))
            tile(2 * p + 1, row + WIDE)
            if step:
                links.reduce_first(unit - 4)
            links.start(unit, PAIR_OUT)
            return carry
        if step == 0:
            for k in range(1, DEVS):
                factor_copy(k).start()
        lax.fori_loop(0, N_TILES // 2, body, 0)
        normed_f, rstd = norm_parts(src[...].astype(F32))
        g_out[...] = (norm_back(acc[...], normed_f, rstd) + g_in[...].astype(F32)).astype(BF16)
    own[LAST * UNIT:LAST * UNIT + WIDE, :] = dot_tn(r2[...], grad_a[...]).astype(BF16)
    grad_b[...] = dot_nt(grad_a[...], mg[...]).astype(BF16)

    def reduced(unit):
        links.reduce_second(unit)
        links.start(unit, SECOND_BACK)

    def finish(unit):
        links.wait(unit, PAIR_BACK)
        start = unit * UNIT
        if unit < LAST:
            for k in range(4):
                matrix = (6 if unit < HELD else 5) + 2 * (k % 2)
                g_sums[matrix] += square_sum(final, start + k * TILE, TILE, SHARD)
        else:
            g_sums[4] = square_sum(final, start, WIDE, SHARD)
            for k in range(4):
                g_sums[k] = square_sum(final, start + WIDE + k * WIDTH, WIDTH, SHARD)

    def weigh(matrix, ref, rows, step):
        w_sums[pl.ds(matrix * SUBLANES, SUBLANES), :] = jnp.broadcast_to(total_of(square_sum(ref, 0, rows, step)), (SUBLANES, WIDTH))

    reloads = [pltpu.make_async_copy(src, dst, sems.at[9 + i]) for i, (src, dst) in enumerate((
        (up2_hbm.at[0], st_up2), (dn2_hbm.at[1], st_dn2), (x_next_hbm, x_v), (dn2_hbm.at[0], st_dn2)))]

    def weigh_small(_):
        for n in range(2):
            weigh(n, st_up1.at[n], WIDTH, SHARD)
            weigh(2 + n, st_dn1.at[n], WIDE, WIDTH)
        weigh(4, st_mg, WIDE, SHARD)
        weigh(6, st_up2, WIDE, 16)
        w_hd = square_sum(st_dn2, 0, 992, 32) + square_sum(st_dn2, 992, SUBLANES, SUBLANES)
        w_sums[pl.ds(9 * SUBLANES, SUBLANES), :] = jnp.broadcast_to(total_of(w_hd), (SUBLANES, WIDTH))
        start_all(reloads[:3])

    def weigh_first(_):
        wait_all(reloads[:3])
        weigh(5, st_up2, WIDE, 16)
        weigh(8, st_dn2, HID_TWO, SHARD)
        reloads[3].start()
        permute_tokens(x_v, x_f32, r0)

    def weigh_second(_):
        reloads[3].wait()
        weigh(7, st_dn2, HID_TWO, SHARD)
        g_sums[9] = square_sum(g_hd, 0, CLASS_PAD, SHARD)

    def back_first(unit):
        links.forward(unit, SECOND_BACK)

    def back_pair(unit):
        links.forward(unit, FIRST_BACK)

    def run_all(steps):
        for action, unit in steps:
            action(unit)

    g_sums[...] = jnp.zeros_like(g_sums)
    links.reduce_pair(7)
    first = links.reduce_first
    slots = {1: (((reduced, 0), (reduced, 1), (reduced, 2), (first, 4)), ((first, 5),), ((reduced, 3),), ((first, 6), (back_first, 0))),
             0: (((back_first, 1),), ((back_first, 2),), ((reduced, 4),), ((first, 7),))}

    for n, src, g_in, g_out in ((1, r1, grad_b, grad_a), (0, r0, grad_a, grad_b)):
        du1[...] = jnp.zeros_like(du1)
        dv1[...] = jnp.zeros_like(dv1)

        def body(j, carry, n=n, src=src, g_in=g_in, g_out=g_out):
            sl = lanes(j, WIDTH)
            normed_f, rstd = norm_parts(src[:, sl].astype(F32))
            normed = normed_f.astype(BF16)
            grad = g_in[:, sl]
            pre = dot_nn(normed, up1[n])
            square, half = gelu_parts(pre)
            act = (pre * half).astype(BF16)
            grad_pre = (gelu_slope(pre, square, half) * dot_nt(grad, dn1[n])).astype(BF16)
            dv1[...] += dot_tn(grad, act)
            du1[...] += dot_tn(normed, grad_pre)
            if n:
                back = norm_back(dot_nt(grad_pre, up1[n]), normed_f, rstd)
                g_out[:, sl] = (back + grad.astype(F32)).astype(BF16)
            for k, steps in enumerate(slots[n]):
                pl.when(j == k)(lambda steps=steps: run_all(steps))
            return carry
        lax.fori_loop(0, 4, body, 0)
        base = LAST * UNIT + WIDE + n * WIDTH
        own[base:base + WIDTH, :] = du1[...].astype(BF16)
        own[base + TILE:base + TILE + WIDTH, :] = dv1[...].astype(BF16)
    links.start(LAST, PAIR_OUT)

    for k in range(1, DEVS):
        factor_copy(k).wait()

    def head_tile(c, carry):
        sl = pl.ds(pl.multiple_of(WIDE + c * WIDTH, WIDTH), WIDTH)
        total = jnp.zeros((WIDTH, WIDE), F32)
        for d in range(DEVS):
            total += dot_tn(factors[d, :, sl], factors[d, :, :WIDE]).astype(BF16).astype(F32)
        g_hd[pl.ds(pl.multiple_of(c * WIDTH, WIDTH), WIDTH), :] = total.astype(BF16)
        return carry
    half_tiles = CLASS_PAD // WIDTH // 2
    lax.fori_loop(0, half_tiles, head_tile, 0)
    run_all(((links.reduce_pair, LAST), (reduced, 5), (back_first, 3)))
    lax.fori_loop(half_tiles, 2 * half_tiles, head_tile, 0)
    run_all(((reduced, 6), (weigh_small, 0), (first, LAST), (weigh_first, 0), (back_pair, 0), (back_pair, 1), (finish, 0), (weigh_second, 0), (back_pair, 2), (finish, 1), (reduced, 7),
             (reduced, LAST), (back_first, 4), (finish, 2), (back_first, 5), (back_pair, 3), (back_first, 6), (back_first, LAST),
             (finish, 3), (back_pair, 4), (back_first, 7), (back_pair, 5), (finish, 4), (back_pair, LAST), (back_pair, 6), (finish, 5),
             (finish, LAST), (back_pair, 7), (finish, 6), (finish, 7)))
    for matrix in range(MATRICES):
        sl = pl.ds(matrix * SUBLANES, SUBLANES)
        scale_ref[sl, :] = TRUST * (jnp.sqrt(w_sums[sl, :]) / jnp.sqrt(total_of(g_sums[matrix])))


def lars_matrix(steps, piece, scale, tails=()):
    def update_piece(w, v, g, b):
        new_v = MOMENTUM * v[...] + scale * g[...].astype(F32)
        new_w = w[...] - new_v
        v[...] = new_v
        w[...] = new_w
        if b is not None:
            b[...] = new_w.astype(BF16)

    def update(i, carry):
        update_piece(*piece(i))
        return carry
    lax.fori_loop(0, steps, update, 0)
    for tail in tails:
        update_piece(*tail)


def row_pieces(w, v, g, b, step):
    def piece(i):
        sl = pl.ds(pl.multiple_of(i * step, step), step)
        return w.at[sl], v.at[sl], g.at[sl], b.at[sl]
    return piece


def up_pieces(w, v, g, b):
    def piece(i):
        h, part = i // 2, lax.rem(i, 2)
        rows, cols = lanes(part, 256), lanes(h, 256)
        g_rows = pl.ds(pl.multiple_of(h * 512, 512), 256)
        return w.at[rows, cols], v.at[rows, cols], g.at[g_rows, rows], b if b is None else b.at[rows, cols]
    return piece


def down_pieces(w, v, g, b):
    def piece(i):
        h, part = i // 2, lax.rem(i, 2)
        rows = pl.ds(pl.multiple_of(i * 128, 128), 128)
        g_rows = pl.ds(pl.multiple_of(h * 512 + 256 + part * 128, 128), 128)
        return w.at[rows], v.at[rows], g.at[g_rows], b if b is None else b.at[rows]
    return piece


class Pair:
    def __init__(self, w, v, out_w, out_v, buf_w, buf_v, sems, scales, slot):
        self.buf_w, self.buf_v = buf_w, buf_v
        self.scale = scales.at[pl.ds(slot * SUBLANES, 1), pl.ds(0, 1)]
        ins = ((v, buf_v),) if w is None else ((v, buf_v), (w, buf_w))
        self.loads, self.stores = ([pltpu.make_async_copy(src, dst, sems.at[slot, k, i]) for i, (src, dst) in enumerate(part)]
                                   for k, part in enumerate((ins, ((buf_w, out_w), (buf_v, out_v)))))

    def update(self, steps, make, grad, cast, *rest, tails=()):
        wait_all(self.loads)
        lars_matrix(steps, make(self.buf_w, self.buf_v, grad, cast, *rest), self.scale[...], tails)
        start_all(self.stores)


def next_kernel(up2_hbm, dn2_hbm, hd_hbm, vup1_hbm, vdn1_hbm, vmg_hbm, vup2_hbm, vdn2_hbm, vhd_hbm,
                sums, in_up1, in_dn1, in_mg, in_up2, in_dn2, r0, g_hd, scales,
                logits_ref, o_up1, o_dn1, o_mg, o_up2, o_dn2, o_hd, ov_up1, ov_dn1, ov_mg, ov_up2, ov_dn2, ov_hd,
                w_up1, w_dn1, w_mg, w_up2, w_dn2,
                vb_up1, vb_dn1, vb_mg, vb_up2, vb_dn2, wb_up2, wb_dn2,
                gb_turn, up1, dn1, mg, up2, dn2, hd, s0, s1, normed_ref, acc, sems):
    ups = [Pair(None, vup1_hbm.at[n], o_up1.at[n], ov_up1.at[n], w_up1.at[n], vb_up1.at[n], sems, scales, n) for n in range(2)]
    downs = [Pair(None, vdn1_hbm.at[n], o_dn1.at[n], ov_dn1.at[n], w_dn1.at[n], vb_dn1.at[n], sems, scales, 2 + n) for n in range(2)]
    merge = Pair(None, vmg_hbm, o_mg, ov_mg, w_mg, vb_mg, sems, scales, 4)
    wide_ups = [Pair((None, up2_hbm.at[1])[n], vup2_hbm.at[n], o_up2.at[n], ov_up2.at[n], (w_up2, wb_up2)[n], vb_up2.at[n],
                     sems, scales, 5 + n) for n in range(2)]
    wide_downs = [Pair((None, dn2_hbm.at[1])[n], vdn2_hbm.at[n], o_dn2.at[n], ov_dn2.at[n], (w_dn2, wb_dn2)[n], vb_dn2.at[n],
                       sems, scales, 7 + n) for n in range(2)]
    wb_hd, vb_hd = wb_dn2.at[pl.ds(0, CLASSES)], vb_dn2.at[1, pl.ds(0, CLASSES)]
    head = Pair(hd_hbm, vhd_hbm, o_hd, ov_hd, wb_hd, vb_hd, sems, scales, 9)
    for each in ups + downs + [merge, head] + wide_ups[:1]:
        start_all(each.loads)
    small = sums.at[pl.ds(LAST * UNIT, UNIT)]
    for n in range(2):
        ups[n].update(2, row_pieces, small.at[pl.ds(WIDE + n * WIDTH, WIDTH)], up1.at[n], SHARD)
        gb_turn[...] = small[pl.ds(WIDE + TILE + n * WIDTH, WIDTH), :].astype(F32).T
        downs[n].update(4, row_pieces, gb_turn, dn1.at[n], WIDTH)
    start_all(wide_downs[0].loads)
    merge.update(8, row_pieces, small.at[pl.ds(0, WIDE)], mg, SHARD)
    tail = pl.ds(992, SUBLANES)
    head.update(31, row_pieces, g_hd, hd, 32, tails=[(wb_hd.at[tail], vb_hd.at[tail], g_hd.at[tail], hd.at[tail])])
    start_all(wide_ups[1].loads)
    wide_ups[0].update(16, up_pieces, sums.at[pl.ds(HELD * UNIT, HELD * UNIT)], up2)
    wide_downs[0].update(16, down_pieces, sums.at[pl.ds(HELD * UNIT, HELD * UNIT)], dn2)
    wait_all(head.stores)
    start_all(wide_downs[1].loads)
    stage_one_forward(r0, s0, s1, up1, dn1)
    wide_ups[1].update(16, up_pieces, sums.at[pl.ds(0, HELD * UNIT)], None)
    wide_downs[1].update(16, down_pieces, sums.at[pl.ds(0, HELD * UNIT)], None)
    s0[...] = dot_nn(s1[...], mg[...]).astype(BF16)
    stage_two_block(s0, s1, normed_ref, acc, up2, dn2)
    cast_rows(up2, wb_up2, WIDE, 16)
    cast_rows(dn2, wb_dn2, HID_TWO, SHARD)
    stage_two_block(s1, s0, normed_ref, acc, up2, dn2)
    head_b = pooled_norm(s0[...])[0].astype(BF16)
    logits_ref[...] = dot_nt(head_b, hd[...])[:IMGS]
    for each in ups + downs + [merge] + wide_ups + wide_downs:
        wait_all(each.stores)


W_SHAPES = ((2, 128, 512), (2, 512, 128), (512, 512), (2, 512, 2048), (2, 2048, 512), (CLASSES, 512))
BUF_SHAPES = W_SHAPES[:3] + ((512, 2048), (2048, 512), (CLASSES, 512))


def vmem(shape, dtype):
    return pltpu.VMEM(shape, dtype)


ANY_SPEC = pl.BlockSpec(memory_space=pl.ANY)
VMEM_SPEC = pl.BlockSpec(memory_space=pltpu.VMEM)


def act(dtype=BF16):
    return vmem((ROWS, WIDE), dtype)


def f32_outs(shapes):
    return [jax.ShapeDtypeStruct(shape, F32) for shape in shapes]


DMA = pltpu.SemaphoreType.DMA


HANDED = ((SHARE_ROWS, WIDE), BF16), *((shape, F32) for shape in BUF_SHAPES[:5]), ((ROWS, WIDE), BF16), ((CLASS_PAD, WIDE), BF16)
HANDED_BYTES = 22_000_000


def run_train(x_now, x_next, labels, params):
    return pl.pallas_call(
        train_kernel,
        out_shape=[vmem(*each) for each in HANDED] + f32_outs([(MATRICES * SUBLANES, WIDTH)]),
        in_specs=[ANY_SPEC] * 2 + [pl.BlockSpec(memory_space=pltpu.SMEM)] + [ANY_SPEC] * 6,
        out_specs=[VMEM_SPEC] * 9,
        scratch_shapes=[vmem((ROWS * 4, WIDTH), BF16), vmem((ROWS * 4, WIDTH), F32)]
        + [vmem(shape, BF16) for shape in W_SHAPES[:5]] + [vmem((CLASS_PAD, WIDE), BF16)]
        + [act()] * 5 + [act(F32), act(), act(), DMA((13,)), vmem((WIDTH, WIDE), F32), vmem((WIDTH, WIDE), F32)]
        + [vmem((rows, WIDE), BF16) for rows in (SHARE_ROWS, N_UNITS * TILE, N_UNITS * WIDTH)]
        + [vmem((DEVS, SUBLANES, WIDE + CLASS_PAD), BF16), vmem((MATRICES * SUBLANES, WIDTH), F32), vmem((MATRICES, SUBLANES, WIDE), F32)]
        + [DMA((N_UNITS, 6, 2, 2)), DMA((DEVS, 2))],
        compiler_params=pltpu.CompilerParams(vmem_limit_bytes=VMEM_BYTES - HANDED_BYTES, collective_id=0, has_side_effects=True),
        cost_estimate=pl.CostEstimate(flops=30_000_000_000, bytes_accessed=40_000_000, transcendentals=0),
        name='train_part',
    )(x_now, x_next, labels, *params)


def run_next(params, velocities, handed):
    held = [vmem(*each) for each in HANDED[1:6]]
    handed = [pltpu.with_memory_space_constraint(each, pltpu.VMEM) for each in handed[:8]] + list(handed[8:])
    outs = pl.pallas_call(
        next_kernel,
        out_shape=f32_outs([(IMGS, CLASSES)] + list(W_SHAPES) * 2) + held,
        in_specs=[ANY_SPEC] * 9 + [VMEM_SPEC] * 9,
        out_specs=[VMEM_SPEC] + [ANY_SPEC] * 12 + [VMEM_SPEC] * 5,
        scratch_shapes=[vmem(shape, F32) for shape in W_SHAPES[:5] + BUF_SHAPES[3:5]] + [vmem((WIDE, WIDTH), F32)]
        + [vmem(shape, BF16) for shape in BUF_SHAPES]
        + [act()] * 3 + [act(F32), DMA((10, 2, 2))],
        input_output_aliases={10 + i: 13 + i for i in range(5)},
        compiler_params=pltpu.CompilerParams(vmem_limit_bytes=VMEM_BYTES - HANDED_BYTES),
        cost_estimate=pl.CostEstimate(flops=10_000_000_000, bytes_accessed=100_000_000, transcendentals=0),
        name='next_part',
    )(*params[3:], *velocities, *handed)
    return outs[:13]


def turn_head(arrays):
    return (*arrays[:5], arrays[5].T)


def solution(mesh):
    def local_step(x_now, labels_now, x_next, *weights):
        params, velocities = turn_head(weights[:6]), turn_head(weights[6:])
        handed = run_train(x_now.reshape(ROWS * 4, WIDTH), x_next.reshape(ROWS * 4, WIDTH), labels_now, params)
        outs = run_next(params, velocities, handed)
        return (outs[0], *turn_head(outs[1:7]), *turn_head(outs[7:]))

    split = P('data')
    in_specs = (split, split, split) + (P(),) * 12
    out_specs = (split,) + (P(),) * 12
    return jax.shard_map(local_step, mesh=mesh, in_specs=in_specs, out_specs=out_specs, check_vma=False)
```

```python
import jax
import jax.numpy as jnp
from jax import lax
from jax.experimental import pallas as pl
from jax.experimental.pallas import tpu as pltpu
from jax.sharding import PartitionSpec as P

MOMENTUM = 0.9
TRUST = 0.1
LN_EPS = 1e-6
GELU_A = 0.7978845608028654
GELU_B = 0.044715 * GELU_A
F32 = jnp.float32
BF16 = jnp.bfloat16
VMEM_BYTES = 66_000_000

IMGS, TOKENS, WIDTH = 4, 784, 128
MERGED = TOKENS // 4
ROWS = IMGS * MERGED
WIDE = 4 * WIDTH
HID_ONE, HID_TWO = 4 * WIDTH, 4 * WIDE
CLASSES = 1000
TILE = 256
SHARD = 64
N_TILES = HID_TWO // TILE
FWD_TILE = 512


def dot_nn(a, b):
    return lax.dot_general(a, b, (((1,), (0,)), ((), ())), preferred_element_type=F32)


def dot_nt(a, b):
    return lax.dot_general(a, b, (((1,), (1,)), ((), ())), preferred_element_type=F32)


def dot_tn(a, b):
    return lax.dot_general(a, b, (((0,), (0,)), ((), ())), preferred_element_type=F32)


def norm_parts(vals):
    centered = vals - jnp.mean(vals, axis=-1, keepdims=True)
    variance = jnp.mean(centered * centered, axis=-1, keepdims=True)
    rstd = lax.rsqrt(variance + LN_EPS)
    return centered * rstd, rstd


def norm_back(grad, normed, rstd):
    mean_g = jnp.mean(grad, axis=-1, keepdims=True)
    mean_gn = jnp.mean(grad * normed, axis=-1, keepdims=True)
    return rstd * (grad - mean_g - normed * mean_gn)


def gelu_parts(pre):
    square = pre * pre
    half = 0.5 * jnp.tanh(pre * (GELU_A + GELU_B * square)) + 0.5
    return square, half


def gelu_slope(pre, square, half):
    return half * (1.0 + pre * (1.0 - half) * (2.0 * GELU_A + 6.0 * GELU_B * square))


def cast_rows(dst, src, rows, step):
    def body(i, carry):
        sl = pl.ds(pl.multiple_of(i * step, step), step)
        dst[sl, :] = src[sl, :].astype(BF16)
        return carry
    lax.fori_loop(0, rows // step, body, 0)


def lanes(index, size):
    return pl.ds(pl.multiple_of(index * size, size), size)


def permute_tokens(x_ref, x_f32, r0):
    x_f32[...] = x_ref[...].astype(F32)
    for j in range(4):
        r0[:, j * WIDTH:(j + 1) * WIDTH] = x_f32[pl.ds(j, ROWS, stride=4), :].astype(BF16)


def stage_one_block(resid, w_up, w_down):
    res_f = resid.astype(F32)
    normed = norm_parts(res_f)[0].astype(BF16)
    pre = dot_nn(normed, w_up)
    act = (pre * gelu_parts(pre)[1]).astype(BF16)
    return (res_f + dot_nn(act, w_down)).astype(BF16)


def stage_one_forward(r0, r1, r2, up_one, down_one, slots=()):
    def body(j, carry):
        for k, steps in enumerate(slots):
            pl.when(j == k)(lambda steps=steps: run_all(steps))
        cuts = [lanes(2 * j + k, WIDTH) for k in range(2)]
        mids = [stage_one_block(r0[:, sl], up_one[0], down_one[0]) for sl in cuts]
        for sl, mid in zip(cuts, mids):
            r1[:, sl] = mid
        for sl, mid in zip(cuts, mids):
            r2[:, sl] = stage_one_block(mid, up_one[1], down_one[1])
        return carry
    lax.fori_loop(0, 2, body, 0)


def stage_two_block(src, dst, normed_ref, acc, up_ref, down_ref):
    res_f = src[...].astype(F32)
    normed_ref[...] = norm_parts(res_f)[0].astype(BF16)
    acc[...] = res_f

    def body(t, carry):
        sl = lanes(t, FWD_TILE)
        pre = dot_nn(normed_ref[...], up_ref[:, sl])
        act = (pre * gelu_parts(pre)[1]).astype(BF16)
        acc[...] += dot_nn(act, down_ref[sl, :])
        return carry
    lax.fori_loop(0, HID_TWO // FWD_TILE, body, 0)
    dst[...] = acc[...].astype(BF16)


def image_rows():
    image = lax.broadcasted_iota(jnp.int32, (8, ROWS), 0)
    row = lax.broadcasted_iota(jnp.int32, (8, ROWS), 1)
    inside = (row >= image * MERGED) & (row < (image + 1) * MERGED)
    return jnp.where(inside, 1.0, 0.0).astype(BF16)


def pooled_norm(resid):
    pooled = dot_nn(image_rows(), resid) * (1.0 / MERGED)
    return norm_parts(pooled)


UNIT = 1024
N_UNITS = 9
SHARE_ROWS = N_UNITS * UNIT
CLASS_PAD = 1024
DEVS = 8
SUBLANES = 8
LAST = N_UNITS - 1
HELD = 4
MATRICES = 10
PAIR_OUT, FIRST_OUT, SECOND_OUT, SECOND_BACK, FIRST_BACK, PAIR_BACK = range(6)


def start_all(copies):
    for copy in copies:
        copy.start()


def wait_all(copies):
    for copy in copies:
        copy.wait()


def sum_rows(tile):
    rows, cols = tile.shape
    return jnp.sum(tile.reshape(rows // 8, 8, cols), axis=0)


def square_sum(ref, start, rows, step):
    def body(i, total):
        part = ref[pl.ds(pl.multiple_of(start + i * step, step), step), :].astype(F32)
        return total + sum_rows(part * part)
    return lax.fori_loop(0, rows // step, body, jnp.zeros((SUBLANES, ref.shape[1]), F32))


def total_of(tile):
    return jnp.sum(jnp.sum(tile, axis=0, keepdims=True), axis=1, keepdims=True)


def run_all(steps):
    for action, unit in steps:
        action(unit)


class Links:
    def __init__(self, own, final, land1, land2, sems):
        self.own, self.final, self.land1, self.land2, self.sems = own, final, land1, land2, sems
        me = lax.axis_index('data')
        self.me = me
        self.core, self.x, self.y = lax.rem(me, 2), lax.rem(me // 2, 2), me // 4
        self.pair = me + 1 - 2 * self.core
        self.x_peer = me + 2 - 4 * self.x
        self.y_peer = me + 4 - 8 * self.y

    def rows(self, unit, offset, size):
        return pl.ds(pl.multiple_of(unit * UNIT + offset, SHARD), size)

    def half(self, unit, offset, size):
        return self.rows(unit, self.core * WIDE + offset, size)

    def copy(self, unit, phase, lane, src, dst, peer):
        return pltpu.make_async_remote_copy(
            src_ref=src, dst_ref=dst, send_sem=self.sems.at[unit, phase, lane, 0], recv_sem=self.sems.at[unit, phase, lane, 1],
            device_id=(peer,), device_id_type=pl.DeviceIdType.MESH)

    def copies(self, unit, phase):
        x, y = self.x, self.y
        own, final = self.own, self.final
        if phase == PAIR_OUT:
            sl = self.rows(unit, (1 - self.core) * WIDE, WIDE)
            return [self.copy(unit, PAIR_OUT, 0, own.at[sl], final.at[sl], self.pair)]
        if phase == FIRST_OUT:
            land = lambda k: self.land1.at[pl.ds(pl.multiple_of(unit * TILE + k * WIDTH, WIDTH), WIDTH)]
            return [self.copy(unit, FIRST_OUT, 0, own.at[self.half(unit, (1 - x) * WIDTH, WIDTH)], land(0), self.x_peer),
                    self.copy(unit, FIRST_OUT, 1, own.at[self.half(unit, TILE + (1 - y) * WIDTH, WIDTH)], land(1), self.y_peer)]
        if phase == SECOND_OUT:
            land = lambda k: self.land2.at[pl.ds(pl.multiple_of(unit * WIDTH + k * SHARD, SHARD), SHARD)]
            return [self.copy(unit, SECOND_OUT, 0, own.at[self.half(unit, x * WIDTH + (1 - y) * SHARD, SHARD)], land(0), self.y_peer),
                    self.copy(unit, SECOND_OUT, 1, own.at[self.half(unit, TILE + y * WIDTH + (1 - x) * SHARD, SHARD)], land(1), self.x_peer)]
        if phase == SECOND_BACK:
            first = self.half(unit, x * WIDTH + y * SHARD, SHARD)
            second = self.half(unit, TILE + y * WIDTH + x * SHARD, SHARD)
            return [self.copy(unit, SECOND_BACK, 0, final.at[first], final.at[first], self.y_peer),
                    self.copy(unit, SECOND_BACK, 1, final.at[second], final.at[second], self.x_peer)]
        if phase == FIRST_BACK:
            first, second = self.half(unit, x * WIDTH, WIDTH), self.half(unit, TILE + y * WIDTH, WIDTH)
            return [self.copy(unit, FIRST_BACK, 0, final.at[first], final.at[first], self.x_peer),
                    self.copy(unit, FIRST_BACK, 1, final.at[second], final.at[second], self.y_peer)]
        sl = self.half(unit, 0, WIDE)
        return [self.copy(unit, PAIR_BACK, 0, final.at[sl], final.at[sl], self.pair)]

    def start(self, unit, phase):
        for copy in self.copies(unit, phase):
            copy.start()

    def wait(self, unit, phase):
        for copy in self.copies(unit, phase):
            copy.wait()

    def reduce_pair(self, unit):
        self.wait(unit, PAIR_OUT)
        x, y = self.x, self.y
        for offset in ((1 - x) * WIDTH, TILE + (1 - y) * WIDTH, x * WIDTH, TILE + y * WIDTH):
            sl = self.half(unit, offset, WIDTH)
            self.own[sl, :] = self.own[sl, :] + self.final[sl, :]
        self.start(unit, FIRST_OUT)

    def reduce_first(self, unit):
        self.wait(unit, FIRST_OUT)
        x, y = self.x, self.y
        for keep in (False, True):
            for lane, base, here, there in ((0, x * WIDTH, y, 0), (1, TILE + y * WIDTH, x, WIDTH)):
                part = here if keep else 1 - here
                sl = self.half(unit, base + part * SHARD, SHARD)
                land = pl.ds(pl.multiple_of(unit * TILE + there + part * SHARD, SHARD), SHARD)
                self.own[sl, :] = self.own[sl, :] + self.land1[land, :]
        self.start(unit, SECOND_OUT)

    def reduce_second(self, unit):
        self.wait(unit, SECOND_OUT)
        for lane, offset in ((0, self.x * WIDTH + self.y * SHARD), (1, TILE + self.y * WIDTH + self.x * SHARD)):
            sl = self.half(unit, offset, SHARD)
            land = pl.ds(pl.multiple_of(unit * WIDTH + lane * SHARD, SHARD), SHARD)
            self.final[sl, :] = self.own[sl, :] + self.land2[land, :]

    def forward(self, unit, phase):
        self.wait(unit, phase)
        self.start(unit, phase + 1)


def train_kernel(x_hbm, x_next_hbm, vup1_hbm, vdn1_hbm, vmg_hbm, labels_ref, up1_hbm, dn1_hbm, mg_hbm, up2_hbm, dn2_hbm, hd_hbm,
                 final, st_up1, st_dn1, st_mg, st_up2, st_dn2, r0, g_hd, x_f32, acc, scale_ref,
                 x_v, gb_turn,
                 up1, dn1, mg, up2, dn2, hd,
                 r1, r2, s0, s1, normed_ref, grad_a, grad_b, sems,
                 du1, dv1, own, land1, land2, factors, w_sums, g_sums, link_sems, factor_sems):
    links = Links(own, final, land1, land2, link_sems)
    me = links.me
    st_hd = st_dn2.at[pl.ds(0, CLASSES)]
    copies = [pltpu.make_async_copy(src, dst, sems.at[i]) for i, (src, dst) in enumerate((
        (x_hbm, x_v), (up1_hbm, st_up1), (dn1_hbm, st_dn1), (mg_hbm, st_mg),
        (up2_hbm.at[0], st_up2), (dn2_hbm.at[0], st_dn2),
        (up2_hbm.at[1], st_up2), (dn2_hbm.at[1], st_dn2), (hd_hbm, st_hd)))]
    start_all(copies[:3])
    barrier = pltpu.get_barrier_semaphore()
    for k in range(1, DEVS):
        pl.semaphore_signal(barrier, inc=1, device_id=(lax.rem(me + k, DEVS),), device_id_type=pl.DeviceIdType.MESH)
    copies[0].wait()
    permute_tokens(x_v, x_f32, r0)
    wait_all(copies[1:3])
    start_all(copies[3:6])
    for n in range(2):
        cast_rows(up1.at[n], st_up1.at[n], WIDTH, SHARD)
        cast_rows(dn1.at[n], st_dn1.at[n], WIDE, TILE)
    stage_one_forward(r0, r1, r2, up1, dn1)
    copies[3].wait()
    cast_rows(mg, st_mg, WIDE, SHARD)
    s0[...] = dot_nn(r2[...], mg[...]).astype(BF16)
    s2 = grad_a
    for n, (src, dst) in enumerate(((s0, s1), (s1, s2))):
        copies[4 + 2 * n].wait()
        cast_rows(up2.at[n], st_up2, WIDE, 16)
        if n == 0:
            copies[6].start()
        copies[5 + 2 * n].wait()
        cast_rows(dn2.at[n], st_dn2, 2048, SHARD)
        copies[7 + n].start()
        stage_two_block(src, dst, normed_ref, acc, up2.at[n], dn2.at[n])
    copies[8].wait()
    cast_rows(hd, st_hd, 992, 32)
    hd[992:CLASSES, :] = st_hd[992:CLASSES, :].astype(BF16)
    hd[CLASSES:, :] = jnp.zeros((CLASS_PAD - CLASSES, WIDE), BF16)
    head_normed, head_rstd = pooled_norm(s2[...])
    head_b = head_normed.astype(BF16)
    class_id = lax.broadcasted_iota(jnp.int32, (SUBLANES, CLASS_PAD), 1)
    row_id = lax.broadcasted_iota(jnp.int32, (SUBLANES, CLASS_PAD), 0)
    logits = jnp.where(class_id < CLASSES, dot_nt(head_b, hd[...]), -jnp.inf)
    top = jnp.max(logits, axis=-1, keepdims=True)
    expd = jnp.exp(logits - top)
    probs = expd / jnp.sum(expd, axis=-1, keepdims=True)
    label = jnp.zeros((SUBLANES, CLASS_PAD), jnp.int32)
    for i in range(IMGS):
        label = jnp.where(row_id == i, labels_ref[i], label)
    onehot = jnp.where(class_id == label, 1.0, 0.0)
    grad_logits = jnp.where(row_id < IMGS, (probs - onehot) * (1.0 / (IMGS * DEVS)), 0.0).astype(BF16)
    factors[me, :, :WIDE] = head_b
    factors[me, :, WIDE:] = grad_logits
    grad_pooled = norm_back(dot_nn(grad_logits, hd[...]), head_normed, head_rstd) * (1.0 / MERGED)
    grad_a[...] = dot_tn(image_rows(), grad_pooled.astype(BF16)).astype(BF16)

    pl.semaphore_wait(barrier, DEVS - 1)

    def factor_copy(k):
        return pltpu.make_async_remote_copy(
            src_ref=factors.at[me], dst_ref=factors.at[me], send_sem=factor_sems.at[k, 0], recv_sem=factor_sems.at[k, 1],
            device_id=(lax.rem(me + k, DEVS),), device_id_type=pl.DeviceIdType.MESH)

    grads = (grad_a, grad_b)
    for step, n in enumerate((1, 0)):
        g_in, g_out = grads[step], grads[1 - step]
        src = (s0, s1)[n]
        normed_ref[...] = norm_parts(src[...].astype(F32))[0].astype(BF16)
        acc[...] = jnp.zeros_like(acc)

        def tile(t, row, n=n, g_in=g_in):
            sl = lanes(t, TILE)
            pre = dot_nn(normed_ref[...], up2[n, :, sl])
            square, half = gelu_parts(pre)
            act = (pre * half).astype(BF16)
            grad_pre = (gelu_slope(pre, square, half) * dot_nt(g_in[...], dn2[n, sl, :])).astype(BF16)
            own[pl.ds(row + TILE, TILE), :] = dot_tn(act, g_in[...]).astype(BF16)
            grad_up = dot_tn(normed_ref[...], grad_pre).astype(BF16)
            own[pl.ds(row, TILE), :TILE] = grad_up[:TILE]
            own[pl.ds(row, TILE), TILE:] = grad_up[TILE:]
            acc[...] += dot_nt(grad_pre, up2[n, :, sl])

        def body(p, carry, step=step, tile=tile):
            unit = step * 4 + p
            row = pl.multiple_of(unit * UNIT, UNIT)

            tile(2 * p, row)
            if step:
                links.reduce_pair(unit - 1)
            else:
                pl.when(p > 0)(lambda: links.reduce_pair(unit - 1))
            tile(2 * p + 1, row + WIDE)
            if step:
                links.reduce_first(unit - 4)
            links.start(unit, PAIR_OUT)
            return carry
        if step == 0:
            for k in range(1, DEVS):
                factor_copy(k).start()
        lax.fori_loop(0, N_TILES // 2, body, 0)
        normed_f, rstd = norm_parts(src[...].astype(F32))
        g_out[...] = (norm_back(acc[...], normed_f, rstd) + g_in[...].astype(F32)).astype(BF16)
    own[LAST * UNIT:LAST * UNIT + WIDE, :] = dot_tn(r2[...], grad_a[...]).astype(BF16)
    grad_b[...] = dot_nt(grad_a[...], mg[...]).astype(BF16)

    def reduced(unit):
        links.reduce_second(unit)
        links.start(unit, SECOND_BACK)

    def finish(unit):
        links.wait(unit, PAIR_BACK)
        start = unit * UNIT
        if unit < LAST:
            for k in range(4):
                matrix = (6 if unit < HELD else 5) + 2 * (k % 2)
                g_sums[matrix] += square_sum(final, start + k * TILE, TILE, SHARD)
        else:
            g_sums[4] = square_sum(final, start, WIDE, SHARD)
            for k in range(4):
                g_sums[k] = square_sum(final, start + WIDE + k * WIDTH, WIDTH, SHARD)

    def weigh(matrix, ref, rows, step):
        w_sums[pl.ds(matrix * SUBLANES, SUBLANES), :] = jnp.broadcast_to(total_of(square_sum(ref, 0, rows, step)), (SUBLANES, WIDTH))

    reloads = [pltpu.make_async_copy(src, dst, sems.at[9 + i]) for i, (src, dst) in enumerate((
        (up2_hbm.at[0], st_up2), (dn2_hbm.at[1], st_dn2), (x_next_hbm, x_v), (dn2_hbm.at[0], st_dn2)))]

    speeds = [pltpu.make_async_copy(src, dst, sems.at[13 + i]) for i, (src, dst) in enumerate((
        (vup1_hbm.at[0], acc.at[pl.ds(0, WIDTH)]), (vup1_hbm.at[1], acc.at[pl.ds(WIDTH, WIDTH)]), (vmg_hbm, acc.at[pl.ds(TILE, WIDE)]),
        (vdn1_hbm.at[0], x_f32.at[pl.ds(0, WIDE)]), (vdn1_hbm.at[1], x_f32.at[pl.ds(WIDE, WIDE)])))]

    def scale_of(matrix):
        sl = pl.ds(matrix * SUBLANES, SUBLANES)
        scale = TRUST * (jnp.sqrt(w_sums[sl, :]) / jnp.sqrt(total_of(g_sums[matrix])))
        scale_ref[sl, :] = scale
        return scale[:1, :1]

    def update_small(_):
        wait_all(speeds)
        small = final.at[pl.ds(LAST * UNIT, UNIT)]
        for n in range(2):
            grad = small.at[pl.ds(WIDE + n * WIDTH, WIDTH)]
            lars_matrix(2, row_pieces(st_up1.at[n], acc.at[pl.ds(n * WIDTH, WIDTH)], grad, up1.at[n], SHARD), scale_of(n))
            gb_turn[...] = small[pl.ds(WIDE + TILE + n * WIDTH, WIDTH), :].astype(F32).T
            lars_matrix(4, row_pieces(st_dn1.at[n], x_f32.at[pl.ds(n * WIDE, WIDE)], gb_turn, dn1.at[n], WIDTH), scale_of(2 + n))
        lars_matrix(8, row_pieces(st_mg, acc.at[pl.ds(TILE, WIDE)], small.at[pl.ds(0, WIDE)], mg, SHARD), scale_of(4))

    def weigh_small(_):
        for n in range(2):
            weigh(n, st_up1.at[n], WIDTH, SHARD)
            weigh(2 + n, st_dn1.at[n], WIDE, WIDTH)
        weigh(4, st_mg, WIDE, SHARD)
        weigh(6, st_up2, WIDE, 16)
        w_hd = square_sum(st_dn2, 0, 992, 32) + square_sum(st_dn2, 992, SUBLANES, SUBLANES)
        w_sums[pl.ds(9 * SUBLANES, SUBLANES), :] = jnp.broadcast_to(total_of(w_hd), (SUBLANES, WIDTH))
        start_all(reloads[:3])

    def weigh_first(_):
        wait_all(reloads[:3])
        weigh(5, st_up2, WIDE, 16)
        weigh(8, st_dn2, HID_TWO, SHARD)
        reloads[3].start()
        permute_tokens(x_v, x_f32, r0)
        start_all(speeds)

    def weigh_second(_):
        reloads[3].wait()
        weigh(7, st_dn2, HID_TWO, SHARD)
        g_sums[9] = square_sum(g_hd, 0, CLASS_PAD, SHARD)

    def back_first(unit):
        links.forward(unit, SECOND_BACK)

    def back_pair(unit):
        links.forward(unit, FIRST_BACK)

    g_sums[...] = jnp.zeros_like(g_sums)
    links.reduce_pair(7)
    first = links.reduce_first
    slots = {1: (((reduced, 0), (reduced, 1), (reduced, 2), (first, 4)), ((first, 5),), ((reduced, 3),), ((first, 6), (back_first, 0))),
             0: (((back_first, 1),), ((back_first, 2),), ((reduced, 4),), ((first, 7),))}

    for n, src, g_in, g_out in ((1, r1, grad_b, grad_a), (0, r0, grad_a, grad_b)):
        du1[...] = jnp.zeros_like(du1)
        dv1[...] = jnp.zeros_like(dv1)

        def body(j, carry, n=n, src=src, g_in=g_in, g_out=g_out):
            sl = lanes(j, WIDTH)
            normed_f, rstd = norm_parts(src[:, sl].astype(F32))
            normed = normed_f.astype(BF16)
            grad = g_in[:, sl]
            pre = dot_nn(normed, up1[n])
            square, half = gelu_parts(pre)
            act = (pre * half).astype(BF16)
            grad_pre = (gelu_slope(pre, square, half) * dot_nt(grad, dn1[n])).astype(BF16)
            dv1[...] += dot_tn(grad, act)
            du1[...] += dot_tn(normed, grad_pre)
            if n:
                back = norm_back(dot_nt(grad_pre, up1[n]), normed_f, rstd)
                g_out[:, sl] = (back + grad.astype(F32)).astype(BF16)
            for k, steps in enumerate(slots[n]):
                pl.when(j == k)(lambda steps=steps: run_all(steps))
            return carry
        lax.fori_loop(0, 4, body, 0)
        base = LAST * UNIT + WIDE + n * WIDTH
        own[base:base + WIDTH, :] = du1[...].astype(BF16)
        own[base + TILE:base + TILE + WIDTH, :] = dv1[...].astype(BF16)
    links.start(LAST, PAIR_OUT)

    for k in range(1, DEVS):
        factor_copy(k).wait()

    def head_tile(c, carry):
        sl = pl.ds(pl.multiple_of(WIDE + c * WIDTH, WIDTH), WIDTH)
        total = jnp.zeros((WIDTH, WIDE), F32)
        for d in range(DEVS):
            total += dot_tn(factors[d, :, sl], factors[d, :, :WIDE]).astype(BF16).astype(F32)
        g_hd[pl.ds(pl.multiple_of(c * WIDTH, WIDTH), WIDTH), :] = total.astype(BF16)
        return carry
    half_tiles = CLASS_PAD // WIDTH // 2
    lax.fori_loop(0, half_tiles, head_tile, 0)
    run_all(((links.reduce_pair, LAST), (reduced, 5), (back_first, 3)))
    lax.fori_loop(half_tiles, 2 * half_tiles, head_tile, 0)
    run_all(((reduced, 6), (weigh_small, 0), (first, LAST), (weigh_first, 0), (back_pair, 0), (back_pair, 1), (finish, 0), (reduced, 7),
             (reduced, LAST), (weigh_second, 0), (back_pair, 2), (finish, 1), (back_first, 4), (finish, 2), (back_first, LAST),
             (back_first, 5), (back_pair, 3), (back_first, 6), (finish, 3), (back_pair, LAST), (back_pair, 4), (back_first, 7),
             (finish, LAST), (update_small, 0)))
    stage_one_forward(r0, r1, r2, up1, dn1, (((back_pair, 5), (finish, 4)), ((back_pair, 6), (finish, 5))))
    run_all(((back_pair, 7), (finish, 6)))
    r0[...] = dot_nn(r2[...], mg[...]).astype(BF16)
    finish(7)
    for matrix in range(5, MATRICES):
        scale_of(matrix)


def lars_matrix(steps, piece, scale, tails=()):
    def update_piece(w, v, g, b):
        new_v = MOMENTUM * v[...] + scale * g[...].astype(F32)
        new_w = w[...] - new_v
        v[...] = new_v
        w[...] = new_w
        if b is not None:
            b[...] = new_w.astype(BF16)

    def update(i, carry):
        update_piece(*piece(i))
        return carry
    lax.fori_loop(0, steps, update, 0)
    for tail in tails:
        update_piece(*tail)


def row_pieces(w, v, g, b, step):
    def piece(i):
        sl = pl.ds(pl.multiple_of(i * step, step), step)
        return w.at[sl], v.at[sl], g.at[sl], b.at[sl]
    return piece


def up_pieces(w, v, g, b):
    def piece(i):
        h, part = i // 2, lax.rem(i, 2)
        rows, cols = lanes(part, 256), lanes(h, 256)
        g_rows = pl.ds(pl.multiple_of(h * 512, 512), 256)
        return w.at[rows, cols], v.at[rows, cols], g.at[g_rows, rows], b if b is None else b.at[rows, cols]
    return piece


def down_pieces(w, v, g, b):
    def piece(i):
        h, part = i // 2, lax.rem(i, 2)
        rows = pl.ds(pl.multiple_of(i * 128, 128), 128)
        g_rows = pl.ds(pl.multiple_of(h * 512 + 256 + part * 128, 128), 128)
        return w.at[rows], v.at[rows], g.at[g_rows], b if b is None else b.at[rows]
    return piece


class Pair:
    def __init__(self, w, v, out_w, out_v, buf_w, buf_v, sems, scales, slot):
        self.buf_w, self.buf_v = buf_w, buf_v
        self.scale = scales.at[pl.ds(slot * SUBLANES, 1), pl.ds(0, 1)]
        ins = ((v, buf_v),) if w is None else ((v, buf_v), (w, buf_w))
        self.loads, self.stores = ([pltpu.make_async_copy(src, dst, sems.at[slot, k, i]) for i, (src, dst) in enumerate(part)]
                                   for k, part in enumerate((ins, ((buf_w, out_w), (buf_v, out_v)))))

    def update(self, steps, make, grad, cast, *rest, tails=()):
        wait_all(self.loads)
        lars_matrix(steps, make(self.buf_w, self.buf_v, grad, cast, *rest), self.scale[...], tails)
        start_all(self.stores)


def next_kernel(up2_hbm, dn2_hbm, hd_hbm, vup2_hbm, vdn2_hbm, vhd_hbm,
                sums, w_up1, w_dn1, w_mg, in_up2, in_dn2, mid, g_hd, v_down, v_rest, scales,
                logits_ref, o_up1, o_dn1, o_mg, o_up2, o_dn2, o_hd, ov_up1, ov_dn1, ov_mg, ov_up2, ov_dn2, ov_hd,
                w_up2, w_dn2,
                vb_up2, vb_dn2, wb_up2, wb_dn2, up2, dn2, hd, s1, normed_ref, acc, sems, small_sems):
    done = [pltpu.make_async_copy(src, dst, small_sems.at[i]) for i, (src, dst) in enumerate((
        (w_up1, o_up1), (w_dn1, o_dn1), (w_mg, o_mg), (v_rest.at[pl.ds(TILE, WIDE)], ov_mg),
        (v_rest.at[pl.ds(0, WIDTH)], ov_up1.at[0]), (v_rest.at[pl.ds(WIDTH, WIDTH)], ov_up1.at[1]),
        (v_down.at[pl.ds(0, WIDE)], ov_dn1.at[0]), (v_down.at[pl.ds(WIDE, WIDE)], ov_dn1.at[1])))]
    wide_ups = [Pair((None, up2_hbm.at[1])[n], vup2_hbm.at[n], o_up2.at[n], ov_up2.at[n], (w_up2, wb_up2)[n], vb_up2.at[n],
                     sems, scales, 5 + n) for n in range(2)]
    wide_downs = [Pair((None, dn2_hbm.at[1])[n], vdn2_hbm.at[n], o_dn2.at[n], ov_dn2.at[n], (w_dn2, wb_dn2)[n], vb_dn2.at[n],
                       sems, scales, 7 + n) for n in range(2)]
    wb_hd, vb_hd = wb_dn2.at[pl.ds(0, CLASSES)], vb_dn2.at[1, pl.ds(0, CLASSES)]
    head = Pair(hd_hbm, vhd_hbm, o_hd, ov_hd, wb_hd, vb_hd, sems, scales, 9)
    for each in [head] + wide_ups[:1] + wide_downs[:1]:
        start_all(each.loads)
    start_all(done)
    start_all(wide_ups[1].loads)
    tail = pl.ds(992, SUBLANES)
    head.update(31, row_pieces, g_hd, hd, 32, tails=[(wb_hd.at[tail], vb_hd.at[tail], g_hd.at[tail], hd.at[tail])])
    wide_ups[0].update(16, up_pieces, sums.at[pl.ds(HELD * UNIT, HELD * UNIT)], up2)
    wide_downs[0].update(16, down_pieces, sums.at[pl.ds(HELD * UNIT, HELD * UNIT)], dn2)
    wait_all(head.stores)
    start_all(wide_downs[1].loads)
    wide_ups[1].update(16, up_pieces, sums.at[pl.ds(0, HELD * UNIT)], None)
    stage_two_block(mid, s1, normed_ref, acc, up2, dn2)
    wide_downs[1].update(16, down_pieces, sums.at[pl.ds(0, HELD * UNIT)], dn2)
    cast_rows(up2, wb_up2, WIDE, 16)
    stage_two_block(s1, s1, normed_ref, acc, up2, dn2)
    head_b = pooled_norm(s1[...])[0].astype(BF16)
    logits_ref[...] = dot_nt(head_b, hd[...])[:IMGS]
    wait_all(done)
    for each in wide_ups + wide_downs:
        wait_all(each.stores)


W_SHAPES = ((2, 128, 512), (2, 512, 128), (512, 512), (2, 512, 2048), (2, 2048, 512), (CLASSES, 512))
BUF_SHAPES = W_SHAPES[:3] + ((512, 2048), (2048, 512), (CLASSES, 512))


def vmem(shape, dtype):
    return pltpu.VMEM(shape, dtype)


ANY_SPEC = pl.BlockSpec(memory_space=pl.ANY)
VMEM_SPEC = pl.BlockSpec(memory_space=pltpu.VMEM)


def act(dtype=BF16):
    return vmem((ROWS, WIDE), dtype)


def f32_outs(shapes):
    return [jax.ShapeDtypeStruct(shape, F32) for shape in shapes]


DMA = pltpu.SemaphoreType.DMA


HANDED = ((SHARE_ROWS, WIDE), BF16), *((shape, F32) for shape in BUF_SHAPES[:5]), ((ROWS, WIDE), BF16), ((CLASS_PAD, WIDE), BF16), \
    ((ROWS * 4, WIDTH), F32), ((ROWS, WIDE), F32)
HANDED_BYTES = 25_200_000


def run_train(x_now, x_next, labels, params, velocities):
    return pl.pallas_call(
        train_kernel,
        out_shape=[vmem(*each) for each in HANDED] + f32_outs([(MATRICES * SUBLANES, WIDTH)]),
        in_specs=[ANY_SPEC] * 5 + [pl.BlockSpec(memory_space=pltpu.SMEM)] + [ANY_SPEC] * 6,
        out_specs=[VMEM_SPEC] * 11,
        scratch_shapes=[vmem((ROWS * 4, WIDTH), BF16), vmem((WIDE, WIDTH), F32)]
        + [vmem(shape, BF16) for shape in W_SHAPES[:5]] + [vmem((CLASS_PAD, WIDE), BF16)]
        + [act()] * 7 + [DMA((18,)), vmem((WIDTH, WIDE), F32), vmem((WIDTH, WIDE), F32)]
        + [vmem((rows, WIDE), BF16) for rows in (SHARE_ROWS, N_UNITS * TILE, N_UNITS * WIDTH)]
        + [vmem((DEVS, SUBLANES, WIDE + CLASS_PAD), BF16), vmem((MATRICES * SUBLANES, WIDTH), F32), vmem((MATRICES, SUBLANES, WIDE), F32)]
        + [DMA((N_UNITS, 6, 2, 2)), DMA((DEVS, 2))],
        compiler_params=pltpu.CompilerParams(vmem_limit_bytes=VMEM_BYTES - HANDED_BYTES, collective_id=0, has_side_effects=True),
        cost_estimate=pl.CostEstimate(flops=30_000_000_000, bytes_accessed=40_000_000, transcendentals=0),
        name='train_part',
    )(x_now, x_next, *velocities[:3], labels, *params)


def run_next(params, velocities, handed):
    held = [vmem(*each) for each in HANDED[4:6]]
    handed = [pltpu.with_memory_space_constraint(each, pltpu.VMEM) for each in handed[:10]] + list(handed[10:])
    outs = pl.pallas_call(
        next_kernel,
        out_shape=f32_outs([(IMGS, CLASSES)] + list(W_SHAPES) * 2) + held,
        in_specs=[ANY_SPEC] * 6 + [VMEM_SPEC] * 11,
        out_specs=[VMEM_SPEC] + [ANY_SPEC] * 12 + [VMEM_SPEC] * 2,
        scratch_shapes=[vmem(shape, F32) for shape in W_SHAPES[3:5] + BUF_SHAPES[3:5]]
        + [vmem(shape, BF16) for shape in BUF_SHAPES[3:]]
        + [act()] * 2 + [act(F32), DMA((10, 2, 2)), DMA((8,))],
        input_output_aliases={10 + i: 13 + i for i in range(2)},
        compiler_params=pltpu.CompilerParams(vmem_limit_bytes=VMEM_BYTES - HANDED_BYTES),
        cost_estimate=pl.CostEstimate(flops=10_000_000_000, bytes_accessed=100_000_000, transcendentals=0),
        name='next_part',
    )(*params[3:], *velocities[3:], *handed)
    return outs[:13]


def turn_head(arrays):
    return (*arrays[:5], arrays[5].T)


def solution(mesh):
    def local_step(x_now, labels_now, x_next, *weights):
        params, velocities = turn_head(weights[:6]), turn_head(weights[6:])
        handed = run_train(x_now.reshape(ROWS * 4, WIDTH), x_next.reshape(ROWS * 4, WIDTH), labels_now, params, velocities)
        outs = run_next(params, velocities, handed)
        return (outs[0], *turn_head(outs[1:7]), *turn_head(outs[7:]))

    split = P('data')
    in_specs = (split, split, split) + (P(),) * 12
    out_specs = (split,) + (P(),) * 12
    return jax.shard_map(local_step, mesh=mesh, in_specs=in_specs, out_specs=out_specs, check_vma=False)
```

```python
import jax
import jax.numpy as jnp
from jax import lax
from jax.experimental import pallas as pl
from jax.experimental.pallas import tpu as pltpu
from jax.sharding import PartitionSpec as P

MOMENTUM = 0.9
TRUST = 0.1
LN_EPS = 1e-6
GELU_A = 0.7978845608028654
GELU_B = 0.044715 * GELU_A
F32 = jnp.float32
BF16 = jnp.bfloat16
VMEM_BYTES = 66_000_000

IMGS, TOKENS, WIDTH = 4, 784, 128
MERGED = TOKENS // 4
ROWS = IMGS * MERGED
WIDE = 4 * WIDTH
HID_ONE, HID_TWO = 4 * WIDTH, 4 * WIDE
CLASSES = 1000
TILE = 256
SHARD = 64
N_TILES = HID_TWO // TILE
FWD_TILE = 512


def dot_nn(a, b):
    return lax.dot_general(a, b, (((1,), (0,)), ((), ())), preferred_element_type=F32)


def dot_nt(a, b):
    return lax.dot_general(a, b, (((1,), (1,)), ((), ())), preferred_element_type=F32)


def dot_tn(a, b):
    return lax.dot_general(a, b, (((0,), (0,)), ((), ())), preferred_element_type=F32)


def norm_parts(vals):
    centered = vals - jnp.mean(vals, axis=-1, keepdims=True)
    variance = jnp.mean(centered * centered, axis=-1, keepdims=True)
    rstd = lax.rsqrt(variance + LN_EPS)
    return centered * rstd, rstd


def norm_back(grad, normed, rstd):
    mean_g = jnp.mean(grad, axis=-1, keepdims=True)
    mean_gn = jnp.mean(grad * normed, axis=-1, keepdims=True)
    return rstd * (grad - mean_g - normed * mean_gn)


def gelu_parts(pre):
    square = pre * pre
    half = 0.5 * jnp.tanh(pre * (GELU_A + GELU_B * square)) + 0.5
    return square, half


def gelu_slope(pre, square, half):
    return half * (1.0 + pre * (1.0 - half) * (2.0 * GELU_A + 6.0 * GELU_B * square))


def cast_rows(dst, src, rows, step):
    def body(i, carry):
        sl = pl.ds(pl.multiple_of(i * step, step), step)
        dst[sl, :] = src[sl, :].astype(BF16)
        return carry
    lax.fori_loop(0, rows // step, body, 0)


def lanes(index, size):
    return pl.ds(pl.multiple_of(index * size, size), size)


def permute_tokens(x_ref, x_f32, r0):
    x_f32[...] = x_ref[...].astype(F32)
    for j in range(4):
        r0[:, j * WIDTH:(j + 1) * WIDTH] = x_f32[pl.ds(j, ROWS, stride=4), :].astype(BF16)


def stage_one_block(resid, w_up, w_down):
    res_f = resid.astype(F32)
    normed = norm_parts(res_f)[0].astype(BF16)
    pre = dot_nn(normed, w_up)
    act = (pre * gelu_parts(pre)[1]).astype(BF16)
    return (res_f + dot_nn(act, w_down)).astype(BF16)


def stage_one_forward(r0, r1, r2, up_one, down_one, slots=(), group=2):
    def body(j, carry):
        for k, steps in enumerate(slots):
            pl.when(j == k)(lambda steps=steps: run_all(steps))
        cuts = [lanes(group * j + k, WIDTH) for k in range(group)]
        mids = [stage_one_block(r0[:, sl], up_one[0], down_one[0]) for sl in cuts]
        for sl, mid in zip(cuts, mids):
            r1[:, sl] = mid
        for sl, mid in zip(cuts, mids):
            r2[:, sl] = stage_one_block(mid, up_one[1], down_one[1])
        return carry
    lax.fori_loop(0, IMGS // group, body, 0)


def stage_two_block(src, dst, normed_ref, acc, up_ref, down_ref):
    res_f = src[...].astype(F32)
    normed_ref[...] = norm_parts(res_f)[0].astype(BF16)
    acc[...] = res_f

    def body(t, carry):
        sl = lanes(t, FWD_TILE)
        pre = dot_nn(normed_ref[...], up_ref[:, sl])
        act = (pre * gelu_parts(pre)[1]).astype(BF16)
        acc[...] += dot_nn(act, down_ref[sl, :])
        return carry
    lax.fori_loop(0, HID_TWO // FWD_TILE, body, 0)
    dst[...] = acc[...].astype(BF16)


def image_rows():
    image = lax.broadcasted_iota(jnp.int32, (8, ROWS), 0)
    row = lax.broadcasted_iota(jnp.int32, (8, ROWS), 1)
    inside = (row >= image * MERGED) & (row < (image + 1) * MERGED)
    return jnp.where(inside, 1.0, 0.0).astype(BF16)


def pooled_norm(resid):
    pooled = dot_nn(image_rows(), resid) * (1.0 / MERGED)
    return norm_parts(pooled)


UNIT = 1024
N_UNITS = 9
SHARE_ROWS = N_UNITS * UNIT
CLASS_PAD = 1024
DEVS = 8
SUBLANES = 8
LAST = N_UNITS - 1
HELD = 4
MATRICES = 10
PAIR_OUT, FIRST_OUT, SECOND_OUT, SECOND_BACK, FIRST_BACK, PAIR_BACK = range(6)


def start_all(copies):
    for copy in copies:
        copy.start()


def wait_all(copies):
    for copy in copies:
        copy.wait()


def sum_rows(tile):
    rows, cols = tile.shape
    return jnp.sum(tile.reshape(rows // 8, 8, cols), axis=0)


def square_sum(ref, start, rows, step):
    def body(i, total):
        part = ref[pl.ds(pl.multiple_of(start + i * step, step), step), :].astype(F32)
        return total + sum_rows(part * part)
    return lax.fori_loop(0, rows // step, body, jnp.zeros((SUBLANES, ref.shape[1]), F32))


def total_of(tile):
    return jnp.sum(jnp.sum(tile, axis=0, keepdims=True), axis=1, keepdims=True)


def run_all(steps):
    for action, unit in steps:
        action(unit)


class Links:
    def __init__(self, own, final, land1, land2, sems):
        self.own, self.final, self.land1, self.land2, self.sems = own, final, land1, land2, sems
        me = lax.axis_index('data')
        self.me = me
        self.core, self.x, self.y = lax.rem(me, 2), lax.rem(me // 2, 2), me // 4
        self.pair = me + 1 - 2 * self.core
        self.x_peer = me + 2 - 4 * self.x
        self.y_peer = me + 4 - 8 * self.y

    def rows(self, unit, offset, size):
        return pl.ds(pl.multiple_of(unit * UNIT + offset, SHARD), size)

    def half(self, unit, offset, size):
        return self.rows(unit, self.core * WIDE + offset, size)

    def copy(self, unit, phase, lane, src, dst, peer):
        return pltpu.make_async_remote_copy(
            src_ref=src, dst_ref=dst, send_sem=self.sems.at[unit, phase, lane, 0], recv_sem=self.sems.at[unit, phase, lane, 1],
            device_id=(peer,), device_id_type=pl.DeviceIdType.MESH)

    def copies(self, unit, phase):
        x, y = self.x, self.y
        own, final = self.own, self.final
        if phase == PAIR_OUT:
            sl = self.rows(unit, (1 - self.core) * WIDE, WIDE)
            return [self.copy(unit, PAIR_OUT, 0, own.at[sl], final.at[sl], self.pair)]
        if phase == FIRST_OUT:
            land = lambda k: self.land1.at[pl.ds(pl.multiple_of(unit * TILE + k * WIDTH, WIDTH), WIDTH)]
            return [self.copy(unit, FIRST_OUT, 0, own.at[self.half(unit, (1 - x) * WIDTH, WIDTH)], land(0), self.x_peer),
                    self.copy(unit, FIRST_OUT, 1, own.at[self.half(unit, TILE + (1 - y) * WIDTH, WIDTH)], land(1), self.y_peer)]
        if phase == SECOND_OUT:
            land = lambda k: self.land2.at[pl.ds(pl.multiple_of(unit * WIDTH + k * SHARD, SHARD), SHARD)]
            return [self.copy(unit, SECOND_OUT, 0, own.at[self.half(unit, x * WIDTH + (1 - y) * SHARD, SHARD)], land(0), self.y_peer),
                    self.copy(unit, SECOND_OUT, 1, own.at[self.half(unit, TILE + y * WIDTH + (1 - x) * SHARD, SHARD)], land(1), self.x_peer)]
        if phase == SECOND_BACK:
            first = self.half(unit, x * WIDTH + y * SHARD, SHARD)
            second = self.half(unit, TILE + y * WIDTH + x * SHARD, SHARD)
            return [self.copy(unit, SECOND_BACK, 0, final.at[first], final.at[first], self.y_peer),
                    self.copy(unit, SECOND_BACK, 1, final.at[second], final.at[second], self.x_peer)]
        if phase == FIRST_BACK:
            first, second = self.half(unit, x * WIDTH, WIDTH), self.half(unit, TILE + y * WIDTH, WIDTH)
            return [self.copy(unit, FIRST_BACK, 0, final.at[first], final.at[first], self.x_peer),
                    self.copy(unit, FIRST_BACK, 1, final.at[second], final.at[second], self.y_peer)]
        sl = self.half(unit, 0, WIDE)
        return [self.copy(unit, PAIR_BACK, 0, final.at[sl], final.at[sl], self.pair)]

    def start(self, unit, phase):
        for copy in self.copies(unit, phase):
            copy.start()

    def wait(self, unit, phase):
        for copy in self.copies(unit, phase):
            copy.wait()

    def reduce_pair(self, unit):
        self.wait(unit, PAIR_OUT)
        x, y = self.x, self.y
        for offset in ((1 - x) * WIDTH, TILE + (1 - y) * WIDTH, x * WIDTH, TILE + y * WIDTH):
            sl = self.half(unit, offset, WIDTH)
            self.own[sl, :] = self.own[sl, :] + self.final[sl, :]
        self.start(unit, FIRST_OUT)

    def reduce_first(self, unit):
        self.wait(unit, FIRST_OUT)
        x, y = self.x, self.y
        for keep in (False, True):
            for lane, base, here, there in ((0, x * WIDTH, y, 0), (1, TILE + y * WIDTH, x, WIDTH)):
                part = here if keep else 1 - here
                sl = self.half(unit, base + part * SHARD, SHARD)
                land = pl.ds(pl.multiple_of(unit * TILE + there + part * SHARD, SHARD), SHARD)
                self.own[sl, :] = self.own[sl, :] + self.land1[land, :]
        self.start(unit, SECOND_OUT)

    def reduce_second(self, unit):
        self.wait(unit, SECOND_OUT)
        for lane, offset in ((0, self.x * WIDTH + self.y * SHARD), (1, TILE + self.y * WIDTH + self.x * SHARD)):
            sl = self.half(unit, offset, SHARD)
            land = pl.ds(pl.multiple_of(unit * WIDTH + lane * SHARD, SHARD), SHARD)
            self.final[sl, :] = self.own[sl, :] + self.land2[land, :]

    def forward(self, unit, phase):
        self.wait(unit, phase)
        self.start(unit, phase + 1)


def train_kernel(x_hbm, x_next_hbm, vup1_hbm, vdn1_hbm, vmg_hbm, labels_ref, up1_hbm, dn1_hbm, mg_hbm, up2_hbm, dn2_hbm, hd_hbm,
                 final, st_up1, st_dn1, st_mg, st_up2, st_dn2, r0, g_hd, x_f32, acc, scale_ref,
                 x_v, gb_turn,
                 up1, dn1, mg, up2, dn2, hd,
                 r1, r2, s0, s1, normed_ref, grad_a, grad_b, sems,
                 du1, dv1, own, land1, land2, factors, w_sums, g_sums, link_sems, factor_sems):
    links = Links(own, final, land1, land2, link_sems)
    me = links.me
    st_hd = st_dn2.at[pl.ds(0, CLASSES)]
    copies = [pltpu.make_async_copy(src, dst, sems.at[i]) for i, (src, dst) in enumerate((
        (x_hbm, x_v), (up1_hbm, st_up1), (dn1_hbm, st_dn1), (mg_hbm, st_mg),
        (up2_hbm.at[0], st_up2), (dn2_hbm.at[0], st_dn2),
        (up2_hbm.at[1], st_up2), (dn2_hbm.at[1], st_dn2), (hd_hbm, st_hd)))]
    start_all(copies[:3])
    barrier = pltpu.get_barrier_semaphore()
    for k in range(1, DEVS):
        pl.semaphore_signal(barrier, inc=1, device_id=(lax.rem(me + k, DEVS),), device_id_type=pl.DeviceIdType.MESH)
    copies[0].wait()
    permute_tokens(x_v, x_f32, r0)
    wait_all(copies[1:3])
    start_all(copies[3:6])
    for n in range(2):
        cast_rows(up1.at[n], st_up1.at[n], WIDTH, SHARD)
        cast_rows(dn1.at[n], st_dn1.at[n], WIDE, TILE)
    stage_one_forward(r0, r1, r2, up1, dn1)
    copies[3].wait()
    cast_rows(mg, st_mg, WIDE, SHARD)
    s0[...] = dot_nn(r2[...], mg[...]).astype(BF16)
    s2 = grad_a
    for n, (src, dst) in enumerate(((s0, s1), (s1, s2))):
        copies[4 + 2 * n].wait()
        cast_rows(up2.at[n], st_up2, WIDE, 16)
        if n == 0:
            copies[6].start()
        copies[5 + 2 * n].wait()
        cast_rows(dn2.at[n], st_dn2, 2048, SHARD)
        copies[7 + n].start()
        stage_two_block(src, dst, normed_ref, acc, up2.at[n], dn2.at[n])
    copies[8].wait()
    cast_rows(hd, st_hd, 992, 32)
    hd[992:CLASSES, :] = st_hd[992:CLASSES, :].astype(BF16)
    hd[CLASSES:, :] = jnp.zeros((CLASS_PAD - CLASSES, WIDE), BF16)
    head_normed, head_rstd = pooled_norm(s2[...])
    head_b = head_normed.astype(BF16)
    class_id = lax.broadcasted_iota(jnp.int32, (SUBLANES, CLASS_PAD), 1)
    row_id = lax.broadcasted_iota(jnp.int32, (SUBLANES, CLASS_PAD), 0)
    logits = jnp.where(class_id < CLASSES, dot_nt(head_b, hd[...]), -jnp.inf)
    top = jnp.max(logits, axis=-1, keepdims=True)
    expd = jnp.exp(logits - top)
    probs = expd / jnp.sum(expd, axis=-1, keepdims=True)
    label = jnp.zeros((SUBLANES, CLASS_PAD), jnp.int32)
    for i in range(IMGS):
        label = jnp.where(row_id == i, labels_ref[i], label)
    onehot = jnp.where(class_id == label, 1.0, 0.0)
    grad_logits = jnp.where(row_id < IMGS, (probs - onehot) * (1.0 / (IMGS * DEVS)), 0.0).astype(BF16)
    factors[me, :, :WIDE] = head_b
    factors[me, :, WIDE:] = grad_logits
    grad_pooled = norm_back(dot_nn(grad_logits, hd[...]), head_normed, head_rstd) * (1.0 / MERGED)
    grad_a[...] = dot_tn(image_rows(), grad_pooled.astype(BF16)).astype(BF16)

    pl.semaphore_wait(barrier, DEVS - 1)

    def factor_copy(k):
        return pltpu.make_async_remote_copy(
            src_ref=factors.at[me], dst_ref=factors.at[me], send_sem=factor_sems.at[k, 0], recv_sem=factor_sems.at[k, 1],
            device_id=(lax.rem(me + k, DEVS),), device_id_type=pl.DeviceIdType.MESH)

    grads = (grad_a, grad_b)
    for step, n in enumerate((1, 0)):
        g_in, g_out = grads[step], grads[1 - step]
        src = (s0, s1)[n]
        normed_ref[...] = norm_parts(src[...].astype(F32))[0].astype(BF16)
        acc[...] = jnp.zeros_like(acc)

        def tile(t, row, n=n, g_in=g_in):
            sl = lanes(t, TILE)
            pre = dot_nn(normed_ref[...], up2[n, :, sl])
            square, half = gelu_parts(pre)
            act = (pre * half).astype(BF16)
            grad_pre = (gelu_slope(pre, square, half) * dot_nt(g_in[...], dn2[n, sl, :])).astype(BF16)
            own[pl.ds(row + TILE, TILE), :] = dot_tn(act, g_in[...]).astype(BF16)
            grad_up = dot_tn(normed_ref[...], grad_pre).astype(BF16)
            own[pl.ds(row, TILE), :TILE] = grad_up[:TILE]
            own[pl.ds(row, TILE), TILE:] = grad_up[TILE:]
            acc[...] += dot_nt(grad_pre, up2[n, :, sl])

        def body(p, carry, step=step, tile=tile):
            unit = step * 4 + p
            row = pl.multiple_of(unit * UNIT, UNIT)

            tile(2 * p, row)
            if step:
                links.reduce_pair(unit - 1)
            else:
                pl.when(p > 0)(lambda: links.reduce_pair(unit - 1))
            tile(2 * p + 1, row + WIDE)
            if step:
                links.reduce_first(unit - 4)
            links.start(unit, PAIR_OUT)
            return carry
        if step == 0:
            for k in range(1, DEVS):
                factor_copy(k).start()
        lax.fori_loop(0, N_TILES // 2, body, 0)
        normed_f, rstd = norm_parts(src[...].astype(F32))
        g_out[...] = (norm_back(acc[...], normed_f, rstd) + g_in[...].astype(F32)).astype(BF16)
    own[LAST * UNIT:LAST * UNIT + WIDE, :] = dot_tn(r2[...], grad_a[...]).astype(BF16)
    grad_b[...] = dot_nt(grad_a[...], mg[...]).astype(BF16)

    def reduced(unit):
        links.reduce_second(unit)
        links.start(unit, SECOND_BACK)

    def finish(unit):
        links.wait(unit, PAIR_BACK)
        start = unit * UNIT
        if unit < LAST:
            for k in range(4):
                matrix = (6 if unit < HELD else 5) + 2 * (k % 2)
                g_sums[matrix] += square_sum(final, start + k * TILE, TILE, SHARD)
        else:
            g_sums[4] = square_sum(final, start, WIDE, SHARD)
            for k in range(4):
                g_sums[k] = square_sum(final, start + WIDE + k * WIDTH, WIDTH, SHARD)

    def weigh(matrix, ref, rows, step):
        w_sums[pl.ds(matrix * SUBLANES, SUBLANES), :] = jnp.broadcast_to(total_of(square_sum(ref, 0, rows, step)), (SUBLANES, WIDTH))

    reloads = [pltpu.make_async_copy(src, dst, sems.at[9 + i]) for i, (src, dst) in enumerate((
        (up2_hbm.at[0], st_up2), (dn2_hbm.at[1], st_dn2), (x_next_hbm, x_v), (dn2_hbm.at[0], st_dn2)))]

    speeds = [pltpu.make_async_copy(src, dst, sems.at[13 + i]) for i, (src, dst) in enumerate((
        (vup1_hbm.at[0], acc.at[pl.ds(0, WIDTH)]), (vup1_hbm.at[1], acc.at[pl.ds(WIDTH, WIDTH)]), (vmg_hbm, acc.at[pl.ds(TILE, WIDE)]),
        (vdn1_hbm.at[0], x_f32.at[pl.ds(0, WIDE)]), (vdn1_hbm.at[1], x_f32.at[pl.ds(WIDE, WIDE)])))]

    def scale_of(matrix):
        sl = pl.ds(matrix * SUBLANES, SUBLANES)
        scale = TRUST * (jnp.sqrt(w_sums[sl, :]) / jnp.sqrt(total_of(g_sums[matrix])))
        scale_ref[sl, :] = scale
        return scale[:1, :1]

    def update_small(_):
        wait_all(speeds)
        small = final.at[pl.ds(LAST * UNIT, UNIT)]
        for n in range(2):
            grad = small.at[pl.ds(WIDE + n * WIDTH, WIDTH)]
            lars_matrix(2, row_pieces(st_up1.at[n], acc.at[pl.ds(n * WIDTH, WIDTH)], grad, up1.at[n], SHARD), scale_of(n))
            gb_turn[...] = small[pl.ds(WIDE + TILE + n * WIDTH, WIDTH), :].astype(F32).T
            lars_matrix(4, row_pieces(st_dn1.at[n], x_f32.at[pl.ds(n * WIDE, WIDE)], gb_turn, dn1.at[n], WIDTH), scale_of(2 + n))
        lars_matrix(8, row_pieces(st_mg, acc.at[pl.ds(TILE, WIDE)], small.at[pl.ds(0, WIDE)], mg, SHARD), scale_of(4))

    def weigh_small(_):
        for n in range(2):
            weigh(n, st_up1.at[n], WIDTH, SHARD)
            weigh(2 + n, st_dn1.at[n], WIDE, WIDTH)
        weigh(4, st_mg, WIDE, SHARD)
        weigh(6, st_up2, WIDE, 16)
        w_hd = square_sum(st_dn2, 0, 992, 32) + square_sum(st_dn2, 992, SUBLANES, SUBLANES)
        w_sums[pl.ds(9 * SUBLANES, SUBLANES), :] = jnp.broadcast_to(total_of(w_hd), (SUBLANES, WIDTH))
        start_all(reloads[:3])

    def weigh_first(_):
        wait_all(reloads[:3])
        weigh(5, st_up2, WIDE, 16)
        weigh(8, st_dn2, HID_TWO, SHARD)
        reloads[3].start()
        permute_tokens(x_v, x_f32, r0)
        start_all(speeds)

    def weigh_second(_):
        reloads[3].wait()
        weigh(7, st_dn2, HID_TWO, SHARD)
        g_sums[9] = square_sum(g_hd, 0, CLASS_PAD, SHARD)

    def back_first(unit):
        links.forward(unit, SECOND_BACK)

    def back_pair(unit):
        links.forward(unit, FIRST_BACK)

    g_sums[...] = jnp.zeros_like(g_sums)
    links.reduce_pair(7)
    first = links.reduce_first
    slots = {1: (((reduced, 0), (reduced, 1), (reduced, 2), (first, 4)), ((first, 5),), ((reduced, 3),), ((first, 6), (back_first, 0))),
             0: (((back_first, 1),), ((back_first, 2),), ((reduced, 4),), ((first, 7),))}

    for n, src, g_in, g_out in ((1, r1, grad_b, grad_a), (0, r0, grad_a, grad_b)):
        du1[...] = jnp.zeros_like(du1)
        dv1[...] = jnp.zeros_like(dv1)

        def body(j, carry, n=n, src=src, g_in=g_in, g_out=g_out):
            sl = lanes(j, WIDTH)
            normed_f, rstd = norm_parts(src[:, sl].astype(F32))
            normed = normed_f.astype(BF16)
            grad = g_in[:, sl]
            pre = dot_nn(normed, up1[n])
            square, half = gelu_parts(pre)
            act = (pre * half).astype(BF16)
            grad_pre = (gelu_slope(pre, square, half) * dot_nt(grad, dn1[n])).astype(BF16)
            dv1[...] += dot_tn(grad, act)
            du1[...] += dot_tn(normed, grad_pre)
            if n:
                back = norm_back(dot_nt(grad_pre, up1[n]), normed_f, rstd)
                g_out[:, sl] = (back + grad.astype(F32)).astype(BF16)
            for k, steps in enumerate(slots[n]):
                pl.when(j == k)(lambda steps=steps: run_all(steps))
            return carry
        lax.fori_loop(0, 4, body, 0)
        base = LAST * UNIT + WIDE + n * WIDTH
        own[base:base + WIDTH, :] = du1[...].astype(BF16)
        own[base + TILE:base + TILE + WIDTH, :] = dv1[...].astype(BF16)
    links.start(LAST, PAIR_OUT)

    for k in range(1, DEVS):
        factor_copy(k).wait()

    def head_tile(c, carry):
        sl = pl.ds(pl.multiple_of(WIDE + c * WIDTH, WIDTH), WIDTH)
        total = jnp.zeros((WIDTH, WIDE), F32)
        for d in range(DEVS):
            total += dot_tn(factors[d, :, sl], factors[d, :, :WIDE]).astype(BF16).astype(F32)
        g_hd[pl.ds(pl.multiple_of(c * WIDTH, WIDTH), WIDTH), :] = total.astype(BF16)
        return carry
    half_tiles = CLASS_PAD // WIDTH // 2
    lax.fori_loop(0, half_tiles, head_tile, 0)
    run_all(((links.reduce_pair, LAST), (reduced, 5), (back_first, 3)))
    lax.fori_loop(half_tiles, 2 * half_tiles, head_tile, 0)
    run_all(((reduced, 6), (weigh_small, 0), (first, LAST), (weigh_first, 0), (back_pair, 0), (back_pair, 1), (finish, 0), (reduced, 7),
             (reduced, LAST), (weigh_second, 0), (back_pair, 2), (finish, 1), (back_first, 4), (finish, 2), (back_first, LAST),
             (back_first, 5), (back_pair, 3), (back_first, 6), (finish, 3), (back_pair, LAST), (back_pair, 4), (back_first, 7),
             (finish, LAST), (update_small, 0)))
    slots = ((back_pair, 5),), ((back_pair, 6), (finish, 4)), ((finish, 5),), ((back_pair, 7), (finish, 6))
    stage_one_forward(r0, r1, r2, up1, dn1, slots, 1)
    r0[...] = dot_nn(r2[...], mg[...]).astype(BF16)
    finish(7)
    for matrix in range(5, MATRICES):
        scale_of(matrix)


def lars_matrix(steps, piece, scale, tails=(), begin=0):
    def update_piece(w, v, g, b):
        new_v = MOMENTUM * v[...] + scale * g[...].astype(F32)
        new_w = w[...] - new_v
        v[...] = new_v
        w[...] = new_w
        if b is not None:
            b[...] = new_w.astype(BF16)

    def update(i, carry):
        update_piece(*piece(i))
        return carry
    lax.fori_loop(begin, begin + steps, update, 0)
    for tail in tails:
        update_piece(*tail)


def row_pieces(w, v, g, b, step):
    def piece(i):
        sl = pl.ds(pl.multiple_of(i * step, step), step)
        return w.at[sl], v.at[sl], g.at[sl], b.at[sl]
    return piece


def up_pieces(w, v, g, b):
    def piece(i):
        part, h = i // N_TILES, lax.rem(i, N_TILES)
        rows, cols = lanes(part, 256), lanes(h, 256)
        g_rows = pl.ds(pl.multiple_of(h * 512, 512), 256)
        return w.at[rows, cols], v.at[rows, cols], g.at[g_rows, rows], b if b is None else b.at[rows, cols]
    return piece


def down_pieces(w, v, g, b):
    def piece(i):
        h, part = i // 2, lax.rem(i, 2)
        rows = pl.ds(pl.multiple_of(i * 128, 128), 128)
        g_rows = pl.ds(pl.multiple_of(h * 512 + 256 + part * 128, 128), 128)
        return w.at[rows], v.at[rows], g.at[g_rows], b if b is None else b.at[rows]
    return piece


class Pair:
    def __init__(self, w, v, out_w, out_v, buf_w, buf_v, sems, scales, slot, parts=1):
        self.buf_w, self.buf_v = buf_w, buf_v
        self.scale = scales.at[pl.ds(slot * SUBLANES, 1), pl.ds(0, 1)]
        ins = ((v, buf_v),) if w is None else ((v, buf_v), (w, buf_w))
        self.loads = [pltpu.make_async_copy(src, dst, sems.at[slot, parts, i]) for i, (src, dst) in enumerate(ins)]
        size = buf_w.shape[0] // parts
        cuts = [pl.ds(k * size, size) for k in range(parts)]
        self.parts = [[pltpu.make_async_copy(src.at[sl], dst.at[sl], sems.at[slot, k, i])
                       for i, (src, dst) in enumerate(((buf_w, out_w), (buf_v, out_v)))] for k, sl in enumerate(cuts)]
        self.stores = sum(self.parts, [])

    def update(self, steps, make, grad, cast, *rest, tails=()):
        wait_all(self.loads)
        count = len(self.parts)
        for k, part in enumerate(self.parts):
            lars_matrix(steps // count, make(self.buf_w, self.buf_v, grad, cast, *rest), self.scale[...], tails, k * (steps // count))
            start_all(part)


def next_kernel(up2_hbm, dn2_hbm, hd_hbm, vup2_hbm, vdn2_hbm, vhd_hbm,
                sums, w_up1, w_dn1, w_mg, in_up2, in_dn2, mid, g_hd, v_down, v_rest, scales,
                logits_ref, o_up1, o_dn1, o_mg, o_up2, o_dn2, o_hd, ov_up1, ov_dn1, ov_mg, ov_up2, ov_dn2, ov_hd,
                w_up2, w_dn2,
                vb_up2, vb_dn2, wb_up2, wb_dn2, up2, dn2, hd, s1, normed_ref, acc, sems, small_sems):
    done = [pltpu.make_async_copy(src, dst, small_sems.at[i]) for i, (src, dst) in enumerate((
        (w_up1, o_up1), (w_dn1, o_dn1), (w_mg, o_mg), (v_rest.at[pl.ds(TILE, WIDE)], ov_mg),
        (v_rest.at[pl.ds(0, WIDTH)], ov_up1.at[0]), (v_rest.at[pl.ds(WIDTH, WIDTH)], ov_up1.at[1]),
        (v_down.at[pl.ds(0, WIDE)], ov_dn1.at[0]), (v_down.at[pl.ds(WIDE, WIDE)], ov_dn1.at[1])))]
    wide_ups = [Pair((None, up2_hbm.at[1])[n], vup2_hbm.at[n], o_up2.at[n], ov_up2.at[n], (w_up2, wb_up2)[n], vb_up2.at[n],
                     sems, scales, 5 + n, 2) for n in range(2)]
    wide_downs = [Pair((None, dn2_hbm.at[1])[n], vdn2_hbm.at[n], o_dn2.at[n], ov_dn2.at[n], (w_dn2, wb_dn2)[n], vb_dn2.at[n],
                       sems, scales, 7 + n, 4) for n in range(2)]
    wb_hd, vb_hd = wb_dn2.at[pl.ds(0, CLASSES)], vb_dn2.at[1, pl.ds(0, CLASSES)]
    head = Pair(hd_hbm, vhd_hbm, o_hd, ov_hd, wb_hd, vb_hd, sems, scales, 9)
    for each in [head] + wide_ups[:1] + wide_downs[:1]:
        start_all(each.loads)
    start_all(done)
    start_all(wide_ups[1].loads)
    tail = pl.ds(992, SUBLANES)
    head.update(31, row_pieces, g_hd, hd, 32, tails=[(wb_hd.at[tail], vb_hd.at[tail], g_hd.at[tail], hd.at[tail])])
    wide_ups[0].update(16, up_pieces, sums.at[pl.ds(HELD * UNIT, HELD * UNIT)], up2)
    wide_downs[0].update(16, down_pieces, sums.at[pl.ds(HELD * UNIT, HELD * UNIT)], dn2)
    wait_all(head.stores)
    start_all(wide_downs[1].loads)
    wide_ups[1].update(16, up_pieces, sums.at[pl.ds(0, HELD * UNIT)], None)
    stage_two_block(mid, s1, normed_ref, acc, up2, dn2)
    wide_downs[1].update(16, down_pieces, sums.at[pl.ds(0, HELD * UNIT)], dn2)
    cast_rows(up2, wb_up2, WIDE, 16)
    stage_two_block(s1, s1, normed_ref, acc, up2, dn2)
    head_b = pooled_norm(s1[...])[0].astype(BF16)
    logits_ref[...] = dot_nt(head_b, hd[...])[:IMGS]
    wait_all(done)
    for each in wide_ups + wide_downs:
        wait_all(each.stores)


W_SHAPES = ((2, 128, 512), (2, 512, 128), (512, 512), (2, 512, 2048), (2, 2048, 512), (CLASSES, 512))
BUF_SHAPES = W_SHAPES[:3] + ((512, 2048), (2048, 512), (CLASSES, 512))


def vmem(shape, dtype):
    return pltpu.VMEM(shape, dtype)


ANY_SPEC = pl.BlockSpec(memory_space=pl.ANY)
VMEM_SPEC = pl.BlockSpec(memory_space=pltpu.VMEM)


def act(dtype=BF16):
    return vmem((ROWS, WIDE), dtype)


def f32_outs(shapes):
    return [jax.ShapeDtypeStruct(shape, F32) for shape in shapes]


DMA = pltpu.SemaphoreType.DMA


HANDED = ((SHARE_ROWS, WIDE), BF16), *((shape, F32) for shape in BUF_SHAPES[:5]), ((ROWS, WIDE), BF16), ((CLASS_PAD, WIDE), BF16), \
    ((ROWS * 4, WIDTH), F32), ((ROWS, WIDE), F32)
HANDED_BYTES = 25_200_000


def run_train(x_now, x_next, labels, params, velocities):
    return pl.pallas_call(
        train_kernel,
        out_shape=[vmem(*each) for each in HANDED] + f32_outs([(MATRICES * SUBLANES, WIDTH)]),
        in_specs=[ANY_SPEC] * 5 + [pl.BlockSpec(memory_space=pltpu.SMEM)] + [ANY_SPEC] * 6,
        out_specs=[VMEM_SPEC] * 11,
        scratch_shapes=[vmem((ROWS * 4, WIDTH), BF16), vmem((WIDE, WIDTH), F32)]
        + [vmem(shape, BF16) for shape in W_SHAPES[:5]] + [vmem((CLASS_PAD, WIDE), BF16)]
        + [act()] * 7 + [DMA((18,)), vmem((WIDTH, WIDE), F32), vmem((WIDTH, WIDE), F32)]
        + [vmem((rows, WIDE), BF16) for rows in (SHARE_ROWS, N_UNITS * TILE, N_UNITS * WIDTH)]
        + [vmem((DEVS, SUBLANES, WIDE + CLASS_PAD), BF16), vmem((MATRICES * SUBLANES, WIDTH), F32), vmem((MATRICES, SUBLANES, WIDE), F32)]
        + [DMA((N_UNITS, 6, 2, 2)), DMA((DEVS, 2))],
        compiler_params=pltpu.CompilerParams(vmem_limit_bytes=VMEM_BYTES - HANDED_BYTES, collective_id=0, has_side_effects=True),
        cost_estimate=pl.CostEstimate(flops=30_000_000_000, bytes_accessed=40_000_000, transcendentals=0),
        name='train_part',
    )(x_now, x_next, *velocities[:3], labels, *params)


def run_next(params, velocities, handed):
    held = [vmem(*each) for each in HANDED[4:6]]
    handed = [pltpu.with_memory_space_constraint(each, pltpu.VMEM) for each in handed[:10]] + list(handed[10:])
    outs = pl.pallas_call(
        next_kernel,
        out_shape=f32_outs([(IMGS, CLASSES)] + list(W_SHAPES) * 2) + held,
        in_specs=[ANY_SPEC] * 6 + [VMEM_SPEC] * 11,
        out_specs=[VMEM_SPEC] + [ANY_SPEC] * 12 + [VMEM_SPEC] * 2,
        scratch_shapes=[vmem(shape, F32) for shape in W_SHAPES[3:5] + BUF_SHAPES[3:5]]
        + [vmem(shape, BF16) for shape in BUF_SHAPES[3:]]
        + [act()] * 2 + [act(F32), DMA((10, 5, 2)), DMA((8,))],
        input_output_aliases={10 + i: 13 + i for i in range(2)},
        compiler_params=pltpu.CompilerParams(vmem_limit_bytes=VMEM_BYTES - HANDED_BYTES),
        cost_estimate=pl.CostEstimate(flops=10_000_000_000, bytes_accessed=100_000_000, transcendentals=0),
        name='next_part',
    )(*params[3:], *velocities[3:], *handed)
    return outs[:13]


def turn_head(arrays):
    return (*arrays[:5], arrays[5].T)


def solution(mesh):
    def local_step(x_now, labels_now, x_next, *weights):
        params, velocities = turn_head(weights[:6]), turn_head(weights[6:])
        handed = run_train(x_now.reshape(ROWS * 4, WIDTH), x_next.reshape(ROWS * 4, WIDTH), labels_now, params, velocities)
        outs = run_next(params, velocities, handed)
        return (outs[0], *turn_head(outs[1:7]), *turn_head(outs[7:]))

    split = P('data')
    in_specs = (split, split, split) + (P(),) * 12
    out_specs = (split,) + (P(),) * 12
    return jax.shard_map(local_step, mesh=mesh, in_specs=in_specs, out_specs=out_specs, check_vma=False)
```
